32 devices in a mesh: data: 32 (over z, y, x, core).
Axes of the slice: x: 2, y: 2, z: 4, core: 2. Of those that a mesh axis runs over, the one named last changes fastest.
Arguments:
- x_act: bfloat16 [256, 196, 512], P('data')
- y_tgt: bfloat16 [256, 196, 512], P('data')
- w_in: float32 [4, 512, 2048], replicated
- w_out: float32 [4, 2048, 512], replicated
Outputs:
- output 1: float32 [4, 512, 2048], replicated
- output 2: float32 [4, 2048, 512], replicated
- output 3: float32 [], replicated
All inputs are finite; a program needn't handle non-finite values.
Results may differ from the reference program's by a relative error of at most 0.00183218.
Values are sent between devices in bfloat16 or wider.
A program may use at most 1 GiB of HBM per device.

```python
import math
import jax
import jax.numpy as jnp
from jax import lax

D = 512
FF = 2048
SEQ = 196
LAYERS = 4
BATCH_DEV = 4
DEVICES = 32
MICRO_STEPS = 2
BLOCKS = DEVICES * MICRO_STEPS
BATCH_ALL = BLOCKS * BATCH_DEV
BLOCK_ROWS = BATCH_DEV * SEQ
RHO_RADIUS = 0.1 * math.sqrt(LAYERS * (D + FF))
LEARN_RATE = 1.0
TOK_SCALE = 1.0 / (BATCH_ALL * SEQ * D)


def setup_inputs(seed: int = 0) -> dict:
    root_key = jax.random.key(seed)
    k_x, k_y, k_in, k_out, k_gain = jax.random.split(root_key, 5)
    x_act = jax.random.normal(k_x, (BATCH_ALL, SEQ, D), jnp.float32).astype(jnp.bfloat16)
    y_tgt = jax.random.normal(k_y, (BATCH_ALL, SEQ, D), jnp.float32).astype(jnp.bfloat16)
    w_in = jax.random.normal(k_in, (LAYERS, D, FF), jnp.float32) * (D ** -0.5)
    layer_gain = jax.random.uniform(k_gain, (LAYERS, 1, 1), jnp.float32, 0.3, 0.9)
    w_out = jax.random.normal(k_out, (LAYERS, FF, D), jnp.float32) * (FF ** -0.5) * layer_gain
    return {"x_act": x_act, "y_tgt": y_tgt, "w_in": w_in, "w_out": w_out}


def gelu_tanh(z_val):
    return jax.nn.gelu(z_val, approximate=True)


def forward_layer(h_act, wi_cast, wo_cast):
    z_pre = jnp.dot(h_act, wi_cast, preferred_element_type=jnp.float32).astype(jnp.bfloat16)
    gelu_out = gelu_tanh(z_pre.astype(jnp.float32)).astype(jnp.bfloat16)
    u_out = jnp.dot(gelu_out, wo_cast, preferred_element_type=jnp.float32)
    return (h_act.astype(jnp.float32) + u_out).astype(jnp.bfloat16), z_pre


def block_sums(x_blk, y_blk, wi_cast, wo_cast):
    h_list = [x_blk]
    z_list = []
    for layer_idx in range(LAYERS):
        h_next, z_pre = forward_layer(h_list[-1], wi_cast[layer_idx], wo_cast[layer_idx])
        h_list.append(h_next)
        z_list.append(z_pre)
    out_err = h_list[-1].astype(jnp.float32) - y_blk.astype(jnp.float32)
    sq_sum = jnp.sum(out_err * out_err)
    back_grad = out_err.astype(jnp.bfloat16)
    sums_in = [None] * LAYERS
    sums_out = [None] * LAYERS
    for layer_idx in range(LAYERS - 1, -1, -1):
        gelu_out, gelu_vjp = jax.vjp(gelu_tanh, z_list[layer_idx].astype(jnp.float32))
        sums_out[layer_idx] = jnp.dot(gelu_out.astype(jnp.bfloat16).T, back_grad, preferred_element_type=jnp.float32)
        d_act = jnp.dot(back_grad, wo_cast[layer_idx].T, preferred_element_type=jnp.float32)
        d_pre = gelu_vjp(d_act)[0].astype(jnp.bfloat16)
        sums_in[layer_idx] = jnp.dot(h_list[layer_idx].T, d_pre, preferred_element_type=jnp.float32)
        if layer_idx > 0:
            back_in = jnp.dot(d_pre, wi_cast[layer_idx].T, preferred_element_type=jnp.float32)
            back_grad = (back_grad.astype(jnp.float32) + back_in).astype(jnp.bfloat16)
    return jnp.stack(sums_in), jnp.stack(sums_out), sq_sum


def grad_sums(x_blocks, y_blocks, wi_cast, wo_cast):
    def scan_body(acc_state, block_pair):
        acc_in, acc_out, acc_sq = acc_state
        s_in, s_out, s_sq = block_sums(block_pair[0], block_pair[1], wi_cast, wo_cast)
        return (acc_in + s_in, acc_out + s_out, acc_sq + s_sq), None
    init_state = (jnp.zeros((LAYERS, D, FF), jnp.float32), jnp.zeros((LAYERS, FF, D), jnp.float32), jnp.zeros((), jnp.float32))
    final_state, _ = lax.scan(scan_body, init_state, (x_blocks, y_blocks))
    return final_state


def reference(x_act, y_tgt, w_in, w_out):
    x_blocks = x_act.reshape(BLOCKS, BLOCK_ROWS, D)
    y_blocks = y_tgt.reshape(BLOCKS, BLOCK_ROWS, D)
    sum_in, sum_out, _ = grad_sums(x_blocks, y_blocks, w_in.astype(jnp.bfloat16), w_out.astype(jnp.bfloat16))
    grad_in = sum_in * TOK_SCALE
    grad_out = sum_out * TOK_SCALE
    grad_norm = jnp.sqrt(jnp.sum(grad_in * grad_in) + jnp.sum(grad_out * grad_out))
    perturb_coef = RHO_RADIUS / grad_norm
    pert_in = (w_in + perturb_coef * grad_in).astype(jnp.bfloat16)
    pert_out = (w_out + perturb_coef * grad_out).astype(jnp.bfloat16)
    second_in, second_out, second_sq = grad_sums(x_blocks, y_blocks, pert_in, pert_out)
    new_in = w_in - LEARN_RATE * (second_in * TOK_SCALE)
    new_out = w_out - LEARN_RATE * (second_out * TOK_SCALE)
    pert_loss = 0.5 * (second_sq * TOK_SCALE)
    return new_in, new_out, pert_loss
```

```python
import functools
import math

import jax
import jax.numpy as jnp
from jax import lax
from jax.experimental import pallas as pl
from jax.experimental.pallas import tpu as pltpu
from jax.sharding import PartitionSpec as P

MESH = pl.DeviceIdType.MESH
F32 = jnp.float32

class Geo:
    pass

def geometry():
    g = Geo()
    me = lax.axis_index("data")
    g.me = me
    g.c = lax.rem(me, 2)
    g.x = lax.rem(me // 2, 2)
    g.y = lax.rem(me // 4, 2)
    g.z = me // 8
    g.partner = me + 1 - 2 * g.c
    g.xn = me + 2 - 4 * g.x
    g.yn = me + 4 - 8 * g.y
    g.zm = me - 8
    g.zp = me + 8
    g.sink = jnp.logical_or(g.z == 0, g.z == 3)
    g.e = g.z // 3
    return g

def entry_barrier(g):
    bar = pltpu.get_barrier_semaphore()
    for d in (g.partner, g.xn, g.yn):
        pl.semaphore_signal(bar, inc=1, device_id=(d,), device_id_type=MESH)
    @pl.when(g.z > 0)
    def _():
        pl.semaphore_signal(bar, inc=1, device_id=(g.zm,), device_id_type=MESH)
    @pl.when(g.z < 3)
    def _():
        pl.semaphore_signal(bar, inc=1, device_id=(g.zp,), device_id_type=MESH)
    @pl.when(g.sink)
    def _():
        pl.semaphore_wait(bar, 4)
    @pl.when(jnp.logical_not(g.sink))
    def _():
        pl.semaphore_wait(bar, 5)

FD, FX1, FY1, FMA, FMB, FPA, FPB, FY3, FX3 = range(9)
NFLOW = 9
CD, CX1, CY1, CM, CP, CY3, CX3 = range(7)
NCRED = 7
SHAPES = ((256, 512), (512, 256))

def rem(a, n):
    return lax.rem(a, n)

class RS:
    def __init__(self, g, n, ns, nsl, lags, bufs, own, sq=None):
        self.g, self.n, self.ns, self.nsl = g, n, ns, nsl
        self.LD, self.L1, self.LZ, self.L3 = lags
        (self.S, self.rD, self.r1, self.rz, self.r3, self.ssem, self.rsem, self.cred) = bufs
        self.own = own
        self.lam1 = self.LD
        self.lam2 = self.lam1 + self.L1
        self.lam3 = self.lam2 + 3 * self.LZ
        self.lam4 = self.lam3 + self.L3

    def copy(self, T, flow, k, src, dst, dev):
        slot = rem(k, self.ns)
        return pltpu.make_async_remote_copy(src_ref=src, dst_ref=dst,
            send_sem=self.ssem.at[T, flow, slot], recv_sem=self.rsem.at[T, flow, slot],
            device_id=(dev,), device_id_type=MESH)

    def take_credit(self, T, cr, k):
        @pl.when(k >= self.ns)
        def _():
            pl.semaphore_wait(self.cred.at[T, cr], 1)

    def give_credit(self, T, cr, k, dev):
        @pl.when(k + self.ns < self.n)
        def _():
            pl.semaphore_signal(self.cred.at[T, cr], inc=1, device_id=(dev,), device_id_type=MESH)

    def rows(self, T):
        R = SHAPES[T][0]
        g = self.g
        half = g.c * (R // 2)
        a, b = half, half + R // 4
        return R, half, a, b

    def ds(self, start, size):
        return pl.ds(pl.multiple_of(start, 8), size)

    def cD(self, T, k):
        R, half, a, b = self.rows(T)
        src = self.S[T].at[rem(k, self.nsl), self.ds((1 - self.g.c) * (R // 2), R // 2), :]
        return self.copy(T, FD, k, src, self.rD[T].at[rem(k, self.ns)], self.g.partner)

    def cX1(self, T, k):
        R, half, a, b = self.rows(T)
        src = self.S[T].at[rem(k, self.nsl), self.ds(a + (1 - self.g.x) * (R // 8), R // 8), :]
        return self.copy(T, FX1, k, src, self.r1[T].at[rem(k, self.ns), 0], self.g.xn)

    def cY1(self, T, k):
        R, half, a, b = self.rows(T)
        src = self.S[T].at[rem(k, self.nsl), self.ds(b + (1 - self.g.y) * (R // 8), R // 8), :]
        return self.copy(T, FY1, k, src, self.r1[T].at[rem(k, self.ns), 1], self.g.yn)

    def zpart(self, T, ab, e):
        R, half, a, b = self.rows(T)
        base = (a + self.g.x * (R // 8)) if ab == 0 else (b + self.g.y * (R // 8))
        return self.ds(base + e * (R // 16), R // 16)

    def cZ(self, T, k, dirn, ab):
        src = self.S[T].at[rem(k, self.nsl), self.zpart(T, ab, dirn), :]
        dst = self.rz[T].at[rem(k, self.ns), ab, dirn]
        flow = (FMA, FMB, FPA, FPB)[2 * dirn + ab]
        return self.copy(T, flow, k, src, dst, self.g.zp if dirn else self.g.zm)

    def fin(self, T, ab, mine):
        R, half, a, b = self.rows(T)
        g = self.g
        base = (a + g.x * (R // 8)) if ab == 0 else (b + g.y * (R // 8))
        base = base + g.e * (R // 16)
        w = g.y if ab == 0 else g.x
        w = w if mine else 1 - w
        if T == 0:
            return self.ds(base, 16), pl.ds(pl.multiple_of(w * 256, 256), 256)
        return self.ds(base + w * 16, 16), pl.ds(0, 256)

    def c3(self, T, k, ab):
        r, cc = self.fin(T, ab, False)
        src = self.S[T].at[rem(k, self.nsl), r, cc]
        dst = self.r3[T].at[rem(k, self.ns), ab]
        return self.copy(T, FY3 if ab == 0 else FX3, k, src, dst, self.g.yn if ab == 0 else self.g.xn)

    def h0(self, T, k):
        self.take_credit(T, CD, k)
        self.cD(T, k).start()

    def h1(self, T, k):
        R, half, a, b = self.rows(T)
        c = self.cD(T, k)
        c.wait()
        s, q = rem(k, self.nsl), rem(k, self.ns)
        h = self.ds(half, R // 2)
        self.S[T][s, h, :] = self.S[T][s, h, :] + self.rD[T][q]
        self.give_credit(T, CD, k, self.g.partner)
        self.take_credit(T, CX1, k)
        self.cX1(T, k).start()
        self.take_credit(T, CY1, k)
        self.cY1(T, k).start()

    def h2(self, T, k):
        R, half, a, b = self.rows(T)
        self.cX1(T, k).wait()
        self.cY1(T, k).wait()
        s, q = rem(k, self.nsl), rem(k, self.ns)
        ra = self.ds(a + self.g.x * (R // 8), R // 8)
        rb = self.ds(b + self.g.y * (R // 8), R // 8)
        self.S[T][s, ra, :] = self.S[T][s, ra, :] + self.r1[T][q, 0]
        self.S[T][s, rb, :] = self.S[T][s, rb, :] + self.r1[T][q, 1]
        self.give_credit(T, CX1, k, self.g.xn)
        self.give_credit(T, CY1, k, self.g.yn)

    def hz(self, T, k, dirn):
        g = self.g
        p = g.z if dirn else 3 - g.z
        s, q = rem(k, self.nsl), rem(k, self.ns)
        cr = CP if dirn else CM
        up = g.zm if dirn else g.zp
        @pl.when(k < self.n)
        def _():
            @pl.when(p > 0)
            def _():
                for ab in (0, 1):
                    self.cZ(T, k, dirn, ab).wait_recv()
                for ab in (0, 1):
                    r = self.zpart(T, ab, dirn)
                    self.S[T][s, r, :] = self.S[T][s, r, :] + self.rz[T][q, ab, dirn]
                self.give_credit(T, cr, k, up)
            @pl.when(p < 3)
            def _():
                self.take_credit(T, cr, k)
                for ab in (0, 1):
                    self.cZ(T, k, dirn, ab).start()
            @pl.when(p == 3)
            def _():
                self.take_credit(T, CY3, k)
                self.c3(T, k, 0).start()
                self.take_credit(T, CX3, k)
                self.c3(T, k, 1).start()
        @pl.when(jnp.logical_and(k >= 1, p < 3))
        def _():
            for ab in (0, 1):
                self.cZ(T, k - 1, dirn, ab).wait_send()

    def h4(self, T, k):
        @pl.when(self.g.sink)
        def _():
            s, q = rem(k, self.nsl), rem(k, self.ns)
            for ab in (0, 1):
                self.c3(T, k, ab).wait()
            for ab in (0, 1):
                r, cc = self.fin(T, ab, True)
                self.own[T][k, ab] = self.S[T][s, r, cc] + self.r3[T][q, ab]
            self.give_credit(T, CY3, k, self.g.yn)
            self.give_credit(T, CX3, k, self.g.xn)

    def due(self, s, j, order):
        n = self.n
        def at(T, lam):
            d = j - T - lam
            return (s + d // 2) if d % 2 == 0 else None
        for what in order:
            for T in (0, 1):
                if what == 1:
                    k = at(T, self.lam1)
                    if k is not None:
                        pl.when(jnp.logical_and(k >= 0, k < n))(functools.partial(self.h1, T, k))
                elif what == 2:
                    k = at(T, self.lam2)
                    if k is not None:
                        pl.when(jnp.logical_and(k >= 0, k < n))(functools.partial(self.h2, T, k))
                        for dirn in (0, 1):
                            p = self.g.z if dirn else 3 - self.g.z
                            kz = k - p * (self.LZ // 2)
                            pl.when(jnp.logical_and(kz >= 0, kz <= n))(functools.partial(self.hz, T, kz, dirn))
                elif what == 4:
                    k = at(T, self.lam4)
                    if k is not None:
                        pl.when(jnp.logical_and(k >= 0, k < n))(functools.partial(self.h4, T, k))

    def n_ticks(self):
        last = 2 * (self.n - 1) + 1 + max(self.lam4, self.lam3 + 2)
        return last // 2 + 1

def rs_scratch(ns, nsl):
    out = []
    for T in (0, 1):
        R, C = SHAPES[T]
        out += [pltpu.VMEM((nsl, R, C), F32), pltpu.VMEM((ns, R // 2, C), F32), pltpu.VMEM((ns, 2, R // 8, C), F32),
                pltpu.VMEM((ns, 2, 2, R // 16, C), F32), pltpu.VMEM((ns, 2, 16, 256), F32)]
    out += [pltpu.SemaphoreType.DMA((2, NFLOW, ns)), pltpu.SemaphoreType.DMA((2, NFLOW, ns)), pltpu.SemaphoreType.REGULAR((2, NCRED))]
    return out

def unpack_scratch(refs):
    o, i = refs[0:5], refs[5:10]
    bufs = [[o[m], i[m]] for m in range(5)]
    return tuple(bufs) + tuple(refs[10:13])

def rs_only_kernel(n, ns, nsl, lags, nl, so_ref, si_ref, own_o, own_i, *scr):
    bufs = unpack_scratch(scr[:13])
    lsem = scr[13]
    g = geometry()
    entry_barrier(g)
    rs = RS(g, n, ns, nsl, lags, bufs, (own_o, own_i))
    def load(T, k):
        li, f = k // 8, rem(k, 8)
        if T == 0:
            src = so_ref.at[li, pl.ds(pl.multiple_of(f * 256, 256), 256), :]
        else:
            src = si_ref.at[li, :, pl.ds(pl.multiple_of(f * 256, 256), 256)]
        return pltpu.make_async_copy(src, bufs[0][T].at[rem(k, nsl)], lsem.at[T, rem(k, 2)])
    for T in (0, 1):
        load(T, 0).start()
    def body(s, _):
        for j in (0, 1):
            @pl.when(s < n)
            def _():
                load(j, s).wait()
                rs.h0(j, s)
                @pl.when(s + 1 < n)
                def _():
                    load(j, s + 1).start()
            rs.due(s, j, (4, 2, 1))
        return 0
    lax.fori_loop(0, rs.n_ticks(), body, 0)

def rs_only(so, si, ns=4, nsl=9, lags=(1, 2, 2, 2), cid=1):
    n = so.shape[0] * 8
    return pl.pallas_call(
        functools.partial(rs_only_kernel, n, ns, nsl, lags, so.shape[0]),
        out_shape=[jax.ShapeDtypeStruct((n, 2, 16, 256), F32)] * 2,
        in_specs=[pl.BlockSpec(memory_space=pl.ANY)] * 2,
        out_specs=[pl.BlockSpec(memory_space=pltpu.VMEM)] * 2,
        scratch_shapes=rs_scratch(ns, nsl) + [pltpu.SemaphoreType.DMA((2, 2))],
        compiler_params=pltpu.CompilerParams(collective_id=cid, has_side_effects=True, vmem_limit_bytes=60 * 2**20),
        name="rs_only",
    )(so, si)


GS3, GM, GP, GE0, GE1, GD = range(6)
NGF = 6

class AG:
    def __init__(self, g, n, lags, own, out, ssem, rsem, lsem, layer, ns):
        self.g, self.n, self.own, self.out = g, n, own, out
        self.ssem, self.rsem, self.lsem = ssem, rsem, lsem
        self.layer, self.ns = layer, ns
        self.G3, self.GZ, self.GE, self.GDL = lags
        self.m1 = self.G3
        self.m2 = self.m1 + 3 * self.GZ + self.GE
        self.m3 = self.m2 + self.GDL

    def region(self, T, k, row, nrow, col=None, ncol=None):
        li, f = self.layer(k // 8), rem(k, 8)
        f0 = f * 256
        if T == 0:
            c = slice(None) if col is None else pl.ds(pl.multiple_of(col, 256), ncol)
            return self.out[0].at[li, pl.ds(pl.multiple_of(f0 + row, 16), nrow), c]
        return self.out[1].at[li, pl.ds(pl.multiple_of(row, 16), nrow), pl.ds(pl.multiple_of(f0, 256), 256)]

    def base(self, T, ab, w):
        R = SHAPES[T][0]
        return self.g.c * (R // 2) + ab * (R // 4) + w * (R // 8)

    def piece(self, T, k, ab):
        R = SHAPES[T][0]
        g = self.g
        b = self.base(T, ab, g.x if ab == 0 else g.y) + g.e * (R // 16)
        w = g.y if ab == 0 else g.x
        if T == 0:
            return self.region(T, k, b, 16, w * 256, 256)
        return self.region(T, k, b + w * 16, 16)

    def zpart(self, T, k, ab, e):
        R = SHAPES[T][0]
        g = self.g
        return self.region(T, k, self.base(T, ab, g.x if ab == 0 else g.y) + e * (R // 16), R // 16)

    def rcopy(self, T, flow, k, src, dst, dev):
        return pltpu.make_async_remote_copy(src_ref=src, dst_ref=dst, send_sem=self.ssem.at[T, flow, rem(k, self.ns)],
            recv_sem=self.rsem.at[T, flow, k], device_id=(dev,), device_id_type=MESH)

    def wait2(self, sem, region):
        pltpu.make_async_copy(region, region, sem).wait()

    def pair(self, T, k):
        R = SHAPES[T][0]
        return self.region(T, k, 0, R // 8)

    def g0(self, T, k):
        g = self.g
        @pl.when(g.sink)
        def _():
            for ab in (0, 1):
                dst = self.piece(T, k, ab)
                src = self.own[T].at[k, ab]
                pltpu.make_async_copy(src, dst, self.lsem.at[T, ab, rem(k, self.ns)]).start()
                self.rcopy(T, GS3, k, src, dst, g.yn if ab == 0 else g.xn).start()

    def wait_s3(self, T, k):
        for ab in (0, 1):
            pltpu.make_async_copy(self.own[T].at[k, ab], self.piece(T, k, ab), self.lsem.at[T, ab, rem(k, self.ns)]).wait()
        two = self.own[T].at[k]
        self.wait2(self.ssem.at[T, GS3, rem(k, self.ns)], two)
        self.wait2(self.rsem.at[T, GS3, k], two)

    def gz(self, T, k, dirn):
        g = self.g
        e = 1 - dirn
        p = g.z if dirn else 3 - g.z
        fz = GP if dirn else GM
        fe = GE1 if e else GE0
        nxt = g.zp if dirn else g.zm
        @pl.when(k < self.n)
        def _():
            @pl.when(p == 0)
            def _():
                self.wait_s3(T, k)
            @pl.when(p > 0)
            def _():
                self.wait2(self.rsem.at[T, fz, k], self.pair(T, k))
            @pl.when(p < 3)
            def _():
                for ab in (0, 1):
                    r = self.zpart(T, k, ab, e)
                    self.rcopy(T, fz, k, r, r, nxt).start()
            for ab in (0, 1):
                r = self.zpart(T, k, ab, e)
                self.rcopy(T, fe, k, r, r, g.xn if ab == 0 else g.yn).start()
        @pl.when(jnp.logical_and(k >= 1, p < 3))
        def _():
            self.wait2(self.ssem.at[T, fz, rem(k - 1, self.ns)], self.pair(T, k - 1))

    def half(self, T, k, c):
        R = SHAPES[T][0]
        return self.region(T, k, c * (R // 2), R // 2)

    def g2(self, T, k):
        g = self.g
        for f in (GE0, GE1):
            self.wait2(self.ssem.at[T, f, rem(k, self.ns)], self.pair(T, k))
            self.wait2(self.rsem.at[T, f, k], self.pair(T, k))
        r = self.half(T, k, g.c)
        self.rcopy(T, GD, k, r, r, g.partner).start()

    def g3(self, T, k):
        r = self.half(T, k, self.g.c)
        self.rcopy(T, GD, k, r, r, self.g.partner).wait()

    def due(self, s, j):
        n = self.n
        def at(T, lam):
            d = j - T - lam
            return (s + d // 2) if d % 2 == 0 else None
        for T in (0, 1):
            k = at(T, 0)
            if k is not None:
                pl.when(jnp.logical_and(k >= 0, k < n))(functools.partial(self.g0, T, k))
        for T in (0, 1):
            k = at(T, self.m1)
            if k is not None:
                for dirn in (0, 1):
                    p = self.g.z if dirn else 3 - self.g.z
                    kz = k - p * (self.GZ // 2)
                    pl.when(jnp.logical_and(kz >= 0, kz <= n))(functools.partial(self.gz, T, kz, dirn))
        for T in (0, 1):
            k = at(T, self.m2)
            if k is not None:
                pl.when(jnp.logical_and(k >= 0, k < n))(functools.partial(self.g2, T, k))
            k = at(T, self.m3)
            if k is not None:
                pl.when(jnp.logical_and(k >= 0, k < n))(functools.partial(self.g3, T, k))

    def n_ticks(self):
        last = 2 * (self.n - 1) + 1 + max(self.m3, self.m1 + 3 * self.GZ + 2)
        return last // 2 + 1

def ag_scratch(n, ns, dtype):
    return [pltpu.VMEM((n, 2, 16, 256), dtype), pltpu.VMEM((n, 2, 16, 256), dtype),
            pltpu.SemaphoreType.DMA((2, NGF, ns)), pltpu.SemaphoreType.DMA((2, NGF, n)), pltpu.SemaphoreType.DMA((2, 2, ns))]

def ag_kernel(n, ns, lags, order, sc_ref, own_o, own_i, wo_ref, wi_ref, out_o, out_i, w_o, w_i, pe_o, pe_i, ssem, rsem, lsem, wsem):
    g = geometry()
    layer = lambda q: order[0] + order[1] * q
    ag = AG(g, n, lags, (pe_o, pe_i), (out_o, out_i), ssem, rsem, lsem, layer, ns)
    wag = AG(g, n, lags, (pe_o, pe_i), (wo_ref, wi_ref), ssem, rsem, lsem, layer, ns)
    entry_barrier(g)
    @pl.when(g.sink)
    def _():
        def issue(k, _):
            for T in (0, 1):
                for ab in (0, 1):
                    pltpu.make_async_copy(wag.piece(T, k, ab), (w_o, w_i)[T].at[k, ab], wsem.at[T]).start()
            return 0
        lax.fori_loop(0, n, issue, 0)
        pltpu.make_async_copy(w_o, w_o, wsem.at[0]).wait()
        pltpu.make_async_copy(w_i, w_i, wsem.at[1]).wait()
    a, b = sc_ref[0], sc_ref[1]
    def body(s, _):
        @pl.when(jnp.logical_and(g.sink, s < n))
        def _():
            for T in (0, 1):
                ow = (own_o, own_i)[T]
                (pe_o, pe_i)[T][s] = ((w_o, w_i)[T][s] + a * (ow[s] * b)).astype(pe_o.dtype)
        for j in (0, 1):
            ag.due(s, j)
        return 0
    lax.fori_loop(0, ag.n_ticks(), body, 0)

def ag_call(sc, own_o, own_i, wo, wi, dtype, order, ns=4, lags=(4, 4, 4, 2), cid=2):
    n = own_o.shape[0]
    L = wo.shape[0]
    vm = pl.BlockSpec(memory_space=pltpu.VMEM)
    anyspec = pl.BlockSpec(memory_space=pl.ANY)
    return pl.pallas_call(
        functools.partial(ag_kernel, n, ns, lags, order),
        out_shape=[jax.ShapeDtypeStruct(wo.shape, dtype), jax.ShapeDtypeStruct(wi.shape, dtype)],
        in_specs=[pl.BlockSpec(memory_space=pltpu.SMEM), vm, vm, anyspec, anyspec],
        out_specs=[anyspec, anyspec],
        scratch_shapes=[pltpu.VMEM((n, 2, 16, 256), F32)] * 2 + ag_scratch(n, ns, dtype) + [pltpu.SemaphoreType.DMA((2,))],
        compiler_params=pltpu.CompilerParams(collective_id=cid, has_side_effects=True, vmem_limit_bytes=40 * 2**20),
        name="gather",
    )(sc, own_o, own_i, wo, wi)


RHO_FRAC = 0.1
LEARN_RATE = 1.0
BF = jnp.bfloat16


def gelu_tanh(z_val):
    return jax.nn.gelu(z_val, approximate=True)


def dot(a, b, dims):
    return lax.dot_general(a, b, (dims, ((), ())), preferred_element_type=F32)


def forward(x, wi, wo):
    h, hs, zs = x, [x], []
    for layer in range(len(wi)):
        z = dot(h, wi[layer], ((1,), (0,))).astype(BF)
        a = gelu_tanh(z.astype(F32)).astype(BF)
        h = (h.astype(F32) + dot(a, wo[layer], ((1,), (0,)))).astype(BF)
        hs.append(h)
        zs.append(z)
    return hs, zs


def backward(hs, zs, q, wi, wo):
    n_layers = len(wi)
    s_in, s_out = [None] * n_layers, [None] * n_layers
    for layer in reversed(range(n_layers)):
        a, vjp = jax.vjp(gelu_tanh, zs[layer].astype(F32))
        s_out[layer] = dot(a.astype(BF), q, ((0,), (0,)))
        p = vjp(dot(q, wo[layer], ((1,), (1,))))[0].astype(BF)
        s_in[layer] = dot(hs[layer], p, ((0,), (0,)))
        if layer:
            q = (q.astype(F32) + dot(p, wi[layer], ((1,), (1,)))).astype(BF)
    return s_in, s_out


def solution(mesh):
    n_dev = mesh.shape["data"]

    def local_step(x_loc, y_loc, w_in, w_out):
        n_layers, d_model, d_ff = w_in.shape
        tok = 1.0 / (x_loc.shape[0] * n_dev * x_loc.shape[1] * d_model)
        rho = RHO_FRAC * math.sqrt(n_layers * (d_model + d_ff))
        x = x_loc.reshape(-1, d_model)
        y = y_loc.reshape(-1, d_model)
        sink = lax.rem(lax.axis_index("data") // 8, 3) == 0

        def one_pass(wi, wo, cid):
            hs, zs = forward(x, wi, wo)
            err = hs[-1].astype(F32) - y.astype(F32)
            s_in, s_out = backward(hs, zs, err.astype(BF), wi, wo)
            own_o, own_i = rs_only(jnp.stack(s_out), jnp.stack(s_in), lags=(1, 4, 4, 4), nsl=14, ns=4, cid=cid)
            return own_o, own_i, jnp.sum(err * err)

        wi = [w_in[k].astype(BF) for k in range(n_layers)]
        wo = [w_out[k].astype(BF) for k in range(n_layers)]
        own_o, own_i, _ = one_pass(wi, wo, 1)
        go, gi = own_o * tok, own_i * tok
        part = jnp.sum(go * go) + jnp.sum(gi * gi)
        sq = lax.psum(jnp.where(sink, part, 0.0), "data")
        coef = rho / jnp.sqrt(sq)
        sc = jnp.stack([coef, jnp.float32(tok)])
        vo, vi = ag_call(sc, own_o, own_i, w_out, w_in, BF, (0, 1), cid=2)
        wi = [vi[k] for k in range(n_layers)]
        wo = [vo[k] for k in range(n_layers)]
        own_o, own_i, sq2 = one_pass(wi, wo, 3)
        sc = jnp.array([-LEARN_RATE, tok], F32)
        new_out, new_in = ag_call(sc, own_o, own_i, w_out, w_in, F32, (0, 1), cid=4)
        loss = 0.5 * (lax.psum(sq2, "data") * tok)
        return new_in, new_out, loss

    return jax.shard_map(local_step, mesh=mesh, in_specs=(P("data"), P("data"), P(), P()), out_specs=(P(), P(), P()), check_vma=False)
```

```python
import functools
import math

import jax
import jax.numpy as jnp
from jax import lax
from jax.experimental import pallas as pl
from jax.experimental.pallas import tpu as pltpu
from jax.sharding import PartitionSpec as P

MESH = pl.DeviceIdType.MESH
F32, BF = jnp.float32, jnp.bfloat16
RHO_FRAC = 0.1
LEARN_RATE = 1.0
D = 512
BLK = 256
PC = 16
RT = 784
BT = 1568
UNITS = 4
SUB, LANE = 8, 128
NZ = 4
HALF = 0.5
MIB = 2**20
GELU_A = math.sqrt(2.0 / math.pi)
GELU_B = 0.044715
TWO = AB = TYPES = DIRS = (0, 1)
SHAPES = ((BLK, D), (D, BLK))
ANY = pl.BlockSpec(memory_space=pl.ANY)
HBM = pl.BlockSpec(memory_space=pltpu.HBM)
VM = pl.BlockSpec(memory_space=pltpu.VMEM)
DMA = pltpu.SemaphoreType.DMA
rem = lax.rem
when = pl.when


def both(*conds):
    return functools.reduce(jnp.logical_and, conds)


def ds(start, size):
    return pl.ds(pl.multiple_of(start, SUB), size)


def cols(f):
    return pl.ds(pl.multiple_of(f * BLK, BLK), BLK)


def dg(a, b, ca, cb):
    return lax.dot_general(a, b, (((ca,), (cb,)), ((), ())), preferred_element_type=F32)


def scratch(dtype, *shape):
    return pltpu.VMEM(shape, dtype)


def local(src, dst, sem):
    return pltpu.make_async_copy(src, dst, sem)


def start(copies):
    for c in copies:
        c.start()


def wait(copies):
    for c in copies:
        c.wait()


class Geo:
    def __init__(self):
        me = lax.axis_index("data")
        flip = lambda step: me + step - 2 * step * rem(me // step, 2)
        self.me = me
        self.c, self.x, self.y, self.z = [rem(me // step, n) for step, n in ((1, 2), (2, 2), (4, 2), (8, NZ))]
        self.partner, self.xn, self.yn, self.z1, self.z2 = [flip(1 << k) for k in range(5)]
        self.zm, self.zp = me - 8, me + 8
        self.e = self.z // (NZ - 1)
        self.sink = rem(self.z, NZ - 1) == 0
        self.far = me + 24 - 48 * self.e
        self.w = (self.x, self.y)
        self.w2 = (self.y, self.x)
        self.n1 = (self.xn, self.yn)
        self.n2 = (self.yn, self.xn)

    def place(self, dirn):
        return self.z if dirn else NZ - 1 - self.z

    def enter(self, far=False, z2=False):
        bar = pltpu.get_barrier_semaphore()
        greet = lambda dev: pl.semaphore_signal(bar, device_id=(dev,), device_id_type=MESH)
        peers = [self.partner, self.xn, self.yn] + ([self.z2] if z2 else [])
        for dev in peers:
            greet(dev)
        when(self.z > 0)(lambda: greet(self.zm))
        when(self.z < NZ - 1)(lambda: greet(self.zp))
        if far:
            when(self.sink)(lambda: greet(self.far))
        n = len(peers) + 1
        when(self.sink)(lambda: pl.semaphore_wait(bar, n + int(far)))
        when(jnp.logical_not(self.sink))(lambda: pl.semaphore_wait(bar, n + 1))

    def half(self, T, c):
        R = SHAPES[T][0]
        return ds(c * (R // 2), R // 2)

    def part(self, T, ab, w):
        R = SHAPES[T][0]
        return self.c * (R // 2) + ab * (R // 4) + w * (R // 8)

    def zrow(self, T, ab, e):
        return self.part(T, ab, self.w[ab]) + e * (SHAPES[T][0] // 16)

    def fin(self, T, ab, mine):
        row = self.zrow(T, ab, self.e)
        w = self.w2[ab] if mine else 1 - self.w2[ab]
        if T:
            return ds(row + w * PC, PC), slice(None)
        return ds(row, PC), cols(w)


def region(out, T, li, f, rows, col=None):
    if T:
        return out[T].at[li, rows, cols(f)]
    return out[T].at[li, ds(f * BLK + rows.start, rows.size), slice(None) if col is None else col]


def schedule(s, j, lag, T):
    d = j - T - lag
    return None if d % 2 else s + d // 2


def run(k, n, what, T, *more):
    if k is not None:
        when(both(k >= 0, k < n))(functools.partial(what, T, k, *more))


class Scatter:
    FLOWS = FD, F1, F3, FM, FP = range(0, 10, 2)
    CREDITS = CD, C1, C3, CM, CP = range(0, 10, 2)

    def __init__(self, g, n, ns, nsl, lags, bufs, deliver):
        self.g, self.n, self.ns, self.nsl, self.deliver = g, n, ns, nsl, deliver
        self.S, self.rD, self.r1, self.rz, self.r3 = [bufs[2 * i : 2 * i + 2] for i in range(5)]
        self.ssem, self.rsem, self.cred = bufs[10:]
        ld, l1, self.lz, l3 = lags
        self.lam1 = ld
        self.lam2 = ld + l1
        self.lam4 = self.lam2 + (NZ - 1) * self.lz + l3

    @staticmethod
    def scratch(ns, nsl):
        out = []
        for lead, div, div2 in (((nsl,), 1, 1), ((ns,), 2, 1), ((ns, 2), 8, 1), ((ns, 2, 2), 16, 1), ((ns, 2), 0, 0)):
            for R, C in SHAPES:
                out.append(scratch(F32, *lead, *((R // div, C) if div else (PC, BLK))))
        return out + [DMA((2, 10, ns))] * 2 + [pltpu.SemaphoreType.REGULAR((2, 10))]

    def copy(self, T, flow, k, src, dst, dev):
        i = (T, flow, rem(k, self.ns))
        return pltpu.make_async_remote_copy(src, dst, self.ssem.at[i], self.rsem.at[i], device_id=(dev,), device_id_type=MESH)

    def take(self, T, credit, k):
        when(k >= self.ns)(lambda: pl.semaphore_wait(self.cred.at[T, credit]))

    def give(self, T, credit, k, dev):
        when(k + self.ns < self.n)(lambda: pl.semaphore_signal(self.cred.at[T, credit], device_id=(dev,), device_id_type=MESH))

    def slots(self, k):
        return rem(k, self.nsl), rem(k, self.ns)

    def to_core(self, T, k):
        s, q = self.slots(k)
        return self.copy(T, self.FD, k, self.S[T].at[s, self.g.half(T, 1 - self.g.c)], self.rD[T].at[q], self.g.partner)

    def first(self, T, k, ab):
        s, q = self.slots(k)
        rows = ds(self.g.part(T, ab, 1 - self.g.w[ab]), SHAPES[T][0] // 8)
        return self.copy(T, self.F1 + ab, k, self.S[T].at[s, rows], self.r1[T].at[q, ab], self.g.n1[ab])

    def zrows(self, T, ab, e):
        return ds(self.g.zrow(T, ab, e), SHAPES[T][0] // 16)

    def along(self, T, k, dirn, ab):
        s, q = self.slots(k)
        flow = (self.FP if dirn else self.FM) + ab
        src = self.S[T].at[s, self.zrows(T, ab, dirn)]
        return self.copy(T, flow, k, src, self.rz[T].at[q, ab, dirn], self.g.zp if dirn else self.g.zm)

    def last(self, T, k, ab):
        s, q = self.slots(k)
        return self.copy(T, self.F3 + ab, k, self.S[T].at[(s, *self.g.fin(T, ab, False))], self.r3[T].at[q, ab], self.g.n2[ab])

    def add(self, T, k, rows, val):
        s, _ = self.slots(k)
        self.S[T][s, rows] = self.S[T][s, rows] + val

    def begin(self, T, k):
        self.take(T, self.CD, k)
        self.to_core(T, k).start()

    def after_core(self, T, k):
        g = self.g
        self.to_core(T, k).wait()
        self.add(T, k, g.half(T, g.c), self.rD[T][rem(k, self.ns)])
        self.give(T, self.CD, k, g.partner)
        for ab in AB:
            self.take(T, self.C1 + ab, k)
            self.first(T, k, ab).start()

    def after_first(self, T, k):
        g = self.g
        for ab in AB:
            self.first(T, k, ab).wait()
        for ab in AB:
            self.add(T, k, ds(g.part(T, ab, g.w[ab]), SHAPES[T][0] // 8), self.r1[T][rem(k, self.ns), ab])
            self.give(T, self.C1 + ab, k, g.n1[ab])

    def line(self, T, k, dirn):
        g = self.g
        p = g.place(dirn)
        credit = self.CP if dirn else self.CM

        @when(k < self.n)
        def _():
            @when(p > 0)
            def _():
                for ab in AB:
                    self.along(T, k, dirn, ab).wait_recv()
                for ab in AB:
                    self.add(T, k, self.zrows(T, ab, dirn), self.rz[T][rem(k, self.ns), ab, dirn])
                self.give(T, credit, k, g.zm if dirn else g.zp)

            @when(p < NZ - 1)
            def _():
                self.take(T, credit, k)
                for ab in AB:
                    self.along(T, k, dirn, ab).start()

            @when(p == NZ - 1)
            def _():
                for ab in AB:
                    self.take(T, self.C3 + ab, k)
                    self.last(T, k, ab).start()

        @when(both(k > 0, p < NZ - 1))
        def _():
            for ab in AB:
                self.along(T, k - 1, dirn, ab).wait_send()

    def after_last(self, T, k):
        g = self.g

        @when(g.sink)
        def _():
            s, q = self.slots(k)
            for ab in AB:
                self.last(T, k, ab).wait()
            for ab in AB:
                self.deliver(T, k, ab, self.S[T][(s, *g.fin(T, ab, True))] + self.r3[T][q, ab])
                self.give(T, self.C3 + ab, k, g.n2[ab])

    def due(self, s, j):
        for T in TYPES:
            run(schedule(s, j, self.lam4, T), self.n, self.after_last, T)
        for T in TYPES:
            k = schedule(s, j, self.lam2, T)
            run(k, self.n, self.after_first, T)
            if k is not None:
                for dirn in DIRS:
                    run(k - self.g.place(dirn) * (self.lz // 2), self.n + 1, self.line, T, dirn)
        for T in TYPES:
            run(schedule(s, j, self.lam1, T), self.n, self.after_core, T)

    def steps(self):
        return self.n + (self.lam4 + 1) // 2 + 1


class Gather:
    FLOWS = F3, FM, FP, FE0, FE1, FD = range(6)

    def __init__(self, g, n, nf, layer, lags, own, out, sems, start=0):
        self.g, self.n, self.nf, self.layer, self.own, self.out = g, n, nf, layer, own, out
        self.ssem, self.rsem, self.lsem = sems
        self.ns = self.ssem.shape[-1]
        l3, self.lz, le, ld = lags
        self.mu0 = start
        self.mu1 = start + l3
        self.mu2 = self.mu1 + (NZ - 1) * self.lz + le
        self.mu3 = self.mu2 + ld

    @staticmethod
    def scratch(n, ns):
        return [DMA((2, 6, ns)), DMA((2, 6, n)), DMA((2, 2, ns))]

    def region(self, T, k, rows, col=None):
        return region(self.out, T, self.layer(k // self.nf), rem(k, self.nf), rows, col)

    def rows(self, T, k, row, div):
        return self.region(T, k, ds(row, SHAPES[T][0] // div))

    def copy(self, T, flow, k, src, dst, dev):
        return pltpu.make_async_remote_copy(src, dst, self.ssem.at[T, flow, rem(k, self.ns)], self.rsem.at[T, flow, k],
            device_id=(dev,), device_id_type=MESH)

    def keep(self, T, k, ab):
        rows, col = self.g.fin(T, ab, True)
        return local(self.own[T].at[k, ab], self.region(T, k, rows, col), self.lsem.at[T, ab, rem(k, self.ns)])

    def begin(self, T, k):
        g = self.g

        @when(g.sink)
        def _():
            for ab in AB:
                rows, col = g.fin(T, ab, True)
                self.keep(T, k, ab).start()
                self.copy(T, self.F3, k, self.own[T].at[k, ab], self.region(T, k, rows, col), g.n2[ab]).start()

    def over(self, T, flow, k, ref, send=True, recv=True):
        if send:
            local(ref, ref, self.ssem.at[T, flow, rem(k, self.ns)]).wait()
        if recv:
            local(ref, ref, self.rsem.at[T, flow, k]).wait()

    def line(self, T, k, dirn):
        g = self.g
        p = g.place(dirn)
        e = 1 - dirn
        flow = self.FP if dirn else self.FM
        pair = lambda k: self.rows(T, k, 0, 8)

        @when(k < self.n)
        def _():
            @when(p == 0)
            def _():
                for ab in AB:
                    self.keep(T, k, ab).wait()
                self.over(T, self.F3, k, self.own[T].at[k])

            when(p > 0)(lambda: self.over(T, flow, k, pair(k), send=False))
            parts = [self.rows(T, k, g.zrow(T, ab, e), 16) for ab in AB]

            @when(p < NZ - 1)
            def _():
                for r in parts:
                    self.copy(T, flow, k, r, r, g.zp if dirn else g.zm).start()

            for ab in AB:
                self.copy(T, self.FE0 + e, k, parts[ab], parts[ab], g.n1[ab]).start()

        when(both(k > 0, p < NZ - 1))(lambda: self.over(T, flow, k - 1, pair(k - 1), recv=False))

    def to_core(self, T, k):
        r = self.region(T, k, self.g.half(T, self.g.c))
        return self.copy(T, self.FD, k, r, r, self.g.partner)

    def after_first(self, T, k):
        for e in TWO:
            self.over(T, self.FE0 + e, k, self.rows(T, k, 0, 8))
        self.to_core(T, k).start()

    def done(self, T, k):
        self.to_core(T, k).wait()

    def due(self, s, j):
        for T in TYPES:
            run(schedule(s, j, self.mu0, T), self.n, self.begin, T)
        for T in TYPES:
            k = schedule(s, j, self.mu1, T)
            if k is not None:
                for dirn in DIRS:
                    run(k - self.g.place(dirn) * (self.lz // 2), self.n + 1, self.line, T, dirn)
        for T in TYPES:
            run(schedule(s, j, self.mu2, T), self.n, self.after_first, T)
            run(schedule(s, j, self.mu3, T), self.n, self.done, T)

    def steps(self):
        return self.n + (self.mu3 + 1) // 2 + 1


class PairSum:
    GAP = 3

    def __init__(self, devs, bufs):
        self.devs = devs
        self.part, self.nbr, self.ssem, self.rsem = bufs

    @staticmethod
    def scratch(n):
        return [scratch(F32, n + 1, SUB, LANE), scratch(F32, n, SUB, LANE), DMA((n,)), DMA((n,))]

    def copy(self, r):
        return pltpu.make_async_remote_copy(self.part.at[r], self.nbr.at[r], self.ssem.at[r], self.rsem.at[r],
            device_id=(self.devs[r],), device_id_type=MESH)

    def finish(self, r):
        self.copy(r).wait()
        self.part[r + 1] = self.part[r] + self.nbr[r]

    def due(self, s):
        for r in range(len(self.devs)):
            when(s == r * self.GAP)(lambda: self.copy(r).start())
            when(s == r * self.GAP + self.GAP - 1)(lambda: self.finish(r))

    def now(self):
        for r in range(len(self.devs)):
            self.copy(r).start()
            self.finish(r)


def gelu(z):
    half = HALF * z
    return half + half * jnp.tanh(z * (GELU_A + (GELU_A * GELU_B) * (z * z)))


def gelu_parts(z):
    zz = z * z
    t = jnp.tanh(z * (GELU_A + (GELU_A * GELU_B) * zz))
    half = HALF * z
    slope = (HALF + HALF * t) + half * ((1 - t * t) * (GELU_A + (3 * GELU_A * GELU_B) * zz))
    return half + half * t, slope


class Forward:
    def __init__(self, nl, tok, hbm, outs, bufs):
        self.nl, self.nt = nl, tok // RT
        self.x, self.y = hbm
        self.h_o, self.z_o, self.q_o, self.loss = outs
        self.h, self.yb, self.a, self.zt, self.wi, self.wo, self.hsem, self.zsem, self.ysem = bufs
        self.dff = self.a.shape[1]

    @staticmethod
    def scratch(tok, dff):
        return [scratch(BF, tok, D), scratch(BF, tok, D), scratch(BF, RT, dff), scratch(BF, 2, RT, dff),
                scratch(BF, 2, D, dff), scratch(BF, 2, dff, D), DMA((tok // RT,)), DMA((2, 2)), DMA((2,))]

    def h_copy(self, r, dst):
        rows = ds(r * RT, RT)
        return local(self.h.at[rows], dst.at[rows], self.hsem.at[r])

    def prologue(self):
        self.cy = local(self.y, self.yb, self.ysem.at[1])
        cx = local(self.x, self.h, self.ysem.at[0])
        cx.start()
        self.cy.start()
        self.loss[...] = jnp.zeros_like(self.loss)
        cx.wait()
        for r in range(self.nt):
            self.h_copy(r, self.h_o.at[0]).start()

    def z_copy(self, li, r, i, slot):
        c = pl.ds(i * (self.dff // 2), self.dff // 2)
        return local(self.zt.at[slot, :, c], self.z_o.at[li, ds(r * RT, RT), c], self.zsem.at[slot, i])

    def z_unit(self, li, r, w, i):
        slot = rem(li * self.nt + r, 2)
        when(li * self.nt + r > 1)(lambda: self.z_copy(0, 0, i, slot).wait())
        h = self.h[ds(r * RT, RT)]
        per = self.dff // D // 2
        for b in range(i * per, i * per + per):
            c = pl.ds(b * D, D)
            z = dg(h, self.wi[w, :, c], 1, 0).astype(BF)
            self.zt[slot, :, c] = z
            self.a[:, c] = gelu(z.astype(F32)).astype(BF)
        self.z_copy(li, r, i, slot).start()

    def h_unit(self, li, r, w, i):
        rows, c = ds(r * RT, RT), pl.ds(i * BLK, BLK)
        hn = (self.h[rows, c].astype(F32) + dg(self.a[...], self.wo[w, :, c], 1, 0)).astype(BF)
        if i == 0:
            self.h_copy(r, self.h_o.at[0]).wait()

        @when(li < self.nl - 1)
        def _():
            self.h[rows, c] = hn
            if i:
                self.h_copy(r, self.h_o.at[li + 1]).start()

        @when(li == self.nl - 1)
        def _():
            if i == 0:
                when(r == 0)(self.cy.wait)
            err = hn.astype(F32) - self.yb[rows, c].astype(F32)
            self.h[rows, c] = err.astype(BF)
            if i:
                self.h_copy(r, self.q_o).start()
            sq = jnp.sum((err * err).reshape(RT // SUB, SUB, BLK), axis=0)
            for b in range(BLK // LANE):
                self.loss[...] += sq[:, b * LANE : (b + 1) * LANE]

    def unit(self, k):
        return functools.partial(self.h_unit if k // 2 else self.z_unit, i=k % 2)

    def epilogue(self):
        for slot in TWO:
            for i in TWO:
                self.z_copy(0, 0, i, slot).wait()
        for r in range(self.nt):
            self.h_copy(r, self.q_o).wait()

    @staticmethod
    def shapes(nl, tok, dff):
        S = jax.ShapeDtypeStruct
        return [S((nl, tok, D), BF), S((nl, tok, dff), BF), S((tok, D), BF), S((SUB, LANE), F32)]


def forward_kernel(nl, tok, x, y, w_out, w_in, h_o, z_o, q_o, loss, wi32, wo32, wsem, *bufs):
    fw = Forward(nl, tok, (x, y), (h_o, z_o, q_o, loss), bufs)
    shares = [(ds(r * (m.shape[1] // fw.nt), m.shape[1] // fw.nt), m, v, w) for m, v, w in ((w_in, wi32, fw.wi), (w_out, wo32, fw.wo)) for r in range(fw.nt)]

    def loads(li, r):
        return [local(m.at[li, rows], v.at[rows], wsem.at[r, i]) for i, (rows, m, v, _) in enumerate(shares[r :: fw.nt])]

    def take(li, r, last):
        if not last:
            wait(loads(li, r))
        for rows, _, v, w in shares[r :: fw.nt]:
            w[rem(li, 2), rows] = v[rows].astype(BF)
        when(li + 1 < nl)(lambda: start(loads(li + 1, r)))

    for r in range(fw.nt):
        start(loads(0, r))
    fw.prologue()
    for r in range(fw.nt):
        take(0, r, False)

    def body(li, _):
        for r in range(fw.nt):
            when(li + 1 < nl)(lambda: wait(loads(li + 1, r)))
            take(li + 1, r, True)
            for k in range(UNITS):
                fw.unit(k)(li, r, rem(li, 2))
        return 0

    lax.fori_loop(0, nl, body, 0)
    fw.epilogue()


def forward(x, y, w_out, w_in):
    nl, dff, _ = w_out.shape
    tok = x.shape[0]
    return pl.pallas_call(
        functools.partial(forward_kernel, nl, tok),
        out_shape=Forward.shapes(nl, tok, dff),
        in_specs=[HBM] * 4,
        out_specs=[HBM] * 3 + [VM],
        scratch_shapes=[scratch(F32, D, dff), scratch(F32, dff, D), DMA((tok // RT, 2))] + Forward.scratch(tok, dff),
        compiler_params=pltpu.CompilerParams(vmem_limit_bytes=56 * MIB),
        name="forward",
    )(x, y, w_out, w_in)


def gather_forward_kernel(nl, tok, lags, pe_o, pe_i, x, y, wo_o, wi_o, h_o, z_o, q_o, loss, own_o, own_i, wsem, *bufs):
    g = Geo()
    n = pe_o.shape[0]
    nf = n // nl
    ga = Gather(g, n, nf, lambda q: q, lags, (own_o, own_i), (wo_o, wi_o), bufs[:3])
    fw = Forward(nl, tok, (x, y), (h_o, z_o, q_o, loss), bufs[3:])
    pieces = [local(src, dst, wsem.at[i]) for i, (src, dst) in enumerate(((pe_o, own_o), (pe_i, own_i)))]
    start(pieces)
    loads = lambda li: [local(wi_o.at[li], fw.wi.at[rem(li, 2)], wsem.at[0]), local(wo_o.at[li], fw.wo.at[rem(li, 2)], wsem.at[1])]
    fw.prologue()
    g.enter()
    wait(pieces)
    lead = (ga.mu3 + 1) // 2 + nf

    def body(s, _):
        ga.due(s, 0)
        u = s - lead
        up = jnp.maximum(u, 0)
        li, i = up // nf, rem(up, nf)

        @when(both(u >= 0, i == 0))
        def _():
            wait(loads(li))

        for k in range(UNITS):
            when(both(u >= 0, i < fw.nt * UNITS, rem(i, UNITS) == k))(lambda: fw.unit(k)(li, i // UNITS, rem(li, 2)))
        ga.due(s, 1)

        @when(both(u + 1 >= 0, rem(u + 1 + n, nf) == 0, u + 1 < n))
        def _():
            start(loads((u + 1) // nf))

        return 0

    lax.fori_loop(0, lead + n, body, 0)
    fw.epilogue()


def gather_forward(pe_o, pe_i, x, y, nl, ns=4, lags=(4, 4, 4, 2), cid=2):
    n, tok = pe_o.shape[0], x.shape[0]
    dff = n // nl * BLK
    S = jax.ShapeDtypeStruct
    return pl.pallas_call(
        functools.partial(gather_forward_kernel, nl, tok, lags),
        out_shape=[S((nl, dff, D), BF), S((nl, D, dff), BF)] + Forward.shapes(nl, tok, dff),
        in_specs=[HBM] * 4,
        out_specs=[HBM] * 5 + [VM],
        scratch_shapes=[scratch(BF, n, 2, PC, BLK)] * 2 + [DMA((2,))] + Gather.scratch(n, ns) + Forward.scratch(tok, dff),
        cost_estimate=pl.CostEstimate(flops=tok * D * dff * nl * 4, bytes_accessed=60 * MIB, transcendentals=0),
        compiler_params=pltpu.CompilerParams(collective_id=cid, has_side_effects=True, vmem_limit_bytes=48 * MIB),
        name="gather_forward",
    )(pe_o, pe_i, x, y)


class Backward:
    def __init__(self, nl, tok, hbm, bufs):
        self.nl, self.tok = nl, tok
        self.q_h, self.h_h, self.z_h, self.wo_h, self.wi_h = hbm
        self.q, self.h, self.z, self.wo, self.wi, self.a, self.p, self.acc, self.sem = bufs
        self.nf = self.z_h.shape[-1] // BLK
        self.n = nl * self.nf

    @staticmethod
    def scratch(tok, wdt):
        return [scratch(BF, tok, D), scratch(BF, 2, tok, D), scratch(BF, 2, tok, BLK), scratch(wdt, 2, BLK, D), scratch(wdt, 2, D, BLK),
                scratch(BF, tok, BLK), scratch(BF, tok, BLK), scratch(F32, tok, D), DMA((5, 2))]

    def at(self, s):
        return self.nl - 1 - s // self.nf, rem(s, self.nf), rem(s, 2)

    def load_h(self, li):
        i = rem(li, 2)
        return local(self.h_h.at[li], self.h.at[i], self.sem.at[0, i])

    def loads(self, s):
        li, f, b = self.at(s)
        return [local(src, dst.at[b], self.sem.at[i + 1, b]) for i, (src, dst) in enumerate((
            (self.z_h.at[li, :, cols(f)], self.z), (self.wo_h.at[li, cols(f)], self.wo), (self.wi_h.at[li, :, cols(f)], self.wi)))]

    def prologue(self):
        cq = local(self.q_h, self.q, self.sem.at[4, 0])
        for c in [cq, *self.loads(0), self.load_h(self.nl - 1)]:
            c.start()
        cq.wait()
        self.acc[...] = self.q[...].astype(F32)

    def tiles(self):
        return [pl.ds(r * BT, BT) for r in range(self.tok // BT)]

    def out_block(self, s, dst):
        li, f, b = self.at(s)
        wait(self.loads(s))

        @when(s + 1 < self.n)
        def _():
            start(self.loads(s + 1))

        @when(f == 0)
        def _():
            self.load_h(li).wait()
            when(li > 0)(lambda: self.load_h(li - 1).start())

        wo = self.wo[b].astype(BF)
        for rows in self.tiles():
            a, slope = gelu_parts(self.z[b, rows].astype(F32))
            self.a[rows] = a.astype(BF)
            self.p[rows] = (dg(self.q[rows], wo, 1, 1) * slope).astype(BF)
        dst[...] = dg(self.a[...], self.q[...], 0, 0)

    def in_block(self, s, dst):
        li, f, b = self.at(s)
        dst[...] = dg(self.h[rem(li, 2)], self.p[...], 0, 0)

        @when(li > 0)
        def _():
            wi = self.wi[b].astype(BF)
            for rows in self.tiles():
                self.acc[rows] = self.acc[rows] + dg(self.p[rows], wi, 1, 1)

            @when(f == self.nf - 1)
            def _():
                for rows in self.tiles():
                    q = self.acc[rows].astype(BF)
                    self.q[rows] = q
                    self.acc[rows] = q.astype(F32)


def load_owned(g, n, nf, layer, mats, dst, sem):
    def issue(k, _):
        for T in TYPES:
            for ab in AB:
                rows, col = g.fin(T, ab, True)
                local(region(mats, T, layer(k // nf), rem(k, nf), rows, col), dst[T].at[k, ab], sem.at[T]).start()
        return 0

    lax.fori_loop(0, n, issue, 0)


def wait_owned(dst, sem):
    for T in TYPES:
        local(dst[T], dst[T], sem.at[T]).wait()


def backward_kernel(nl, tok, ns, nsl, lags, glags, norm, scale, coef, *refs):
    q_h, h_h, z_h, wo_h, wi_h, refs = *refs[:5], refs[5:]
    if norm:
        mats = wo_h, wi_h
    else:
        mats, tile, refs = refs[:2], refs[2], refs[3:]
    bw_hbm = q_h, h_h, z_h, wo_h, wi_h
    n = nl * (z_h.shape[-1] // BLK)
    nf = n // nl
    last_first = lambda q: nl - 1 - q
    out, refs = refs[:2], refs[2:]
    if not norm:
        loss, refs = refs[0], refs[1:]
    n_sc = len(Scatter.scratch(ns, nsl))
    sc_bufs, refs = refs[:n_sc], refs[n_sc:]
    bw, refs = Backward(nl, tok, bw_hbm, refs[:9]), refs[9:]
    w_p, wsem, refs = refs[:2], refs[2], refs[3:]
    g = Geo()
    bw.prologue()
    when(g.sink)(lambda: load_owned(g, n, nf, last_first, mats, w_p, wsem))
    if norm:
        own, pieces, sq, pair = refs[:2], refs[2:4], refs[4], refs[5:]
        ps = PairSum((g.partner, g.xn, g.yn, g.far), pair)
        sq[...] = jnp.zeros_like(sq)
    else:
        ps = PairSum((g.partner, g.xn, g.yn, g.z1, g.z2), refs[:4])
        ps.part[0] = tile[...]

    def deliver(T, k, ab, val):
        val = val * scale
        if norm:
            own[T][k, ab] = val
            sq[...] += val * val
        else:
            w_p[T][k, ab] = w_p[T][k, ab] - coef * val

    g.enter(far=norm, z2=not norm)
    sc = Scatter(g, n, ns, nsl, lags, sc_bufs, deliver)
    steps = sc.steps()
    if not norm:
        ga = Gather(g, n, nf, last_first, glags, w_p, out, refs[4:], sc.lam4 + 1)
        steps = ga.steps()

    def body(s, _):
        when(both(s == 1, g.sink))(lambda: wait_owned(w_p, wsem))
        for j, block in enumerate((bw.out_block, bw.in_block)):

            @when(s < n)
            def _():
                block(s, sc.S[j].at[rem(s, nsl)])
                sc.begin(j, s)

            sc.due(s, j)
            if not norm:
                ga.due(s, j)
        if not norm:
            ps.due(s)
        return 0

    lax.fori_loop(0, steps, body, 0)
    if not norm:
        loss[...] = ps.part[5]
        return

    @when(g.sink)
    def _():
        quarters = [sq[i * SUB : (i + 1) * SUB, j * LANE : (j + 1) * LANE] for i in TWO for j in TWO]
        ps.part[0] = sum(quarters[1:], quarters[0])
        ps.now()
        step = coef / jnp.sqrt(jnp.broadcast_to(jnp.sum(ps.part[4]), (1, 1)))

        def piece(k, _):
            to = (nl - 1 - k // nf) * nf + rem(k, nf)
            for T in TYPES:
                pieces[T][to] = (w_p[T][k] + step * own[T][k]).astype(BF)
            return 0

        lax.fori_loop(0, n, piece, 0)
        copies = [local(pieces[T], out[T], wsem.at[T]) for T in TYPES]
        start(copies)
        wait(copies)


def backward(q, h, z, wo, wi, scale, coef, new=None, ns=4, nsl=10, lags=(1, 4, 2, 4), glags=(4, 4, 4, 2), cid=1):
    nl, tok, dff = z.shape
    n = nl * dff // BLK
    norm = new is None
    S = jax.ShapeDtypeStruct
    piece = lambda dt: scratch(dt, n, 2, PC, BLK)
    scr = Scatter.scratch(ns, nsl) + Backward.scratch(tok, wo.dtype) + [piece(F32)] * 2 + [DMA((2,))]
    if norm:
        scr += [piece(F32)] * 2 + [piece(BF)] * 2 + [scratch(F32, PC, BLK)] + PairSum.scratch(4)
        outs, specs, more = [S((n, 2, PC, BLK), BF)] * 2, [HBM] * 2, ()
    else:
        scr += PairSum.scratch(5) + Gather.scratch(n, ns)
        outs, specs, more = [S(new[0].shape, F32), S(new[1].shape, F32), S((SUB, LANE), F32)], [HBM] * 2 + [VM], new
    return pl.pallas_call(
        functools.partial(backward_kernel, nl, tok, ns, nsl, lags, glags, norm, scale, coef),
        out_shape=outs,
        in_specs=[HBM] * 5 + [HBM, HBM, VM][: len(more)],
        out_specs=specs,
        scratch_shapes=scr,
        cost_estimate=pl.CostEstimate(flops=tok * D * dff * nl * 8, bytes_accessed=60 * MIB, transcendentals=0),
        compiler_params=pltpu.CompilerParams(collective_id=cid, has_side_effects=True, vmem_limit_bytes=56 * MIB),
        name="backward_norm" if norm else "backward_update",
    )(q, h, z, wo, wi, *more)


def solution(mesh):
    n_dev = mesh.shape["data"]

    def local_step(x_loc, y_loc, w_in, w_out):
        nl, d_model, d_ff = w_in.shape
        scale = 1.0 / (x_loc.shape[0] * n_dev * x_loc.shape[1] * d_model)
        rho = RHO_FRAC * math.sqrt(nl * (d_model + d_ff))
        x, y = [v.reshape(-1, d_model) for v in (x_loc, y_loc)]
        h, z, q, _ = forward(x, y, w_out, w_in)
        pieces = backward(q, h, z, w_out, w_in, scale, rho, cid=1)
        wo, wi, h, z, q, tile = gather_forward(*pieces, x, y, nl, cid=2)
        new_out, new_in, tile = backward(q, h, z, wo, wi, scale, LEARN_RATE, (w_out, w_in, tile), cid=3)
        return new_in, new_out, HALF * (jnp.sum(tile) * scale)

    specs = P("data"), P("data"), P(), P()
    return jax.shard_map(local_step, mesh=mesh, in_specs=specs, out_specs=(P(), P(), P()), check_vma=False)
```

```python
import functools
import math

import jax
import jax.numpy as jnp
from jax import lax
from jax.experimental import pallas as pl
from jax.experimental.pallas import tpu as pltpu
from jax.sharding import PartitionSpec as P

MESH = pl.DeviceIdType.MESH
F32, BF = jnp.float32, jnp.bfloat16
RHO_FRAC = 0.1
LEARN_RATE = 1.0
D = 512
BLK = 256
PC = 16
FT = 224
BT = 1568
SUB, LANE = 8, 128
NZ = 4
HALF = 0.5
MIB = 2**20
GELU_A = math.sqrt(2.0 / math.pi)
GELU_B = 0.044715
TWO = AB = TYPES = DIRS = (0, 1)
SHAPES = ((BLK, D), (D, BLK))
ANY = pl.BlockSpec(memory_space=pl.ANY)
HBM = pl.BlockSpec(memory_space=pltpu.HBM)
VM = pl.BlockSpec(memory_space=pltpu.VMEM)
DMA = pltpu.SemaphoreType.DMA
rem = lax.rem
when = pl.when


def both(*conds):
    return functools.reduce(jnp.logical_and, conds)


def ds(start, size):
    return pl.ds(pl.multiple_of(start, SUB), size)


def cols(f):
    return pl.ds(pl.multiple_of(f * BLK, BLK), BLK)


def dg(a, b, ca, cb):
    return lax.dot_general(a, b, (((ca,), (cb,)), ((), ())), preferred_element_type=F32)


def scratch(dtype, *shape):
    return pltpu.VMEM(shape, dtype)


def local(src, dst, sem):
    return pltpu.make_async_copy(src, dst, sem)


def start(copies):
    for c in copies:
        c.start()


def wait(copies):
    for c in copies:
        c.wait()


class Geo:
    def __init__(self):
        me = lax.axis_index("data")
        flip = lambda step: me + step - 2 * step * rem(me // step, 2)
        self.me = me
        self.c, self.x, self.y, self.z = [rem(me // step, n) for step, n in ((1, 2), (2, 2), (4, 2), (8, NZ))]
        self.partner, self.xn, self.yn, self.z1, self.z2 = [flip(1 << k) for k in range(5)]
        self.zm, self.zp = me - 8, me + 8
        self.e = self.z // (NZ - 1)
        self.sink = rem(self.z, NZ - 1) == 0
        self.far = me + 24 - 48 * self.e
        self.w = (self.x, self.y)
        self.w2 = (self.y, self.x)
        self.n1 = (self.xn, self.yn)
        self.n2 = (self.yn, self.xn)

    def place(self, dirn):
        return self.z if dirn else NZ - 1 - self.z

    def enter(self, far=False, z2=False):
        bar = pltpu.get_barrier_semaphore()
        greet = lambda dev: pl.semaphore_signal(bar, device_id=(dev,), device_id_type=MESH)
        peers = [self.partner, self.xn, self.yn] + ([self.z2] if z2 else [])
        for dev in peers:
            greet(dev)
        when(self.z > 0)(lambda: greet(self.zm))
        when(self.z < NZ - 1)(lambda: greet(self.zp))
        if far:
            when(self.sink)(lambda: greet(self.far))
        n = len(peers) + 1
        when(self.sink)(lambda: pl.semaphore_wait(bar, n + int(far)))
        when(jnp.logical_not(self.sink))(lambda: pl.semaphore_wait(bar, n + 1))

    def half(self, T, c):
        R = SHAPES[T][0]
        return ds(c * (R // 2), R // 2)

    def part(self, T, ab, w):
        R = SHAPES[T][0]
        return self.c * (R // 2) + ab * (R // 4) + w * (R // 8)

    def zrow(self, T, ab, e):
        return self.part(T, ab, self.w[ab]) + e * (SHAPES[T][0] // 16)

    def fin(self, T, ab, mine):
        row = self.zrow(T, ab, self.e)
        w = self.w2[ab] if mine else 1 - self.w2[ab]
        if T:
            return ds(row + w * PC, PC), slice(None)
        return ds(row, PC), cols(w)


def region(out, T, li, f, rows, col=None):
    if T:
        return out[T].at[li, rows, cols(f)]
    return out[T].at[li, ds(f * BLK + rows.start, rows.size), slice(None) if col is None else col]


def schedule(s, j, lag, T):
    d = j - T - lag
    return None if d % 2 else s + d // 2


def run(k, n, what, T, *more):
    if k is not None:
        when(both(k >= 0, k < n))(functools.partial(what, T, k, *more))


class Scatter:
    FLOWS = FD, F1, F3, FM, FP = range(0, 10, 2)
    CREDITS = CD, C1, C3, CM, CP = range(0, 10, 2)

    def __init__(self, g, n, ns, nsl, lags, bufs, deliver):
        self.g, self.n, self.ns, self.nsl, self.deliver = g, n, ns, nsl, deliver
        self.S, self.rD, self.r1, self.rz, self.r3 = [bufs[2 * i : 2 * i + 2] for i in range(5)]
        self.ssem, self.rsem, self.cred = bufs[10:]
        ld, l1, self.lz, l3 = lags
        self.lam1 = ld
        self.lam2 = ld + l1
        self.lam4 = self.lam2 + (NZ - 1) * self.lz + l3

    @staticmethod
    def scratch(ns, nsl):
        out = []
        for lead, div, div2 in (((nsl,), 1, 1), ((ns,), 2, 1), ((ns, 2), 8, 1), ((ns, 2, 2), 16, 1), ((ns, 2), 0, 0)):
            for R, C in SHAPES:
                out.append(scratch(F32, *lead, *((R // div, C) if div else (PC, BLK))))
        return out + [DMA((2, 10, ns))] * 2 + [pltpu.SemaphoreType.REGULAR((2, 10))]

    def copy(self, T, flow, k, src, dst, dev):
        i = (T, flow, rem(k, self.ns))
        return pltpu.make_async_remote_copy(src, dst, self.ssem.at[i], self.rsem.at[i], device_id=(dev,), device_id_type=MESH)

    def take(self, T, credit, k):
        when(k >= self.ns)(lambda: pl.semaphore_wait(self.cred.at[T, credit]))

    def give(self, T, credit, k, dev):
        when(k + self.ns < self.n)(lambda: pl.semaphore_signal(self.cred.at[T, credit], device_id=(dev,), device_id_type=MESH))

    def slots(self, k):
        return rem(k, self.nsl), rem(k, self.ns)

    def to_core(self, T, k):
        s, q = self.slots(k)
        return self.copy(T, self.FD, k, self.S[T].at[s, self.g.half(T, 1 - self.g.c)], self.rD[T].at[q], self.g.partner)

    def first(self, T, k, ab):
        s, q = self.slots(k)
        rows = ds(self.g.part(T, ab, 1 - self.g.w[ab]), SHAPES[T][0] // 8)
        return self.copy(T, self.F1 + ab, k, self.S[T].at[s, rows], self.r1[T].at[q, ab], self.g.n1[ab])

    def zrows(self, T, ab, e):
        return ds(self.g.zrow(T, ab, e), SHAPES[T][0] // 16)

    def along(self, T, k, dirn, ab):
        s, q = self.slots(k)
        flow = (self.FP if dirn else self.FM) + ab
        src = self.S[T].at[s, self.zrows(T, ab, dirn)]
        return self.copy(T, flow, k, src, self.rz[T].at[q, ab, dirn], self.g.zp if dirn else self.g.zm)

    def last(self, T, k, ab):
        s, q = self.slots(k)
        return self.copy(T, self.F3 + ab, k, self.S[T].at[(s, *self.g.fin(T, ab, False))], self.r3[T].at[q, ab], self.g.n2[ab])

    def add(self, T, k, rows, val):
        s, _ = self.slots(k)
        self.S[T][s, rows] = self.S[T][s, rows] + val

    def begin(self, T, k):
        self.take(T, self.CD, k)
        self.to_core(T, k).start()

    def after_core(self, T, k):
        g = self.g
        self.to_core(T, k).wait()
        self.add(T, k, g.half(T, g.c), self.rD[T][rem(k, self.ns)])
        self.give(T, self.CD, k, g.partner)
        for ab in AB:
            self.take(T, self.C1 + ab, k)
            self.first(T, k, ab).start()

    def after_first(self, T, k):
        g = self.g
        for ab in AB:
            self.first(T, k, ab).wait()
        for ab in AB:
            self.add(T, k, ds(g.part(T, ab, g.w[ab]), SHAPES[T][0] // 8), self.r1[T][rem(k, self.ns), ab])
            self.give(T, self.C1 + ab, k, g.n1[ab])

    def line(self, T, k, dirn):
        g = self.g
        p = g.place(dirn)
        credit = self.CP if dirn else self.CM

        @when(k < self.n)
        def _():
            @when(p > 0)
            def _():
                for ab in AB:
                    self.along(T, k, dirn, ab).wait_recv()
                for ab in AB:
                    self.add(T, k, self.zrows(T, ab, dirn), self.rz[T][rem(k, self.ns), ab, dirn])
                self.give(T, credit, k, g.zm if dirn else g.zp)

            @when(p < NZ - 1)
            def _():
                self.take(T, credit, k)
                for ab in AB:
                    self.along(T, k, dirn, ab).start()

            @when(p == NZ - 1)
            def _():
                for ab in AB:
                    self.take(T, self.C3 + ab, k)
                    self.last(T, k, ab).start()

        @when(both(k > 0, p < NZ - 1))
        def _():
            for ab in AB:
                self.along(T, k - 1, dirn, ab).wait_send()

    def after_last(self, T, k):
        g = self.g

        @when(g.sink)
        def _():
            s, q = self.slots(k)
            for ab in AB:
                self.last(T, k, ab).wait()
            for ab in AB:
                self.deliver(T, k, ab, self.S[T][(s, *g.fin(T, ab, True))] + self.r3[T][q, ab])
                self.give(T, self.C3 + ab, k, g.n2[ab])

    def due(self, s, j):
        for T in TYPES:
            run(schedule(s, j, self.lam4, T), self.n, self.after_last, T)
        for T in TYPES:
            k = schedule(s, j, self.lam2, T)
            run(k, self.n, self.after_first, T)
            if k is not None:
                for dirn in DIRS:
                    run(k - self.g.place(dirn) * (self.lz // 2), self.n + 1, self.line, T, dirn)
        for T in TYPES:
            run(schedule(s, j, self.lam1, T), self.n, self.after_core, T)

    def steps(self):
        return self.n + (self.lam4 + 1) // 2 + 1


class Gather:
    FLOWS = F3, FM, FP, FE0, FE1, FD = range(6)

    def __init__(self, g, n, nf, layer, lags, own, out, sems, start=0):
        self.g, self.n, self.nf, self.layer, self.own, self.out = g, n, nf, layer, own, out
        self.ssem, self.rsem, self.lsem = sems
        self.ns = self.ssem.shape[-1]
        l3, self.lz, le, ld = lags
        self.mu0 = start
        self.mu1 = start + l3
        self.mu2 = self.mu1 + (NZ - 1) * self.lz + le
        self.mu3 = self.mu2 + ld

    @staticmethod
    def scratch(n, ns):
        return [DMA((2, 6, ns)), DMA((2, 6, n)), DMA((2, 2, ns))]

    def region(self, T, k, rows, col=None):
        return region(self.out, T, self.layer(k // self.nf), rem(k, self.nf), rows, col)

    def rows(self, T, k, row, div):
        return self.region(T, k, ds(row, SHAPES[T][0] // div))

    def copy(self, T, flow, k, src, dst, dev):
        return pltpu.make_async_remote_copy(src, dst, self.ssem.at[T, flow, rem(k, self.ns)], self.rsem.at[T, flow, k],
            device_id=(dev,), device_id_type=MESH)

    def keep(self, T, k, ab):
        rows, col = self.g.fin(T, ab, True)
        return local(self.own[T].at[k, ab], self.region(T, k, rows, col), self.lsem.at[T, ab, rem(k, self.ns)])

    def begin(self, T, k):
        g = self.g

        @when(g.sink)
        def _():
            for ab in AB:
                rows, col = g.fin(T, ab, True)
                self.keep(T, k, ab).start()
                self.copy(T, self.F3, k, self.own[T].at[k, ab], self.region(T, k, rows, col), g.n2[ab]).start()

    def over(self, T, flow, k, ref, send=True, recv=True):
        if send:
            local(ref, ref, self.ssem.at[T, flow, rem(k, self.ns)]).wait()
        if recv:
            local(ref, ref, self.rsem.at[T, flow, k]).wait()

    def line(self, T, k, dirn):
        g = self.g
        p = g.place(dirn)
        e = 1 - dirn
        flow = self.FP if dirn else self.FM
        pair = lambda k: self.rows(T, k, 0, 8)

        @when(k < self.n)
        def _():
            @when(p == 0)
            def _():
                for ab in AB:
                    self.keep(T, k, ab).wait()
                self.over(T, self.F3, k, self.own[T].at[k])

            when(p > 0)(lambda: self.over(T, flow, k, pair(k), send=False))
            parts = [self.rows(T, k, g.zrow(T, ab, e), 16) for ab in AB]

            @when(p < NZ - 1)
            def _():
                for r in parts:
                    self.copy(T, flow, k, r, r, g.zp if dirn else g.zm).start()

            for ab in AB:
                self.copy(T, self.FE0 + e, k, parts[ab], parts[ab], g.n1[ab]).start()

        when(both(k > 0, p < NZ - 1))(lambda: self.over(T, flow, k - 1, pair(k - 1), recv=False))

    def to_core(self, T, k):
        r = self.region(T, k, self.g.half(T, self.g.c))
        return self.copy(T, self.FD, k, r, r, self.g.partner)

    def after_first(self, T, k):
        for e in TWO:
            self.over(T, self.FE0 + e, k, self.rows(T, k, 0, 8))
        self.to_core(T, k).start()

    def done(self, T, k):
        self.to_core(T, k).wait()

    def due(self, s, j):
        for T in TYPES:
            run(schedule(s, j, self.mu0, T), self.n, self.begin, T)
        for T in TYPES:
            k = schedule(s, j, self.mu1, T)
            if k is not None:
                for dirn in DIRS:
                    run(k - self.g.place(dirn) * (self.lz // 2), self.n + 1, self.line, T, dirn)
        for T in TYPES:
            run(schedule(s, j, self.mu2, T), self.n, self.after_first, T)
            run(schedule(s, j, self.mu3, T), self.n, self.done, T)

    def steps(self):
        return self.n + (self.mu3 + 1) // 2 + 1


class PairSum:
    GAP = 3

    def __init__(self, devs, bufs):
        self.devs = devs
        self.part, self.nbr, self.ssem, self.rsem = bufs

    @staticmethod
    def scratch(n):
        return [scratch(F32, n + 1, SUB, LANE), scratch(F32, n, SUB, LANE), DMA((n,)), DMA((n,))]

    def copy(self, r):
        return pltpu.make_async_remote_copy(self.part.at[r], self.nbr.at[r], self.ssem.at[r], self.rsem.at[r],
            device_id=(self.devs[r],), device_id_type=MESH)

    def finish(self, r):
        self.copy(r).wait()
        self.part[r + 1] = self.part[r] + self.nbr[r]

    def due(self, s):
        for r in range(len(self.devs)):
            when(s == r * self.GAP)(lambda: self.copy(r).start())
            when(s == r * self.GAP + self.GAP - 1)(lambda: self.finish(r))

    def now(self):
        for r in range(len(self.devs)):
            self.copy(r).start()
            self.finish(r)


def gelu(z):
    half = HALF * z
    return half + half * jnp.tanh(z * (GELU_A + (GELU_A * GELU_B) * (z * z)))


def gelu_parts(z):
    zz = z * z
    t = jnp.tanh(z * (GELU_A + (GELU_A * GELU_B) * zz))
    half = HALF * z
    slope = (HALF + HALF * t) + half * ((1 - t * t) * (GELU_A + (3 * GELU_A * GELU_B) * zz))
    return half + half * t, slope


class Forward:
    def __init__(self, nl, nf, hbm, outs, bufs):
        self.nl, self.nf = nl, nf
        self.x, self.y, self.wo_h, self.wi_h = hbm
        self.h_o, self.z_o, self.q_o, self.loss = outs
        self.h, self.yb, self.acc, self.a, self.z, self.wo, self.wi, self.hsem, self.zsem, self.wsem = bufs

    @staticmethod
    def scratch(tok, wdt):
        return [scratch(BF, tok, D), scratch(BF, tok, D), scratch(F32, tok, D), scratch(BF, tok, BLK), scratch(BF, 2, tok, BLK),
                scratch(wdt, 2, BLK, D), scratch(wdt, 2, D, BLK), DMA((3,)), DMA((2,)), DMA((2, 2))]

    @staticmethod
    def shapes(nl, tok, dff):
        S = jax.ShapeDtypeStruct
        return [S((nl, tok, D), BF), S((nl, tok, dff), BF), S((tok, D), BF), S((SUB, LANE), F32)]

    def tiles(self):
        return [pl.ds(r, FT) for r in range(0, self.h.shape[0], FT)]

    def h_copy(self, dst):
        return local(self.h, dst, self.hsem.at[0])

    def z_copy(self, s):
        b = rem(s, 2)
        return local(self.z.at[b], self.z_o.at[s // self.nf, :, cols(rem(s, self.nf))], self.zsem.at[b])

    def loads(self, s):
        li, f, b = s // self.nf, rem(s, self.nf), rem(s, 2)
        return [local(self.wo_h.at[li, cols(f)], self.wo.at[b], self.wsem.at[0, b]),
                local(self.wi_h.at[li, :, cols(f)], self.wi.at[b], self.wsem.at[1, b])]

    def prologue(self):
        self.cy = local(self.y, self.yb, self.hsem.at[2])
        cx = local(self.x, self.h, self.hsem.at[1])
        start([cx, self.cy])
        self.loss[...] = jnp.zeros_like(self.loss)
        cx.wait()
        self.acc[...] = self.h[...].astype(F32)
        self.h_copy(self.h_o.at[0]).start()

    def block(self, s):
        li, f, b = s // self.nf, rem(s, self.nf), rem(s, 2)
        wait(self.loads(s))
        when(s > 1)(lambda: self.z_copy(s).wait())
        wi, wo = self.wi[b].astype(BF), self.wo[b].astype(BF)
        for rows in self.tiles():
            z = dg(self.h[rows], wi, 1, 0).astype(BF)
            self.z[b, rows] = z
            self.a[rows] = gelu(z.astype(F32)).astype(BF)
        self.z_copy(s).start()
        for rows in self.tiles():
            self.acc[rows] = self.acc[rows] + dg(self.a[rows], wo, 1, 0)

        @when(f == self.nf - 1)
        def _():
            self.h_copy(self.h_o.at[0]).wait()
            step = PC * 7

            @when(li < self.nl - 1)
            def _():
                for r in range(0, self.h.shape[0], step):
                    h = self.acc[r : r + step].astype(BF)
                    self.h[r : r + step] = h
                    self.acc[r : r + step] = h.astype(F32)
                self.h_copy(self.h_o.at[li + 1]).start()

            @when(li == self.nl - 1)
            def _():
                self.cy.wait()
                for r in range(0, self.h.shape[0], step):
                    err = self.acc[r : r + step].astype(BF).astype(F32) - self.yb[r : r + step].astype(F32)
                    self.h[r : r + step] = err.astype(BF)
                    sq = jnp.sum((err * err).reshape(step // SUB, SUB, D), axis=0)
                    for b in range(D // LANE):
                        self.loss[...] += sq[:, b * LANE : (b + 1) * LANE]
                self.h_copy(self.q_o).start()

    def epilogue(self):
        wait([self.z_copy(s) for s in TWO] + [self.h_copy(self.q_o)])


def forward_kernel(nl, x, y, w_out, w_in, h_o, z_o, q_o, loss, *bufs):
    n = nl * w_out.shape[1] // BLK
    fw = Forward(nl, n // nl, (x, y, w_out, w_in), (h_o, z_o, q_o, loss), bufs)
    start(fw.loads(0))
    fw.prologue()

    def body(s, _):
        when(s + 1 < n)(lambda: start(fw.loads(s + 1)))
        fw.block(s)
        return 0

    lax.fori_loop(0, n, body, 0)
    fw.epilogue()


def forward(x, y, w_out, w_in):
    nl, dff, _ = w_out.shape
    tok = x.shape[0]
    return pl.pallas_call(
        functools.partial(forward_kernel, nl),
        out_shape=Forward.shapes(nl, tok, dff),
        in_specs=[HBM] * 4,
        out_specs=[HBM] * 3 + [VM],
        scratch_shapes=Forward.scratch(tok, F32),
        compiler_params=pltpu.CompilerParams(vmem_limit_bytes=63 * MIB),
        name="forward",
    )(x, y, w_out, w_in)


def gather_forward_kernel(nl, lags, pe_o, pe_i, x, y, wo_o, wi_o, h_o, z_o, q_o, loss, own_o, own_i, wsem, *bufs):
    g = Geo()
    n = pe_o.shape[0]
    nf = n // nl
    ga = Gather(g, n, nf, lambda q: q, lags, (own_o, own_i), (wo_o, wi_o), bufs[:3])
    fw = Forward(nl, nf, (x, y, wo_o, wi_o), (h_o, z_o, q_o, loss), bufs[3:])
    pieces = [local(src, dst, wsem.at[i]) for i, (src, dst) in enumerate(((pe_o, own_o), (pe_i, own_i)))]
    start(pieces)
    fw.prologue()
    g.enter()
    wait(pieces)
    lead = (ga.mu3 + 1) // 2 + 2

    def body(s, _):
        ga.due(s, 0)
        when(both(s + 1 >= lead, s + 1 < lead + n))(lambda: start(fw.loads(s + 1 - lead)))
        when(s >= lead)(lambda: fw.block(s - lead))
        ga.due(s, 1)
        return 0

    lax.fori_loop(0, lead + n, body, 0)
    fw.epilogue()


def gather_forward(pe_o, pe_i, x, y, nl, ns=12, lags=(4, 4, 4, 3), cid=2):
    n, tok = pe_o.shape[0], x.shape[0]
    dff = n // nl * BLK
    S = jax.ShapeDtypeStruct
    return pl.pallas_call(
        functools.partial(gather_forward_kernel, nl, lags),
        out_shape=[S((nl, dff, D), BF), S((nl, D, dff), BF)] + Forward.shapes(nl, tok, dff),
        in_specs=[HBM] * 4,
        out_specs=[HBM] * 5 + [VM],
        scratch_shapes=[scratch(BF, n, 2, PC, BLK)] * 2 + [DMA((2,))] + Gather.scratch(n, ns) + Forward.scratch(tok, BF),
        cost_estimate=pl.CostEstimate(flops=tok * D * dff * nl * 4, bytes_accessed=60 * MIB, transcendentals=0),
        compiler_params=pltpu.CompilerParams(collective_id=cid, has_side_effects=True, vmem_limit_bytes=63 * MIB),
        name="gather_forward",
    )(pe_o, pe_i, x, y)


class Backward:
    def __init__(self, nl, tok, hbm, bufs):
        self.nl, self.tok = nl, tok
        self.q_h, self.h_h, self.z_h, self.wo_h, self.wi_h = hbm
        self.q, self.h, self.z, self.wo, self.wi, self.a, self.p, self.acc, self.sem = bufs
        self.nf = self.z_h.shape[-1] // BLK
        self.n = nl * self.nf

    @staticmethod
    def scratch(tok, wdt):
        return [scratch(BF, tok, D), scratch(BF, 2, tok, D), scratch(BF, 2, tok, BLK), scratch(wdt, 2, BLK, D), scratch(wdt, 2, D, BLK),
                scratch(BF, tok, BLK), scratch(BF, tok, BLK), scratch(F32, tok, D), DMA((5, 2))]

    def at(self, s):
        return self.nl - 1 - s // self.nf, rem(s, self.nf), rem(s, 2)

    def load_h(self, li):
        i = rem(li, 2)
        return local(self.h_h.at[li], self.h.at[i], self.sem.at[0, i])

    def loads(self, s):
        li, f, b = self.at(s)
        return [local(src, dst.at[b], self.sem.at[i + 1, b]) for i, (src, dst) in enumerate((
            (self.z_h.at[li, :, cols(f)], self.z), (self.wo_h.at[li, cols(f)], self.wo), (self.wi_h.at[li, :, cols(f)], self.wi)))]

    def prologue(self):
        cq = local(self.q_h, self.q, self.sem.at[4, 0])
        for c in [cq, *self.loads(0), self.load_h(self.nl - 1)]:
            c.start()
        cq.wait()
        self.acc[...] = self.q[...].astype(F32)

    def tiles(self):
        return [pl.ds(r * BT, BT) for r in range(self.tok // BT)]

    def out_block(self, s, dst):
        li, f, b = self.at(s)
        wait(self.loads(s))

        @when(s + 1 < self.n)
        def _():
            start(self.loads(s + 1))

        @when(f == 0)
        def _():
            self.load_h(li).wait()
            when(li > 0)(lambda: self.load_h(li - 1).start())

        wo = self.wo[b].astype(BF)
        for rows in self.tiles():
            a, slope = gelu_parts(self.z[b, rows].astype(F32))
            self.a[rows] = a.astype(BF)
            self.p[rows] = (dg(self.q[rows], wo, 1, 1) * slope).astype(BF)
        dst[...] = dg(self.a[...], self.q[...], 0, 0)

    def in_block(self, s, dst):
        li, f, b = self.at(s)
        dst[...] = dg(self.h[rem(li, 2)], self.p[...], 0, 0)

        @when(li > 0)
        def _():
            wi = self.wi[b].astype(BF)
            for rows in self.tiles():
                self.acc[rows] = self.acc[rows] + dg(self.p[rows], wi, 1, 1)

            @when(f == self.nf - 1)
            def _():
                for rows in self.tiles():
                    q = self.acc[rows].astype(BF)
                    self.q[rows] = q
                    self.acc[rows] = q.astype(F32)


def load_owned(g, n, nf, layer, mats, dst, sem):
    def issue(k, _):
        for T in TYPES:
            for ab in AB:
                rows, col = g.fin(T, ab, True)
                local(region(mats, T, layer(k // nf), rem(k, nf), rows, col), dst[T].at[k, ab], sem.at[T]).start()
        return 0

    lax.fori_loop(0, n, issue, 0)


def wait_owned(dst, sem):
    for T in TYPES:
        local(dst[T], dst[T], sem.at[T]).wait()


def backward_kernel(nl, tok, ns, nsl, lags, glags, norm, scale, coef, *refs):
    q_h, h_h, z_h, wo_h, wi_h, refs = *refs[:5], refs[5:]
    if norm:
        mats = wo_h, wi_h
    else:
        mats, tile, refs = refs[:2], refs[2], refs[3:]
    bw_hbm = q_h, h_h, z_h, wo_h, wi_h
    n = nl * (z_h.shape[-1] // BLK)
    nf = n // nl
    last_first = lambda q: nl - 1 - q
    out, refs = refs[:2], refs[2:]
    if not norm:
        loss, refs = refs[0], refs[1:]
    n_sc = len(Scatter.scratch(ns, nsl))
    sc_bufs, refs = refs[:n_sc], refs[n_sc:]
    bw, refs = Backward(nl, tok, bw_hbm, refs[:9]), refs[9:]
    w_p, wsem, refs = refs[:2], refs[2], refs[3:]
    g = Geo()
    bw.prologue()
    when(g.sink)(lambda: load_owned(g, n, nf, last_first, mats, w_p, wsem))
    if norm:
        own, pieces, sq, pair = refs[:2], refs[2:4], refs[4], refs[5:]
        ps = PairSum((g.partner, g.xn, g.yn, g.far), pair)
        sq[...] = jnp.zeros_like(sq)
    else:
        ps = PairSum((g.partner, g.xn, g.yn, g.z1, g.z2), refs[:4])
        ps.part[0] = tile[...]

    def deliver(T, k, ab, val):
        val = val * scale
        if norm:
            own[T][k, ab] = val
            sq[...] += val * val
        else:
            w_p[T][k, ab] = w_p[T][k, ab] - coef * val

    g.enter(far=norm, z2=not norm)
    sc = Scatter(g, n, ns, nsl, lags, sc_bufs, deliver)
    steps = sc.steps()
    if not norm:
        ga = Gather(g, n, nf, last_first, glags, w_p, out, refs[4:], sc.lam4 + 1)
        steps = ga.steps()

    def body(s, _):
        when(both(s == 1, g.sink))(lambda: wait_owned(w_p, wsem))
        for j, block in enumerate((bw.out_block, bw.in_block)):

            @when(s < n)
            def _():
                block(s, sc.S[j].at[rem(s, nsl)])
                sc.begin(j, s)

            sc.due(s, j)
            if not norm:
                ga.due(s, j)
        if not norm:
            ps.due(s)
        return 0

    lax.fori_loop(0, steps, body, 0)
    if not norm:
        loss[...] = ps.part[5]
        return

    @when(g.sink)
    def _():
        quarters = [sq[i * SUB : (i + 1) * SUB, j * LANE : (j + 1) * LANE] for i in TWO for j in TWO]
        ps.part[0] = sum(quarters[1:], quarters[0])
        ps.now()
        step = coef / jnp.sqrt(jnp.broadcast_to(jnp.sum(ps.part[4]), (1, 1)))

        def piece(k, _):
            to = (nl - 1 - k // nf) * nf + rem(k, nf)
            for T in TYPES:
                pieces[T][to] = (w_p[T][k] + step * own[T][k]).astype(BF)
            return 0

        lax.fori_loop(0, n, piece, 0)
        copies = [local(pieces[T], out[T], wsem.at[T]) for T in TYPES]
        start(copies)
        wait(copies)


def backward(q, h, z, wo, wi, scale, coef, new=None, ns=4, nsl=12, lags=(1, 4, 4, 4), glags=(4, 4, 4, 3), ngs=12, cid=1):
    nl, tok, dff = z.shape
    n = nl * dff // BLK
    norm = new is None
    S = jax.ShapeDtypeStruct
    piece = lambda dt: scratch(dt, n, 2, PC, BLK)
    scr = Scatter.scratch(ns, nsl) + Backward.scratch(tok, wo.dtype) + [piece(F32)] * 2 + [DMA((2,))]
    if norm:
        scr += [piece(F32)] * 2 + [piece(BF)] * 2 + [scratch(F32, PC, BLK)] + PairSum.scratch(4)
        outs, specs, more = [S((n, 2, PC, BLK), BF)] * 2, [HBM] * 2, ()
    else:
        scr += PairSum.scratch(5) + Gather.scratch(n, ngs)
        outs, specs, more = [S(new[0].shape, F32), S(new[1].shape, F32), S((SUB, LANE), F32)], [HBM] * 2 + [VM], new
    return pl.pallas_call(
        functools.partial(backward_kernel, nl, tok, ns, nsl, lags, glags, norm, scale, coef),
        out_shape=outs,
        in_specs=[HBM] * 5 + [HBM, HBM, VM][: len(more)],
        out_specs=specs,
        scratch_shapes=scr,
        cost_estimate=pl.CostEstimate(flops=tok * D * dff * nl * 8, bytes_accessed=60 * MIB, transcendentals=0),
        compiler_params=pltpu.CompilerParams(collective_id=cid, has_side_effects=True, vmem_limit_bytes=63 * MIB),
        name="backward_norm" if norm else "backward_update",
    )(q, h, z, wo, wi, *more)


def solution(mesh):
    n_dev = mesh.shape["data"]

    def local_step(x_loc, y_loc, w_in, w_out):
        nl, d_model, d_ff = w_in.shape
        scale = 1.0 / (x_loc.shape[0] * n_dev * x_loc.shape[1] * d_model)
        rho = RHO_FRAC * math.sqrt(nl * (d_model + d_ff))
        x, y = [v.reshape(-1, d_model) for v in (x_loc, y_loc)]
        h, z, q, _ = forward(x, y, w_out, w_in)
        pieces = backward(q, h, z, w_out, w_in, scale, rho, cid=1)
        wo, wi, h, z, q, tile = gather_forward(*pieces, x, y, nl, cid=2)
        new_out, new_in, tile = backward(q, h, z, wo, wi, scale, LEARN_RATE, (w_out, w_in, tile), cid=3)
        return new_in, new_out, HALF * (jnp.sum(tile) * scale)

    specs = P("data"), P("data"), P(), P()
    return jax.shard_map(local_step, mesh=mesh, in_specs=specs, out_specs=(P(), P(), P()), check_vma=False)
```

```python
import functools
import math

import jax
import jax.numpy as jnp
from jax import lax
from jax.experimental import pallas as pl
from jax.experimental.pallas import tpu as pltpu
from jax.sharding import PartitionSpec as P

MESH = pl.DeviceIdType.MESH
F32, BF = jnp.float32, jnp.bfloat16
RHO_FRAC = 0.1
LEARN_RATE = 1.0
D = 512
BLK = 256
PC = 16
FT = 224
BT = 1568
SUB, LANE = 8, 128
NZ = 4
HALF = 0.5
MIB = 2**20
GELU_A = math.sqrt(2.0 / math.pi)
GELU_B = 0.044715
TWO = AB = TYPES = DIRS = (0, 1)
SHAPES = ((BLK, D), (D, BLK))
ANY = pl.BlockSpec(memory_space=pl.ANY)
HBM = pl.BlockSpec(memory_space=pltpu.HBM)
VM = pl.BlockSpec(memory_space=pltpu.VMEM)
DMA = pltpu.SemaphoreType.DMA
rem, div = lax.rem, lax.div
when = pl.when


def both(*conds):
    return functools.reduce(jnp.logical_and, conds)


def ds(start, size):
    return pl.ds(pl.multiple_of(start, SUB), size)


def cols(f):
    return pl.ds(pl.multiple_of(f * BLK, BLK), BLK)


def dg(a, b, ca, cb):
    return lax.dot_general(a, b, (((ca,), (cb,)), ((), ())), preferred_element_type=F32)


def scratch(dtype, *shape):
    return pltpu.VMEM(shape, dtype)


def local(src, dst, sem):
    return pltpu.make_async_copy(src, dst, sem)


def start(copies):
    for c in copies:
        c.start()


def wait(copies):
    for c in copies:
        c.wait()


class Geo:
    def __init__(self):
        me = lax.axis_index("data")
        flip = lambda step: me + step - 2 * step * rem(me // step, 2)
        self.me = me
        self.c, self.x, self.y, self.z = [rem(me // step, n) for step, n in ((1, 2), (2, 2), (4, 2), (8, NZ))]
        self.partner, self.xn, self.yn, self.z1, self.z2 = [flip(1 << k) for k in range(5)]
        self.zm, self.zp = me - 8, me + 8
        self.e = self.z // (NZ - 1)
        self.sink = rem(self.z, NZ - 1) == 0
        self.far = me + 24 - 48 * self.e
        self.w = (self.x, self.y)
        self.w2 = (self.y, self.x)
        self.n1 = (self.xn, self.yn)
        self.n2 = (self.yn, self.xn)

    def place(self, dirn):
        return self.z if dirn else NZ - 1 - self.z

    def greet(self):
        self.bar = pltpu.get_barrier_semaphore()
        hello = lambda dev: pl.semaphore_signal(self.bar, device_id=(dev,), device_id_type=MESH)
        for dev in (self.partner, self.xn, self.yn, self.z2):
            hello(dev)
        when(self.z > 0)(lambda: hello(self.zm))
        when(self.z < NZ - 1)(lambda: hello(self.zp))
        when(self.sink)(lambda: hello(self.far))

    def meet(self):
        pl.semaphore_wait(self.bar, 6)

    def half(self, T, c):
        R = SHAPES[T][0]
        return ds(c * (R // 2), R // 2)

    def part(self, T, ab, w):
        R = SHAPES[T][0]
        return self.c * (R // 2) + ab * (R // 4) + w * (R // 8)

    def zrow(self, T, ab, e):
        return self.part(T, ab, self.w[ab]) + e * (SHAPES[T][0] // 16)

    def fin(self, T, ab, mine):
        row = self.zrow(T, ab, self.e)
        w = self.w2[ab] if mine else 1 - self.w2[ab]
        if T:
            return ds(row + w * PC, PC), slice(None)
        return ds(row, PC), cols(w)


def region(out, T, li, f, rows, col=None):
    if T:
        return out[T].at[li, rows, cols(f)]
    return out[T].at[li, ds(f * BLK + rows.start, rows.size), slice(None) if col is None else col]


def schedule(s, j, lag, T):
    d = j - T - lag
    return None if d % 2 else s + d // 2


def run(k, n, what, T, *more):
    if k is not None:
        when(both(k >= 0, k < n))(functools.partial(what, T, k, *more))


class Scatter:
    FLOWS = FD, F1, F3, FM, FP = range(0, 10, 2)
    CREDITS = CD, C1, C3, CM, CP = range(0, 10, 2)

    def __init__(self, g, n, ns, nsl, lags, bufs, deliver):
        self.g, self.n, self.ns, self.nsl, self.deliver = g, n, ns, nsl, deliver
        self.S, self.rD, self.r1, self.rz, self.r3 = [bufs[2 * i : 2 * i + 2] for i in range(5)]
        self.ssem, self.rsem, self.cred = bufs[10:]
        ld, l1, self.lz, l3 = lags
        self.lam1 = ld
        self.lam2 = ld + l1
        self.lam4 = self.lam2 + (NZ - 1) * self.lz + l3

    @staticmethod
    def scratch(ns, nsl):
        out = []
        for lead, div, div2 in (((nsl,), 1, 1), ((ns,), 2, 1), ((ns, 2), 8, 1), ((ns, 2, 2), 16, 1), ((ns, 2), 0, 0)):
            for R, C in SHAPES:
                out.append(scratch(F32, *lead, *((R // div, C) if div else (PC, BLK))))
        return out + [DMA((2, 10, ns))] * 2 + [pltpu.SemaphoreType.REGULAR((2, 10))]

    def copy(self, T, flow, k, src, dst, dev):
        i = (T, flow, rem(k, self.ns))
        return pltpu.make_async_remote_copy(src, dst, self.ssem.at[i], self.rsem.at[i], device_id=(dev,), device_id_type=MESH)

    def take(self, T, credit, k):
        when(k >= self.ns)(lambda: pl.semaphore_wait(self.cred.at[T, credit]))

    def give(self, T, credit, k, dev):
        when(k + self.ns < self.n)(lambda: pl.semaphore_signal(self.cred.at[T, credit], device_id=(dev,), device_id_type=MESH))

    def slots(self, k):
        return rem(k, self.nsl), rem(k, self.ns)

    def to_core(self, T, k):
        s, q = self.slots(k)
        return self.copy(T, self.FD, k, self.S[T].at[s, self.g.half(T, 1 - self.g.c)], self.rD[T].at[q], self.g.partner)

    def first(self, T, k, ab):
        s, q = self.slots(k)
        rows = ds(self.g.part(T, ab, 1 - self.g.w[ab]), SHAPES[T][0] // 8)
        return self.copy(T, self.F1 + ab, k, self.S[T].at[s, rows], self.r1[T].at[q, ab], self.g.n1[ab])

    def zrows(self, T, ab, e):
        return ds(self.g.zrow(T, ab, e), SHAPES[T][0] // 16)

    def along(self, T, k, dirn, ab):
        s, q = self.slots(k)
        flow = (self.FP if dirn else self.FM) + ab
        src = self.S[T].at[s, self.zrows(T, ab, dirn)]
        return self.copy(T, flow, k, src, self.rz[T].at[q, ab, dirn], self.g.zp if dirn else self.g.zm)

    def last(self, T, k, ab):
        s, q = self.slots(k)
        return self.copy(T, self.F3 + ab, k, self.S[T].at[(s, *self.g.fin(T, ab, False))], self.r3[T].at[q, ab], self.g.n2[ab])

    def add(self, T, k, rows, val):
        s, _ = self.slots(k)
        self.S[T][s, rows] = self.S[T][s, rows] + val

    def begin(self, T, k):
        self.take(T, self.CD, k)
        self.to_core(T, k).start()

    def after_core(self, T, k):
        g = self.g
        self.to_core(T, k).wait()
        self.add(T, k, g.half(T, g.c), self.rD[T][rem(k, self.ns)])
        self.give(T, self.CD, k, g.partner)
        for ab in AB:
            self.take(T, self.C1 + ab, k)
            self.first(T, k, ab).start()

    def after_first(self, T, k):
        g = self.g
        for ab in AB:
            self.first(T, k, ab).wait()
        for ab in AB:
            self.add(T, k, ds(g.part(T, ab, g.w[ab]), SHAPES[T][0] // 8), self.r1[T][rem(k, self.ns), ab])
            self.give(T, self.C1 + ab, k, g.n1[ab])

    def line(self, T, k, dirn):
        g = self.g
        p = g.place(dirn)
        credit = self.CP if dirn else self.CM

        @when(k < self.n)
        def _():
            @when(p > 0)
            def _():
                for ab in AB:
                    self.along(T, k, dirn, ab).wait_recv()
                for ab in AB:
                    self.add(T, k, self.zrows(T, ab, dirn), self.rz[T][rem(k, self.ns), ab, dirn])
                self.give(T, credit, k, g.zm if dirn else g.zp)

            @when(p < NZ - 1)
            def _():
                self.take(T, credit, k)
                for ab in AB:
                    self.along(T, k, dirn, ab).start()

            @when(p == NZ - 1)
            def _():
                for ab in AB:
                    self.take(T, self.C3 + ab, k)
                    self.last(T, k, ab).start()

        @when(both(k > 0, p < NZ - 1))
        def _():
            for ab in AB:
                self.along(T, k - 1, dirn, ab).wait_send()

    def after_last(self, T, k):
        g = self.g

        @when(g.sink)
        def _():
            s, q = self.slots(k)
            for ab in AB:
                self.last(T, k, ab).wait()
            for ab in AB:
                self.deliver(T, k, ab, self.S[T][(s, *g.fin(T, ab, True))] + self.r3[T][q, ab])
                self.give(T, self.C3 + ab, k, g.n2[ab])

    def due(self, s, j):
        for T in TYPES:
            run(schedule(s, j, self.lam4, T), self.n, self.after_last, T)
        for T in TYPES:
            k = schedule(s, j, self.lam2, T)
            run(k, self.n, self.after_first, T)
            if k is not None:
                for dirn in DIRS:
                    run(k - self.g.place(dirn) * (self.lz // 2), self.n + 1, self.line, T, dirn)
        for T in TYPES:
            run(schedule(s, j, self.lam1, T), self.n, self.after_core, T)

    def steps(self):
        return self.n + (self.lam4 + 1) // 2 + 1


class Gather:
    FLOWS = F3, FM, FP, FE0, FE1, FD = range(6)

    def __init__(self, g, n, nf, layer, lags, own, out, sems, start=0, whole=None):
        self.g, self.n, self.nf, self.layer, self.own, self.out, self.whole = g, n, nf, layer, own, out, whole
        self.ssem, self.rsem, self.lsem = sems
        self.ns = self.ssem.shape[-1]
        l3, self.lz, le, ld = lags
        self.mu0 = start
        self.mu1 = start + l3
        self.mu2 = self.mu1 + (NZ - 1) * self.lz + le
        self.mu3 = self.mu2 + ld

    @staticmethod
    def scratch(n, ns):
        return [DMA((2, 6, ns)), DMA((2, 6, n)), DMA((2, 2, ns))]

    def region(self, T, k, rows, col=None):
        return region(self.out, T, self.layer(div(k, self.nf)), rem(k, self.nf), rows, col)

    def rows(self, T, k, row, div):
        return self.region(T, k, ds(row, SHAPES[T][0] // div))

    def copy(self, T, flow, k, src, dst, dev):
        return pltpu.make_async_remote_copy(src, dst, self.ssem.at[T, flow, rem(k, self.ns)], self.rsem.at[T, flow, k],
            device_id=(dev,), device_id_type=MESH)

    def keep(self, T, k, ab):
        rows, col = self.g.fin(T, ab, True)
        return local(self.own[T].at[k, ab], self.region(T, k, rows, col), self.lsem.at[T, ab, rem(k, self.ns)])

    def begin(self, T, k):
        g = self.g

        @when(g.sink)
        def _():
            for ab in AB:
                rows, col = g.fin(T, ab, True)
                self.keep(T, k, ab).start()
                self.copy(T, self.F3, k, self.own[T].at[k, ab], self.region(T, k, rows, col), g.n2[ab]).start()

    def over(self, T, flow, k, ref, send=True, recv=True):
        if send:
            local(ref, ref, self.ssem.at[T, flow, rem(k, self.ns)]).wait()
        if recv:
            local(ref, ref, self.rsem.at[T, flow, k]).wait()

    def line(self, T, k, dirn):
        g = self.g
        p = g.place(dirn)
        e = 1 - dirn
        flow = self.FP if dirn else self.FM
        pair = lambda k: self.rows(T, k, 0, 8)

        @when(k < self.n)
        def _():
            @when(p == 0)
            def _():
                for ab in AB:
                    self.keep(T, k, ab).wait()
                self.over(T, self.F3, k, self.own[T].at[k])

            when(p > 0)(lambda: self.over(T, flow, k, pair(k), send=False))
            parts = [self.rows(T, k, g.zrow(T, ab, e), 16) for ab in AB]

            @when(p < NZ - 1)
            def _():
                for r in parts:
                    self.copy(T, flow, k, r, r, g.zp if dirn else g.zm).start()

            for ab in AB:
                self.copy(T, self.FE0 + e, k, parts[ab], parts[ab], g.n1[ab]).start()

        when(both(k > 0, p < NZ - 1))(lambda: self.over(T, flow, k - 1, pair(k - 1), recv=False))

    def to_core(self, T, k):
        r = self.region(T, k, self.g.half(T, self.g.c))
        return self.copy(T, self.FD, k, r, r, self.g.partner)

    def after_first(self, T, k):
        for e in TWO:
            self.over(T, self.FE0 + e, k, self.rows(T, k, 0, 8))
        self.to_core(T, k).start()

    def done(self, T, k):
        self.to_core(T, k).wait()
        if self.whole:
            self.whole(T, k)

    def due(self, s, j):
        for T in TYPES:
            run(schedule(s, j, self.mu0, T), self.n, self.begin, T)
        for T in TYPES:
            k = schedule(s, j, self.mu1, T)
            if k is not None:
                for dirn in DIRS:
                    run(k - self.g.place(dirn) * (self.lz // 2), self.n + 1, self.line, T, dirn)
        for T in TYPES:
            run(schedule(s, j, self.mu2, T), self.n, self.after_first, T)
            run(schedule(s, j, self.mu3, T), self.n, self.done, T)

    def steps(self):
        return self.n + (self.mu3 + 1) // 2 + 1


class PairSum:
    GAP = 3

    def __init__(self, devs, bufs):
        self.devs = devs
        self.part, self.nbr, self.ssem, self.rsem = bufs

    @staticmethod
    def scratch(n):
        return [scratch(F32, n + 1, SUB, LANE), scratch(F32, n, SUB, LANE), DMA((n,)), DMA((n,))]

    def copy(self, r):
        return pltpu.make_async_remote_copy(self.part.at[r], self.nbr.at[r], self.ssem.at[r], self.rsem.at[r],
            device_id=(self.devs[r],), device_id_type=MESH)

    def finish(self, r):
        self.copy(r).wait()
        self.part[r + 1] = self.part[r] + self.nbr[r]

    def due(self, s):
        for r in range(len(self.devs)):
            when(s == r * self.GAP)(lambda: self.copy(r).start())
            when(s == r * self.GAP + self.GAP - 1)(lambda: self.finish(r))

    def now(self):
        for r in range(len(self.devs)):
            self.copy(r).start()
            self.finish(r)


def gelu(z):
    return z * (HALF + HALF * jnp.tanh(z * (GELU_A + (GELU_A * GELU_B) * (z * z))))


def gelu_parts(z):
    zz = z * z
    half = HALF + HALF * jnp.tanh(z * (GELU_A + (GELU_A * GELU_B) * zz))
    slope = half + (z * (half - half * half)) * (2 * GELU_A + (6 * GELU_A * GELU_B) * zz)
    return z * half, slope


class Weights:
    def __init__(self, mats, bufs):
        self.wo_h, self.wi_h = mats
        self.wo, self.wi, self.sem = bufs

    @staticmethod
    def scratch():
        return [scratch(F32, 2, BLK, D), scratch(F32, 2, D, BLK), DMA((2, 2))]

    def loads(self, li, f, b):
        return [local(self.wo_h.at[li, cols(f)], self.wo.at[b], self.sem.at[0, b]), local(self.wi_h.at[li, :, cols(f)], self.wi.at[b], self.sem.at[1, b])]

    def load(self, *at):
        start(self.loads(*at))

    def ready(self, *at):
        wait(self.loads(*at))

    def w_out(self, li, f, b):
        return self.wo[b].astype(BF)

    def w_in(self, li, f, b):
        return self.wi[b].astype(BF)


class Whole:
    def __init__(self, vo, vi):
        self.vo, self.vi = vo, vi

    def load(self, *at):
        pass

    ready = load

    def w_out(self, li, f, b):
        return self.vo[li, cols(f)]

    def w_in(self, li, f, b):
        return self.vi[li, :, cols(f)]


class Acts:
    def __init__(self, hbm, bufs):
        self.h_o, self.z_o = hbm
        self.h, self.hb, self.acc, self.a, self.p, self.z, self.img, self.loss, self.hsem, self.zsem, self.isem = bufs
        self.nl, self.tok, dff = self.z_o.shape
        self.nf = dff // BLK
        self.n = self.nl * self.nf
        self.small = [pl.ds(r, PC * 7) for r in range(0, self.tok, PC * 7)]

    @staticmethod
    def scratch(images, rows):
        tok = images * rows
        return [scratch(BF, tok, D), scratch(BF, 2, tok, D), scratch(F32, tok, D), scratch(BF, tok, BLK), scratch(BF, tok, BLK),
                scratch(BF, 2, tok, BLK), scratch(BF, images, rows, D), scratch(F32, SUB, LANE), DMA((2,)), DMA((2,)), DMA((2,))]

    def tiles(self, size):
        return [pl.ds(r, size) for r in range(0, self.tok, size)]

    def images(self):
        count, rows, _ = self.img.shape
        return [(i, pl.ds(i * rows, rows)) for i in range(count)]

    def z_rows(self, li, f):
        return self.z_o.at[li, :, cols(f)]


class Forward:
    def __init__(self, acts, x, y, weights):
        self.t, self.x, self.y, self.w = acts, x, y, weights

    def at(self, s):
        return div(s, self.t.nf), rem(s, self.t.nf), rem(s, 2)

    def h_copy(self, li):
        return local(self.t.h, self.t.h_o.at[li], self.t.hsem.at[0])

    def z_copy(self, s):
        li, f, b = self.at(s)
        return local(self.t.z.at[b], self.t.z_rows(li, f), self.t.zsem.at[b])

    def image(self, src, i):
        return local(src, self.t.img, self.t.isem.at[i])

    def prologue(self):
        self.image(self.x, 0).start()
        self.w.load(*self.at(0))

    def take_x(self):
        t = self.t
        self.image(self.x, 0).wait()
        for i, rows in t.images():
            t.acc[rows] = t.img[i].astype(F32)
        self.image(self.y, 1).start()
        for rows in t.small:
            t.h[rows] = t.acc[rows].astype(BF)
        self.h_copy(0).start()

    def block(self, s):
        t = self.t
        at = li, f, b = self.at(s)
        self.w.ready(*at)
        when(s + 1 < t.n)(lambda: self.w.load(*self.at(s + 1)))
        when(s > 1)(lambda: self.z_copy(s).wait())
        wi, wo = self.w.w_in(*at), self.w.w_out(*at)
        for rows in t.tiles(FT):
            z = dg(t.h[rows], wi, 1, 0).astype(BF)
            t.z[b, rows] = z
            t.a[rows] = gelu(z.astype(F32)).astype(BF)
        self.z_copy(s).start()
        for rows in t.tiles(FT):
            t.acc[rows] = t.acc[rows] + dg(t.a[rows], wo, 1, 0)
        when(f == t.nf - 1)(functools.partial(self.layer_end, li))

    def layer_end(self, li):
        t = self.t
        self.h_copy(0).wait()

        @when(li < t.nl - 1)
        def _():
            for rows in t.small:
                h = t.acc[rows].astype(BF)
                t.h[rows] = h
                t.acc[rows] = h.astype(F32)
            self.h_copy(li + 1).start()

        @when(li == t.nl - 1)
        def _():
            self.image(self.y, 1).wait()
            for i, rows in t.images():
                t.acc[rows] = t.acc[rows].astype(BF).astype(F32) - t.img[i].astype(F32)
            t.loss[...] = jnp.zeros_like(t.loss)
            for rows in t.small:
                err = t.acc[rows]
                q = err.astype(BF)
                t.h[rows] = q
                t.acc[rows] = q.astype(F32)
                sq = jnp.sum((err * err).reshape(PC * 7 // SUB, SUB, D), axis=0)
                for c in range(0, D, LANE):
                    t.loss[...] += sq[:, c : c + LANE]

    def epilogue(self):
        wait([self.z_copy(s) for s in TWO])


class Backward:
    def __init__(self, acts, weights):
        self.t, self.w = acts, weights

    def at(self, s):
        t = self.t
        return t.nl - 1 - div(s, t.nf), rem(s, t.nf), rem(s, 2)

    def h_load(self, li):
        i = rem(li, 2)
        return local(self.t.h_o.at[li], self.t.hb.at[i], self.t.hsem.at[i])

    def z_load(self, s):
        li, f, b = self.at(s)
        return local(self.t.z_rows(li, f), self.t.z.at[b], self.t.zsem.at[b])

    def load(self, s):
        self.z_load(s).start()
        self.w.load(*self.at(s))

    def prologue(self):
        self.load(0)
        self.h_load(self.t.nl - 1).start()

    def out_block(self, s, dst):
        t = self.t
        at = li, f, b = self.at(s)
        self.z_load(s).wait()
        self.w.ready(*at)
        when(s + 1 < t.n)(lambda: self.load(s + 1))

        @when(f == 0)
        def _():
            self.h_load(li).wait()
            when(li > 0)(lambda: self.h_load(li - 1).start())

        wo = self.w.w_out(*at)
        for rows in t.tiles(BT):
            a, slope = gelu_parts(t.z[b, rows].astype(F32))
            t.a[rows] = a.astype(BF)
            t.p[rows] = (dg(t.h[rows], wo, 1, 1) * slope).astype(BF)
        dst[...] = dg(t.a[...], t.h[...], 0, 0)

    def in_block(self, s, dst):
        t = self.t
        at = li, f, b = self.at(s)
        dst[...] = dg(t.hb[rem(li, 2)], t.p[...], 0, 0)

        @when(li > 0)
        def _():
            wi = self.w.w_in(*at)
            for rows in t.tiles(BT):
                t.acc[rows] = t.acc[rows] + dg(t.p[rows], wi, 1, 1)

            @when(f == t.nf - 1)
            def _():
                for rows in t.small:
                    q = t.acc[rows].astype(BF)
                    t.h[rows] = q
                    t.acc[rows] = q.astype(F32)


class Owned:
    AHEAD = 4

    def __init__(self, g, n, nf, layer, mats, dst, sem):
        self.g, self.n, self.nf, self.layer, self.mats, self.dst, self.sem = g, n, nf, layer, mats, dst, sem

    def due(self, s):
        g = self.g
        sem = self.sem.at[rem(s, self.AHEAD)]

        @when(both(g.sink, s < self.n + self.AHEAD))
        def _():
            @when(s >= self.AHEAD)
            def _():
                for T in TYPES:
                    local(self.dst[T].at[0], self.dst[T].at[0], sem).wait()

            @when(s < self.n)
            def _():
                for T in TYPES:
                    for ab in AB:
                        rows, col = g.fin(T, ab, True)
                        local(region(self.mats, T, self.layer(div(s, self.nf)), rem(s, self.nf), rows, col), self.dst[T].at[s, ab], sem).start()


def step_kernel(ns, nsl, lags, glags, scale, rho, lr, x, y, w_out, w_in, out_o, out_i, loss, h_o, z_o, *refs):
    def take(n):
        nonlocal refs
        mine, refs = refs[:n], refs[n:]
        return mine

    g = Geo()
    g.greet()
    mats = w_out, w_in
    acts = Acts((h_o, z_o), take(11))
    blocks = Weights(mats, take(3))
    whole = vo, vi = take(2)
    sc_bufs, ga_bufs = take(13), take(3)
    own, w_p, pieces = take(2), take(2), take(2)
    sq, wsem = take(2)
    norm = PairSum((g.partner, g.xn, g.yn, g.far), take(4))
    total = PairSum((g.partner, g.xn, g.yn, g.z1, g.z2), take(4))
    n, nf = acts.n, acts.nf
    last_first = lambda q: acts.nl - 1 - q

    fw = Forward(acts, x, y, blocks)
    fw.prologue()
    fw.take_x()

    def forward_step(s, _):
        fw.block(s)
        return 0

    lax.fori_loop(0, n, forward_step, 0)
    fw.epilogue()

    g.meet()
    sq[...] = jnp.zeros_like(sq)
    bw = Backward(acts, blocks)
    bw.prologue()
    owned = Owned(g, n, nf, last_first, mats, w_p, wsem)

    def keep_sums(T, k, ab, val):
        val = val * scale
        own[T][k, ab] = val
        sq[...] += val * val

    def add_up(bw, sc, s, j):
        block = bw.in_block if j else bw.out_block

        @when(s < n)
        def _():
            block(s, sc.S[j].at[rem(s, nsl)])
            sc.begin(j, s)

        sc.due(s, j)

    sc = Scatter(g, n, ns, nsl, lags, sc_bufs, keep_sums)

    def first_sums(s, _):
        owned.due(s)
        for j in TWO:
            add_up(bw, sc, s, j)
        return 0

    lax.fori_loop(0, sc.steps(), first_sums, 0)

    fw = Forward(acts, x, y, Whole(vo, vi))
    fw.prologue()

    @when(g.sink)
    def _():
        quarters = [sq[i * SUB : (i + 1) * SUB, j * LANE : (j + 1) * LANE] for i in TWO for j in TWO]
        norm.part[0] = sum(quarters[1:], quarters[0])
        norm.now()
        sq[...] = jnp.broadcast_to(rho / jnp.sqrt(jnp.broadcast_to(jnp.sum(norm.part[4]), (1, 1))), sq.shape)

    def piece(k):
        of = last_first(div(k, nf)) * nf + rem(k, nf)

        @when(both(g.sink, k < n))
        def _():
            for T in TYPES:
                for ab in AB:
                    pieces[T][k, ab] = (w_p[T][of, ab] + sq[...] * own[T][of, ab]).astype(BF)

    ga = Gather(g, n, nf, lambda q: q, glags, pieces, whole, ga_bufs)
    lead = (ga.mu3 + 1) // 2
    piece(0)

    def gather_step(s, _):
        piece(s + 1)
        ga.due(s, 0)
        when(s == 1)(fw.take_x)
        when(both(s >= lead, s < lead + n))(lambda: fw.block(s - lead))
        ga.due(s, 1)
        return 0

    lax.fori_loop(0, ga.steps(), gather_step, 0)
    fw.epilogue()

    bw2 = Backward(acts, Whole(vo, vi))
    bw2.prologue()
    total.part[0] = acts.loss[...]

    def update(T, k, ab, val):
        w_p[T][k, ab] = w_p[T][k, ab] - lr * (val * scale)

    sc2 = Scatter(g, n, ns, nsl, lags, sc_bufs, update)
    ga2 = Gather(g, n, nf, last_first, glags, w_p, (out_o, out_i), ga_bufs, sc2.lam4 + 1)

    def second_sums(s, _):
        owned.due(s)
        for j in TWO:
            add_up(bw2, sc2, s, j)
            ga2.due(s, j)
        total.due(s)
        return 0

    lax.fori_loop(0, ga2.steps(), second_sums, 0)
    loss[0, 0] = HALF * (jnp.sum(total.part[5]) * scale)


def sam_step(x, y, w_out, w_in, scale, rho, lr, ns=4, nsl=12, lags=(1, 4, 4, 4), glags=(4, 4, 4, 3), ngs=12):
    nl, dff, _ = w_out.shape
    images, rows, _ = x.shape
    tok = images * rows
    n = nl * dff // BLK
    S = jax.ShapeDtypeStruct
    piece = lambda dt: [scratch(dt, n, 2, PC, BLK)] * 2
    bufs = Acts.scratch(images, rows) + Weights.scratch() + [scratch(BF, nl, dff, D), scratch(BF, nl, D, dff)]
    bufs += Scatter.scratch(ns, nsl) + Gather.scratch(n, ngs) + piece(F32) + piece(F32) + piece(BF)
    bufs += [scratch(F32, PC, BLK), DMA((Owned.AHEAD,))] + PairSum.scratch(4) + PairSum.scratch(5)
    return pl.pallas_call(
        functools.partial(step_kernel, ns, nsl, lags, glags, scale, rho, lr),
        out_shape=[S(w_out.shape, F32), S(w_in.shape, F32), S((1, 1), F32), S((nl, tok, D), BF), S((nl, tok, dff), BF)],
        in_specs=[HBM] * 4,
        out_specs=[HBM] * 2 + [pl.BlockSpec(memory_space=pltpu.SMEM)] + [HBM] * 2,
        scratch_shapes=bufs,
        cost_estimate=pl.CostEstimate(flops=tok * D * dff * nl * 24, bytes_accessed=200 * MIB, transcendentals=0),
        compiler_params=pltpu.CompilerParams(collective_id=1, has_side_effects=True, vmem_limit_bytes=67043328),
        name="sam_step",
    )(x, y, w_out, w_in)


def solution(mesh):
    n_dev = mesh.shape["data"]

    def local_step(x_loc, y_loc, w_in, w_out):
        nl, d_model, d_ff = w_in.shape
        scale = 1.0 / (x_loc.shape[0] * n_dev * x_loc.shape[1] * d_model)
        rho = RHO_FRAC * math.sqrt(nl * (d_model + d_ff))
        new_out, new_in, loss, _, _ = sam_step(x_loc, y_loc, w_out, w_in, scale, rho, LEARN_RATE)
        return new_in, new_out, loss.reshape(())

    specs = P("data"), P("data"), P(), P()
    return jax.shard_map(local_step, mesh=mesh, in_specs=specs, out_specs=(P(), P(), P()), check_vma=False)
```

```python
import functools
import math

import jax
import jax.numpy as jnp
from jax import lax
from jax.experimental import pallas as pl
from jax.experimental.pallas import tpu as pltpu
from jax.sharding import PartitionSpec as P

MESH = pl.DeviceIdType.MESH
F32, BF = jnp.float32, jnp.bfloat16
RHO_FRAC = 0.1
LEARN_RATE = 1.0
D = 512
BLK = 256
PC = 16
FT = 224
BT = 1568
SUB, LANE = 8, 128
NZ = 4
HALF = 0.5
MIB = 2**20
GELU_A = math.sqrt(2.0 / math.pi)
GELU_B = 0.044715
TWO = AB = TYPES = DIRS = (0, 1)
SHAPES = ((BLK, D), (D, BLK))
ANY = pl.BlockSpec(memory_space=pl.ANY)
HBM = pl.BlockSpec(memory_space=pltpu.HBM)
VM = pl.BlockSpec(memory_space=pltpu.VMEM)
DMA = pltpu.SemaphoreType.DMA
rem, div = lax.rem, lax.div
when = pl.when


def both(*conds):
    return functools.reduce(jnp.logical_and, conds)


def ds(start, size):
    return pl.ds(pl.multiple_of(start, SUB), size)


def cols(f):
    return pl.ds(pl.multiple_of(f * BLK, BLK), BLK)


def dg(a, b, ca, cb):
    return lax.dot_general(a, b, (((ca,), (cb,)), ((), ())), preferred_element_type=F32)


def scratch(dtype, *shape):
    return pltpu.VMEM(shape, dtype)


def local(src, dst, sem):
    return pltpu.make_async_copy(src, dst, sem)


def start(copies):
    for c in copies:
        c.start()


def wait(copies):
    for c in copies:
        c.wait()


class Geo:
    def __init__(self):
        me = lax.axis_index("data")
        flip = lambda step: me + step - 2 * step * rem(me // step, 2)
        self.me = me
        self.c, self.x, self.y, self.z = [rem(me // step, n) for step, n in ((1, 2), (2, 2), (4, 2), (8, NZ))]
        self.partner, self.xn, self.yn, self.z1, self.z2 = [flip(1 << k) for k in range(5)]
        self.zm, self.zp = me - 8, me + 8
        self.e = self.z // (NZ - 1)
        self.sink = rem(self.z, NZ - 1) == 0
        self.w = (self.x, self.y)
        self.w2 = (self.y, self.x)
        self.n1 = (self.xn, self.yn)
        self.n2 = (self.yn, self.xn)

    def place(self, dirn):
        return self.z if dirn else NZ - 1 - self.z

    def greet(self):
        self.bar = pltpu.get_barrier_semaphore()
        hello = lambda dev: pl.semaphore_signal(self.bar, device_id=(dev,), device_id_type=MESH)
        for dev in (self.partner, self.xn, self.yn, self.z2):
            hello(dev)
        when(self.z > 0)(lambda: hello(self.zm))
        when(self.z < NZ - 1)(lambda: hello(self.zp))
        known = 1, 2, 4
        rest = [d for d in range(1, 16) if d not in known]
        when(self.sink)(lambda: [hello(self.mirror(d)) for d in rest] and None)
        self.sink_hellos = len(rest)

    def mirror(self, d):
        flips = (1 - 2 * self.c, 2 - 4 * self.x, 4 - 8 * self.y, 24 - 48 * self.e)
        return self.me + sum(flip for i, flip in enumerate(flips) if d >> i & 1)

    def meet(self):
        when(self.sink)(lambda: pl.semaphore_wait(self.bar, 5 + self.sink_hellos))
        when(jnp.logical_not(self.sink))(lambda: pl.semaphore_wait(self.bar, 6))

    def half(self, T, c):
        R = SHAPES[T][0]
        return ds(c * (R // 2), R // 2)

    def part(self, T, ab, w):
        R = SHAPES[T][0]
        return self.c * (R // 2) + ab * (R // 4) + w * (R // 8)

    def zrow(self, T, ab, e):
        return self.part(T, ab, self.w[ab]) + e * (SHAPES[T][0] // 16)

    def fin(self, T, ab, mine):
        row = self.zrow(T, ab, self.e)
        w = self.w2[ab] if mine else 1 - self.w2[ab]
        if T:
            return ds(row + w * PC, PC), slice(None)
        return ds(row, PC), cols(w)


def region(out, T, li, f, rows, col=None):
    if T:
        return out[T].at[li, rows, cols(f)]
    return out[T].at[li, ds(f * BLK + rows.start, rows.size), slice(None) if col is None else col]


def schedule(s, j, lag, T):
    d = j - T - lag
    return None if d % 2 else s + d // 2


def run(k, n, what, T, *more):
    if k is not None:
        when(both(k >= 0, k < n))(functools.partial(what, T, k, *more))


class Scatter:
    FLOWS = FD, F1, F3, FM, FP = range(0, 10, 2)
    CREDITS = CD, C1, C3, CM, CP = range(0, 10, 2)

    def __init__(self, g, n, ns, nsl, lags, bufs, deliver):
        self.g, self.n, self.ns, self.nsl, self.deliver = g, n, ns, nsl, deliver
        self.S, self.rD, self.r1, self.rz, self.r3 = [bufs[2 * i : 2 * i + 2] for i in range(5)]
        self.ssem, self.rsem, self.cred = bufs[10:]
        ld, l1, self.lz, l3 = lags
        self.lam1 = ld
        self.lam2 = ld + l1
        self.lam4 = self.lam2 + (NZ - 1) * self.lz + l3

    @staticmethod
    def scratch(ns, nsl):
        out = []
        for lead, div, div2 in (((nsl,), 1, 1), ((ns,), 2, 1), ((ns, 2), 8, 1), ((ns, 2, 2), 16, 1), ((ns, 2), 0, 0)):
            for R, C in SHAPES:
                out.append(scratch(F32, *lead, *((R // div, C) if div else (PC, BLK))))
        return out + [DMA((2, 10, ns))] * 2 + [pltpu.SemaphoreType.REGULAR((2, 10))]

    def copy(self, T, flow, k, src, dst, dev):
        i = (T, flow, rem(k, self.ns))
        return pltpu.make_async_remote_copy(src, dst, self.ssem.at[i], self.rsem.at[i], device_id=(dev,), device_id_type=MESH)

    def take(self, T, credit, k):
        when(k >= self.ns)(lambda: pl.semaphore_wait(self.cred.at[T, credit]))

    def give(self, T, credit, k, dev):
        when(k + self.ns < self.n)(lambda: pl.semaphore_signal(self.cred.at[T, credit], device_id=(dev,), device_id_type=MESH))

    def slots(self, k):
        return rem(k, self.nsl), rem(k, self.ns)

    def to_core(self, T, k):
        s, q = self.slots(k)
        return self.copy(T, self.FD, k, self.S[T].at[s, self.g.half(T, 1 - self.g.c)], self.rD[T].at[q], self.g.partner)

    def first(self, T, k, ab):
        s, q = self.slots(k)
        rows = ds(self.g.part(T, ab, 1 - self.g.w[ab]), SHAPES[T][0] // 8)
        return self.copy(T, self.F1 + ab, k, self.S[T].at[s, rows], self.r1[T].at[q, ab], self.g.n1[ab])

    def zrows(self, T, ab, e):
        return ds(self.g.zrow(T, ab, e), SHAPES[T][0] // 16)

    def along(self, T, k, dirn, ab):
        s, q = self.slots(k)
        flow = (self.FP if dirn else self.FM) + ab
        src = self.S[T].at[s, self.zrows(T, ab, dirn)]
        return self.copy(T, flow, k, src, self.rz[T].at[q, ab, dirn], self.g.zp if dirn else self.g.zm)

    def last(self, T, k, ab):
        s, q = self.slots(k)
        return self.copy(T, self.F3 + ab, k, self.S[T].at[(s, *self.g.fin(T, ab, False))], self.r3[T].at[q, ab], self.g.n2[ab])

    def add(self, T, k, rows, val):
        s, _ = self.slots(k)
        self.S[T][s, rows] = self.S[T][s, rows] + val

    def begin(self, T, k):
        self.take(T, self.CD, k)
        self.to_core(T, k).start()

    def after_core(self, T, k):
        g = self.g
        self.to_core(T, k).wait()
        self.add(T, k, g.half(T, g.c), self.rD[T][rem(k, self.ns)])
        self.give(T, self.CD, k, g.partner)
        for ab in AB:
            self.take(T, self.C1 + ab, k)
            self.first(T, k, ab).start()

    def after_first(self, T, k):
        g = self.g
        for ab in AB:
            self.first(T, k, ab).wait()
        for ab in AB:
            self.add(T, k, ds(g.part(T, ab, g.w[ab]), SHAPES[T][0] // 8), self.r1[T][rem(k, self.ns), ab])
            self.give(T, self.C1 + ab, k, g.n1[ab])

    def line(self, T, k, dirn):
        g = self.g
        p = g.place(dirn)
        credit = self.CP if dirn else self.CM

        @when(k < self.n)
        def _():
            @when(p > 0)
            def _():
                for ab in AB:
                    self.along(T, k, dirn, ab).wait_recv()
                for ab in AB:
                    self.add(T, k, self.zrows(T, ab, dirn), self.rz[T][rem(k, self.ns), ab, dirn])
                self.give(T, credit, k, g.zm if dirn else g.zp)

            @when(p < NZ - 1)
            def _():
                self.take(T, credit, k)
                for ab in AB:
                    self.along(T, k, dirn, ab).start()

            @when(p == NZ - 1)
            def _():
                for ab in AB:
                    self.take(T, self.C3 + ab, k)
                    self.last(T, k, ab).start()

        @when(both(k > 0, p < NZ - 1))
        def _():
            for ab in AB:
                self.along(T, k - 1, dirn, ab).wait_send()

    def after_last(self, T, k):
        g = self.g

        @when(g.sink)
        def _():
            s, q = self.slots(k)
            for ab in AB:
                self.last(T, k, ab).wait()
            for ab in AB:
                self.deliver(T, k, ab, self.S[T][(s, *g.fin(T, ab, True))] + self.r3[T][q, ab])
                self.give(T, self.C3 + ab, k, g.n2[ab])

    def due(self, s, j):
        for T in TYPES:
            run(schedule(s, j, self.lam4, T), self.n, self.after_last, T)
        for T in TYPES:
            k = schedule(s, j, self.lam2, T)
            run(k, self.n, self.after_first, T)
            if k is not None:
                for dirn in DIRS:
                    run(k - self.g.place(dirn) * (self.lz // 2), self.n + 1, self.line, T, dirn)
        for T in TYPES:
            run(schedule(s, j, self.lam1, T), self.n, self.after_core, T)

    def steps(self):
        return self.n + (self.lam4 + 1) // 2 + 1


class Gather:
    FLOWS = F3, FM, FP, FE0, FE1, FD = range(6)

    def __init__(self, g, n, nf, layer, lags, own, out, sems, start=0):
        self.g, self.n, self.nf, self.layer, self.own, self.out = g, n, nf, layer, own, out
        self.ssem, self.rsem, self.lsem = sems
        self.ns = self.ssem.shape[-1]
        l3, self.lz, le, ld = lags
        self.mu0 = start
        self.mu1 = start + l3
        self.mu2 = self.mu1 + (NZ - 1) * self.lz + le
        self.mu3 = self.mu2 + ld

    @staticmethod
    def scratch(n, ns):
        return [DMA((2, 6, ns)), DMA((2, 6, n)), DMA((2, 2, ns))]

    def region(self, T, k, rows, col=None):
        return region(self.out, T, self.layer(div(k, self.nf)), rem(k, self.nf), rows, col)

    def rows(self, T, k, row, div):
        return self.region(T, k, ds(row, SHAPES[T][0] // div))

    def copy(self, T, flow, k, src, dst, dev):
        return pltpu.make_async_remote_copy(src, dst, self.ssem.at[T, flow, rem(k, self.ns)], self.rsem.at[T, flow, k],
            device_id=(dev,), device_id_type=MESH)

    def keep(self, T, k, ab):
        rows, col = self.g.fin(T, ab, True)
        return local(self.own[T].at[k, ab], self.region(T, k, rows, col), self.lsem.at[T, ab, rem(k, self.ns)])

    def begin(self, T, k):
        g = self.g

        @when(g.sink)
        def _():
            for ab in AB:
                rows, col = g.fin(T, ab, True)
                self.keep(T, k, ab).start()
                self.copy(T, self.F3, k, self.own[T].at[k, ab], self.region(T, k, rows, col), g.n2[ab]).start()

    def over(self, T, flow, k, ref, send=True, recv=True):
        if send:
            local(ref, ref, self.ssem.at[T, flow, rem(k, self.ns)]).wait()
        if recv:
            local(ref, ref, self.rsem.at[T, flow, k]).wait()

    def line(self, T, k, dirn):
        g = self.g
        p = g.place(dirn)
        e = 1 - dirn
        flow = self.FP if dirn else self.FM
        pair = lambda k: self.rows(T, k, 0, 8)

        @when(k < self.n)
        def _():
            @when(p == 0)
            def _():
                for ab in AB:
                    self.keep(T, k, ab).wait()
                self.over(T, self.F3, k, self.own[T].at[k])

            when(p > 0)(lambda: self.over(T, flow, k, pair(k), send=False))
            parts = [self.rows(T, k, g.zrow(T, ab, e), 16) for ab in AB]

            @when(p < NZ - 1)
            def _():
                for r in parts:
                    self.copy(T, flow, k, r, r, g.zp if dirn else g.zm).start()

            for ab in AB:
                self.copy(T, self.FE0 + e, k, parts[ab], parts[ab], g.n1[ab]).start()

        when(both(k > 0, p < NZ - 1))(lambda: self.over(T, flow, k - 1, pair(k - 1), recv=False))

    def to_core(self, T, k):
        r = self.region(T, k, self.g.half(T, self.g.c))
        return self.copy(T, self.FD, k, r, r, self.g.partner)

    def after_first(self, T, k):
        for e in TWO:
            self.over(T, self.FE0 + e, k, self.rows(T, k, 0, 8))
        self.to_core(T, k).start()

    def done(self, T, k):
        self.to_core(T, k).wait()

    def due(self, s, j):
        for T in TYPES:
            run(schedule(s, j, self.mu0, T), self.n, self.begin, T)
        for T in TYPES:
            k = schedule(s, j, self.mu1, T)
            if k is not None:
                for dirn in DIRS:
                    run(k - self.g.place(dirn) * (self.lz // 2), self.n + 1, self.line, T, dirn)
        for T in TYPES:
            run(schedule(s, j, self.mu2, T), self.n, self.after_first, T)
            run(schedule(s, j, self.mu3, T), self.n, self.done, T)

    def steps(self):
        return self.n + (self.mu3 + 1) // 2 + 1


class PairSum:
    GAP = 3

    def __init__(self, devs, bufs):
        self.devs = devs
        self.part, self.nbr, self.ssem, self.rsem = bufs

    @staticmethod
    def scratch(n):
        return [scratch(F32, n + 1, SUB, LANE), scratch(F32, n, SUB, LANE), DMA((n,)), DMA((n,))]

    def copy(self, r):
        return pltpu.make_async_remote_copy(self.part.at[r], self.nbr.at[r], self.ssem.at[r], self.rsem.at[r],
            device_id=(self.devs[r],), device_id_type=MESH)

    def finish(self, r):
        self.copy(r).wait()
        self.part[r + 1] = self.part[r] + self.nbr[r]

    def due(self, s):
        for r in range(len(self.devs)):
            when(s == r * self.GAP)(lambda: self.copy(r).start())
            when(s == r * self.GAP + self.GAP - 1)(lambda: self.finish(r))


def gelu(z):
    return z * (HALF + HALF * jnp.tanh(z * (GELU_A + (GELU_A * GELU_B) * (z * z))))


def gelu_parts(z):
    zz = z * z
    half = HALF + HALF * jnp.tanh(z * (GELU_A + (GELU_A * GELU_B) * zz))
    slope = half + (z * (half - half * half)) * (2 * GELU_A + (6 * GELU_A * GELU_B) * zz)
    return z * half, slope


AHEAD = 2


class Weights:
    def __init__(self, mats, bufs):
        self.wo_h, self.wi_h = mats
        self.wo, self.wi, self.sem = bufs

    @staticmethod
    def scratch():
        return [scratch(F32, AHEAD + 1, BLK, D), scratch(F32, AHEAD + 1, D, BLK), DMA((2, AHEAD + 1))]

    def loads(self, li, f, b):
        return [local(self.wo_h.at[li, cols(f)], self.wo.at[b], self.sem.at[0, b]), local(self.wi_h.at[li, :, cols(f)], self.wi.at[b], self.sem.at[1, b])]

    def load(self, *at):
        start(self.loads(*at))

    def ready(self, *at):
        wait(self.loads(*at))

    def w_out(self, li, f, b):
        return self.wo[b].astype(BF)

    def w_in(self, li, f, b):
        return self.wi[b].astype(BF)


class Whole:
    def __init__(self, vo, vi):
        self.vo, self.vi = vo, vi

    def load(self, *at):
        pass

    ready = load

    def w_out(self, li, f, b):
        return self.vo[li, cols(f)]

    def w_in(self, li, f, b):
        return self.vi[li, :, cols(f)]


class Acts:
    def __init__(self, hbm, bufs):
        self.h_o, self.z_o = hbm
        self.h, self.hb, self.acc, self.a, self.p, self.z, self.y, self.loss, self.hsem, self.zsem, self.isem = bufs
        self.nl, self.tok, dff = self.z_o.shape
        self.nf = dff // BLK
        self.n = self.nl * self.nf
        self.small = [pl.ds(r, PC * 7) for r in range(0, self.tok, PC * 7)]

    @staticmethod
    def scratch(tok):
        return [scratch(BF, tok, D), scratch(BF, 2, tok, D), scratch(F32, tok, D), scratch(BF, tok, BLK), scratch(BF, tok, BLK),
                scratch(BF, 2, tok, BLK), scratch(BF, tok, D), scratch(F32, SUB, LANE), DMA((2,)), DMA((2,)), DMA((2,))]

    def tiles(self, size):
        return [pl.ds(r, size) for r in range(0, self.tok, size)]

    def z_rows(self, li, f):
        return self.z_o.at[li, :, cols(f)]


class Forward:
    def __init__(self, acts, x, y, weights):
        self.t, self.x, self.y, self.w = acts, x, y, weights

    def at(self, s):
        return div(s, self.t.nf), rem(s, self.t.nf), rem(s, AHEAD + 1)

    def h_copy(self, li):
        return local(self.t.h, self.t.h_o.at[li], self.t.hsem.at[0])

    def z_copy(self, s):
        li, f, _ = self.at(s)
        b = rem(s, 2)
        return local(self.t.z.at[b], self.t.z_rows(li, f), self.t.zsem.at[b])

    def x_load(self):
        return local(self.x, self.t.h, self.t.isem.at[0])

    def y_load(self):
        return local(self.y, self.t.y, self.t.isem.at[1])

    def prologue(self):
        start([self.x_load(), self.y_load()])
        for s in range(AHEAD):
            self.w.load(*self.at(s))

    def take_x(self):
        t = self.t
        self.x_load().wait()
        for rows in t.small:
            t.acc[rows] = t.h[rows].astype(F32)
        self.h_copy(0).start()

    def block(self, s):
        t = self.t
        at = li, f, _ = self.at(s)
        b = rem(s, 2)
        self.w.ready(*at)
        when(s + AHEAD < t.n)(lambda: self.w.load(*self.at(s + AHEAD)))
        when(s > 1)(lambda: self.z_copy(s).wait())
        wi, wo = self.w.w_in(*at), self.w.w_out(*at)
        for rows in t.tiles(FT):
            z = dg(t.h[rows], wi, 1, 0).astype(BF)
            t.z[b, rows] = z
            t.a[rows] = gelu(z.astype(F32)).astype(BF)
        self.z_copy(s).start()
        for rows in t.tiles(FT):
            t.acc[rows] = t.acc[rows] + dg(t.a[rows], wo, 1, 0)
        when(f == t.nf - 1)(functools.partial(self.layer_end, li))

    def layer_end(self, li):
        t = self.t
        self.h_copy(0).wait()

        @when(li < t.nl - 1)
        def _():
            for rows in t.small:
                h = t.acc[rows].astype(BF)
                t.h[rows] = h
                t.acc[rows] = h.astype(F32)
            self.h_copy(li + 1).start()

        @when(li == t.nl - 1)
        def _():
            self.y_load().wait()
            t.loss[...] = jnp.zeros_like(t.loss)
            for rows in t.small:
                err = t.acc[rows].astype(BF).astype(F32) - t.y[rows].astype(F32)
                q = err.astype(BF)
                t.h[rows] = q
                t.acc[rows] = q.astype(F32)
                sq = jnp.sum((err * err).reshape(PC * 7 // SUB, SUB, D), axis=0)
                for c in range(0, D, LANE):
                    t.loss[...] += sq[:, c : c + LANE]

    def epilogue(self):
        wait([self.z_copy(s) for s in TWO])


class Backward:
    def __init__(self, acts, weights):
        self.t, self.w = acts, weights

    def at(self, s):
        t = self.t
        return t.nl - 1 - div(s, t.nf), rem(s, t.nf), rem(s, AHEAD + 1)

    def h_load(self, li):
        i = rem(li, 2)
        return local(self.t.h_o.at[li], self.t.hb.at[i], self.t.hsem.at[i])

    def z_load(self, s):
        li, f, _ = self.at(s)
        b = rem(s, 2)
        return local(self.t.z_rows(li, f), self.t.z.at[b], self.t.zsem.at[b])

    def prologue(self):
        self.z_load(0).start()
        for s in range(AHEAD):
            self.w.load(*self.at(s))
        self.h_load(self.t.nl - 1).start()

    def out_block(self, s, dst):
        t = self.t
        at = li, f, _ = self.at(s)
        b = rem(s, 2)
        self.z_load(s).wait()
        self.w.ready(*at)
        when(s + 1 < t.n)(lambda: self.z_load(s + 1).start())
        when(s + AHEAD < t.n)(lambda: self.w.load(*self.at(s + AHEAD)))

        @when(f == 0)
        def _():
            self.h_load(li).wait()
            when(li > 0)(lambda: self.h_load(li - 1).start())

        wo = self.w.w_out(*at)
        for rows in t.tiles(BT):
            a, slope = gelu_parts(t.z[b, rows].astype(F32))
            t.a[rows] = a.astype(BF)
            t.p[rows] = (dg(t.h[rows], wo, 1, 1) * slope).astype(BF)
        dst[...] = dg(t.a[...], t.h[...], 0, 0)

    def in_block(self, s, dst):
        t = self.t
        at = li, f, _ = self.at(s)
        dst[...] = dg(t.hb[rem(li, 2)], t.p[...], 0, 0)

        @when(li > 0)
        def _():
            wi = self.w.w_in(*at)
            for rows in t.tiles(BT):
                t.acc[rows] = t.acc[rows] + dg(t.p[rows], wi, 1, 1)

            @when(f == t.nf - 1)
            def _():
                for rows in t.small:
                    q = t.acc[rows].astype(BF)
                    t.h[rows] = q
                    t.acc[rows] = q.astype(F32)


class Owned:
    AHEAD = 4

    def __init__(self, g, n, nf, layer, mats, dst, sem):
        self.g, self.n, self.nf, self.layer, self.mats, self.dst, self.sem = g, n, nf, layer, mats, dst, sem

    def due(self, s):
        g = self.g
        sem = self.sem.at[rem(s, self.AHEAD)]

        @when(both(g.sink, s < self.n + self.AHEAD))
        def _():
            @when(s >= self.AHEAD)
            def _():
                for T in TYPES:
                    local(self.dst[T].at[0], self.dst[T].at[0], sem).wait()

            @when(s < self.n)
            def _():
                for T in TYPES:
                    for ab in AB:
                        rows, col = g.fin(T, ab, True)
                        local(region(self.mats, T, self.layer(div(s, self.nf)), rem(s, self.nf), rows, col), self.dst[T].at[s, ab], sem).start()


def step_kernel(ns, nsl, lags, glags, lags2, glags2, scale, rho, lr, x, y, w_out, w_in, out_o, out_i, loss, h_o, z_o, *refs):
    def take(n):
        nonlocal refs
        mine, refs = refs[:n], refs[n:]
        return mine

    g = Geo()
    g.greet()
    mats = w_out, w_in
    acts = Acts((h_o, z_o), take(11))
    blocks = Weights(mats, take(3))
    whole = vo, vi = take(2)
    sc_bufs, ga_bufs = take(13), take(3)
    own, w_p, pieces = take(2), take(2), take(2)
    sq, wsem = take(2)
    shares, ssem, rsem = take(3)
    total = PairSum((g.partner, g.xn, g.yn, g.z1, g.z2), take(4))
    n, nf = acts.n, acts.nf
    last_first = lambda q: acts.nl - 1 - q

    fw = Forward(acts, x, y, blocks)
    fw.prologue()
    fw.take_x()

    def forward_step(s, _):
        fw.block(s)
        return 0

    lax.fori_loop(0, n, forward_step, 0)
    fw.epilogue()

    g.meet()
    sq[...] = jnp.zeros_like(sq)
    bw = Backward(acts, blocks)
    bw.prologue()
    owned = Owned(g, n, nf, last_first, mats, w_p, wsem)

    def keep_sums(T, k, ab, val):
        val = val * scale
        own[T][k, ab] = val
        sq[...] += val * val

    def add_up(bw, sc, s, j):
        block = bw.in_block if j else bw.out_block

        @when(s < n)
        def _():
            block(s, sc.S[j].at[rem(s, nsl)])
            sc.begin(j, s)

        sc.due(s, j)

    sc = Scatter(g, n, ns, nsl, lags, sc_bufs, keep_sums)

    def first_sums(s, _):
        owned.due(s)
        for j in TWO:
            add_up(bw, sc, s, j)
        return 0

    lax.fori_loop(0, sc.steps(), first_sums, 0)

    fw = Forward(acts, x, y, Whole(vo, vi))
    fw.prologue()

    @when(g.sink)
    def _():
        quarters = [sq[i * SUB : (i + 1) * SUB, j * LANE : (j + 1) * LANE] for i in TWO for j in TWO]
        shares[0] = sum(quarters[1:], quarters[0])
        copies = [pltpu.make_async_remote_copy(shares.at[0], shares.at[d], ssem.at[d], rsem.at[d], device_id=(g.mirror(d),), device_id_type=MESH)
                  for d in range(1, 16)]
        start(copies)
        wait(copies)
        squares = jnp.sum(jnp.sum(shares[...], axis=0))
        sq[...] = jnp.broadcast_to(rho / jnp.sqrt(jnp.broadcast_to(squares, (1, 1))), sq.shape)

    def piece(k):
        of = last_first(div(k, nf)) * nf + rem(k, nf)

        @when(both(g.sink, k < n))
        def _():
            for T in TYPES:
                for ab in AB:
                    pieces[T][k, ab] = (w_p[T][of, ab] + sq[...] * own[T][of, ab]).astype(BF)

    ga = Gather(g, n, nf, lambda q: q, glags, pieces, whole, ga_bufs)
    lead = (ga.mu3 + 1) // 2
    piece(0)

    def gather_step(s, _):
        piece(s + 1)
        ga.due(s, 0)
        when(s == 1)(fw.take_x)
        when(both(s >= lead, s < lead + n))(lambda: fw.block(s - lead))
        ga.due(s, 1)
        return 0

    lax.fori_loop(0, ga.steps(), gather_step, 0)
    fw.epilogue()

    bw2 = Backward(acts, Whole(vo, vi))
    bw2.prologue()
    total.part[0] = acts.loss[...]

    def update(T, k, ab, val):
        w_p[T][k, ab] = w_p[T][k, ab] - lr * (val * scale)

    sc2 = Scatter(g, n, ns, nsl, lags2, sc_bufs, update)
    ga2 = Gather(g, n, nf, last_first, glags2, w_p, (out_o, out_i), ga_bufs, sc2.lam4 + 1)

    def second_sums(s, _):
        owned.due(s)
        for j in TWO:
            add_up(bw2, sc2, s, j)
            ga2.due(s, j)
        total.due(s)
        return 0

    lax.fori_loop(0, ga2.steps(), second_sums, 0)
    loss[0, 0] = HALF * (jnp.sum(total.part[5]) * scale)


def sam_step(x, y, w_out, w_in, scale, rho, lr, ns=4, nsl=12, lags=(1, 4, 4, 4), glags=(4, 4, 4, 3), lags2=(1, 4, 2, 4), glags2=(4, 4, 4, 3), ngs=12):
    nl, dff, _ = w_out.shape
    tok = x.shape[0]
    n = nl * dff // BLK
    S = jax.ShapeDtypeStruct
    piece = lambda dt: [scratch(dt, n, 2, PC, BLK)] * 2
    bufs = Acts.scratch(tok) + Weights.scratch() + [scratch(BF, nl, dff, D), scratch(BF, nl, D, dff)]
    bufs += Scatter.scratch(ns, nsl) + Gather.scratch(n, ngs) + piece(F32) + piece(F32) + piece(BF)
    bufs += [scratch(F32, PC, BLK), DMA((Owned.AHEAD,))] + [scratch(F32, 16, SUB, LANE), DMA((16,)), DMA((16,))] + PairSum.scratch(5)
    return pl.pallas_call(
        functools.partial(step_kernel, ns, nsl, lags, glags, lags2, glags2, scale, rho, lr),
        out_shape=[S(w_out.shape, F32), S(w_in.shape, F32), S((1, 1), F32), S((nl, tok, D), BF), S((nl, tok, dff), BF)],
        in_specs=[HBM] * 4,
        out_specs=[HBM] * 2 + [pl.BlockSpec(memory_space=pltpu.SMEM)] + [HBM] * 2,
        scratch_shapes=bufs,
        cost_estimate=pl.CostEstimate(flops=tok * D * dff * nl * 24, bytes_accessed=200 * MIB, transcendentals=0),
        compiler_params=pltpu.CompilerParams(collective_id=1, has_side_effects=True, vmem_limit_bytes=67043328),
        name="sam_step",
    )(x, y, w_out, w_in)


def solution(mesh):
    n_dev = mesh.shape["data"]

    def local_step(x_loc, y_loc, w_in, w_out):
        nl, d_model, d_ff = w_in.shape
        scale = 1.0 / (x_loc.shape[0] * n_dev * x_loc.shape[1] * d_model)
        rho = RHO_FRAC * math.sqrt(nl * (d_model + d_ff))
        x, y = [v.transpose(1, 0, 2).reshape(-1, d_model) for v in (x_loc, y_loc)]
        new_out, new_in, loss, _, _ = sam_step(x, y, w_out, w_in, scale, rho, LEARN_RATE)
        return new_in, new_out, loss.reshape(())

    specs = P("data"), P("data"), P(), P()
    return jax.shard_map(local_step, mesh=mesh, in_specs=specs, out_specs=(P(), P(), P()), check_vma=False)
```

```python
import functools
import math

import jax
import jax.numpy as jnp
from jax import lax
from jax.experimental import pallas as pl
from jax.experimental.pallas import tpu as pltpu
from jax.sharding import PartitionSpec as P

MESH = pl.DeviceIdType.MESH
F32, BF = jnp.float32, jnp.bfloat16
RHO_FRAC = 0.1
LEARN_RATE = 1.0
D = 512
BLK = 256
PC = 16
FT = 224
BT = 1568
SUB, LANE = 8, 128
NZ = 4
INSIDE = (1,)
HALF = 0.5
MIB = 2**20
GELU_A = math.sqrt(2.0 / math.pi)
GELU_B = 0.044715
TWO = AB = TYPES = DIRS = (0, 1)
SHAPES = ((BLK, D), (D, BLK))
ANY = pl.BlockSpec(memory_space=pl.ANY)
HBM = pl.BlockSpec(memory_space=pltpu.HBM)
VM = pl.BlockSpec(memory_space=pltpu.VMEM)
DMA = pltpu.SemaphoreType.DMA
rem, div = lax.rem, lax.div
when = pl.when


def both(*conds):
    return functools.reduce(jnp.logical_and, conds)


def ds(start, size):
    return pl.ds(pl.multiple_of(start, SUB), size)


def cols(f):
    return pl.ds(pl.multiple_of(f * BLK, BLK), BLK)


def dg(a, b, ca, cb):
    return lax.dot_general(a, b, (((ca,), (cb,)), ((), ())), preferred_element_type=F32)


def scratch(dtype, *shape):
    return pltpu.VMEM(shape, dtype)


def local(src, dst, sem):
    return pltpu.make_async_copy(src, dst, sem)


def start(copies):
    for c in copies:
        c.start()


def wait(copies):
    for c in copies:
        c.wait()


class Geo:
    def __init__(self):
        me = lax.axis_index("data")
        flip = lambda step: me + step - 2 * step * rem(me // step, 2)
        self.me = me
        self.c, self.x, self.y, self.z = [rem(me // step, n) for step, n in ((1, 2), (2, 2), (4, 2), (8, NZ))]
        self.partner, self.xn, self.yn, self.z1, self.z2 = [flip(1 << k) for k in range(5)]
        self.zm, self.zp = me - 8, me + 8
        self.e = self.z // 2
        self.sink = rem(self.z, NZ - 1) == 0
        self.inner = jnp.logical_not(self.sink)
        self.outward = self.me + 16 * self.e - 8
        self.inward = self.me + 8 - 16 * self.e
        self.across = self.inward
        self.w = (self.x, self.y)
        self.w2 = (self.y, self.x)
        self.n1 = (self.xn, self.yn)
        self.n2 = (self.yn, self.xn)

    def place(self, dirn):
        return self.z if dirn else NZ - 1 - self.z

    def greet(self):
        self.bar = pltpu.get_barrier_semaphore()
        hello = lambda dev: pl.semaphore_signal(self.bar, device_id=(dev,), device_id_type=MESH)
        for dev in (self.partner, self.xn, self.yn, self.z2):
            hello(dev)
        when(self.z > 0)(lambda: hello(self.zm))
        when(self.z < NZ - 1)(lambda: hello(self.zp))
        known = 1, 2, 4
        rest = [d for d in range(1, 16) if d not in known]
        when(self.sink)(lambda: [hello(self.mirror(d)) for d in rest] and None)
        self.sink_hellos = len(rest)

    def mirror(self, d):
        flips = (1 - 2 * self.c, 2 - 4 * self.x, 4 - 8 * self.y, 24 - 48 * self.e)
        return self.me + sum(flip for i, flip in enumerate(flips) if d >> i & 1)

    def meet(self):
        when(self.sink)(lambda: pl.semaphore_wait(self.bar, 5 + self.sink_hellos))
        when(self.inner)(lambda: pl.semaphore_wait(self.bar, 6))

    def half(self, T, c):
        R = SHAPES[T][0]
        return ds(c * (R // 2), R // 2)

    def part(self, T, ab, w):
        R = SHAPES[T][0]
        return self.c * (R // 2) + ab * (R // 4) + w * (R // 8)

    def zrow(self, T, ab, e):
        return self.part(T, ab, self.w[ab]) + e * (SHAPES[T][0] // 16)

    def fin(self, T, ab, mine):
        row = self.zrow(T, ab, self.e)
        w = self.w2[ab] if mine else 1 - self.w2[ab]
        if T:
            return ds(row + w * PC, PC), slice(None)
        return ds(row, PC), cols(w)


def region(out, T, li, f, rows, col=None):
    if T:
        return out[T].at[li, rows, cols(f)]
    return out[T].at[li, ds(f * BLK + rows.start, rows.size), slice(None) if col is None else col]


def schedule(s, j, lag, T):
    d = j - T - lag
    return None if d % 2 else s + d // 2


def run(k, n, what, T, *more):
    if k is not None:
        when(both(k >= 0, k < n))(functools.partial(what, T, k, *more))


class Scatter:
    FLOWS = FD, F1, F3, FM, FP, FI = range(0, 12, 2)
    CREDITS = CD, C1, C3, CM, CP = range(0, 10, 2)

    def __init__(self, g, n, ns, nsl, lags, bufs, deliver, inside=()):
        self.g, self.n, self.ns, self.nsl, self.deliver, self.inside = g, n, ns, nsl, deliver, inside
        self.S, self.rD, self.r1, self.rz, self.r3, self.ri = [bufs[2 * i : 2 * i + 2] for i in range(6)]
        self.ssem, self.rsem, self.cred = bufs[12:]
        ld, l1, self.lz, l3 = lags
        self.lam1 = ld
        self.lam2 = ld + l1
        self.lam4 = self.lam2 + (NZ - 1) * self.lz + l3

    @staticmethod
    def scratch(ns, nsl):
        out = []
        for lead, div in (((nsl,), 1), ((ns,), 2), ((ns, 2), 8), ((ns, 2, 2), 16), ((ns, 2), 0), ((ns, 2), 16)):
            for R, C in SHAPES:
                out.append(scratch(F32, *lead, *((R // div, C) if div else (PC, BLK))))
        return out + [DMA((2, 12, ns))] * 2 + [pltpu.SemaphoreType.REGULAR((2, 10))]

    def copy(self, T, flow, k, src, dst, dev):
        i = (T, flow, rem(k, self.ns))
        return pltpu.make_async_remote_copy(src, dst, self.ssem.at[i], self.rsem.at[i], device_id=(dev,), device_id_type=MESH)

    def take(self, T, credit, k):
        when(k >= self.ns)(lambda: pl.semaphore_wait(self.cred.at[T, credit]))

    def give(self, T, credit, k, dev):
        when(k + self.ns < self.n)(lambda: pl.semaphore_signal(self.cred.at[T, credit], device_id=(dev,), device_id_type=MESH))

    def slots(self, k):
        return rem(k, self.nsl), rem(k, self.ns)

    def to_core(self, T, k):
        s, q = self.slots(k)
        return self.copy(T, self.FD, k, self.S[T].at[s, self.g.half(T, 1 - self.g.c)], self.rD[T].at[q], self.g.partner)

    def first(self, T, k, ab):
        s, q = self.slots(k)
        rows = ds(self.g.part(T, ab, 1 - self.g.w[ab]), SHAPES[T][0] // 8)
        return self.copy(T, self.F1 + ab, k, self.S[T].at[s, rows], self.r1[T].at[q, ab], self.g.n1[ab])

    def zrows(self, T, ab, e):
        return ds(self.g.zrow(T, ab, e), SHAPES[T][0] // 16)

    def along(self, T, k, dirn, ab):
        s, q = self.slots(k)
        flow = (self.FP if dirn else self.FM) + ab
        src = self.S[T].at[s, self.zrows(T, ab, dirn)]
        return self.copy(T, flow, k, src, self.rz[T].at[q, ab, dirn], self.g.zp if dirn else self.g.zm)

    def last(self, T, k, ab):
        s, q = self.slots(k)
        return self.copy(T, self.F3 + ab, k, self.S[T].at[(s, *self.g.fin(T, ab, False))], self.r3[T].at[q, ab], self.g.n2[ab])

    def add(self, T, k, rows, val):
        s, _ = self.slots(k)
        self.S[T][s, rows] = self.S[T][s, rows] + val

    def begin(self, T, k):
        self.take(T, self.CD, k)
        self.to_core(T, k).start()

    def after_core(self, T, k):
        g = self.g
        self.to_core(T, k).wait()
        self.add(T, k, g.half(T, g.c), self.rD[T][rem(k, self.ns)])
        self.give(T, self.CD, k, g.partner)
        for ab in AB:
            self.take(T, self.C1 + ab, k)
            self.first(T, k, ab).start()

    def after_first(self, T, k):
        g = self.g
        for ab in AB:
            self.first(T, k, ab).wait()
        for ab in AB:
            self.add(T, k, ds(g.part(T, ab, g.w[ab]), SHAPES[T][0] // 8), self.r1[T][rem(k, self.ns), ab])
            self.give(T, self.C1 + ab, k, g.n1[ab])

    def line(self, T, k, dirn):
        g = self.g
        p = g.place(dirn)
        credit = self.CP if dirn else self.CM

        @when(k < self.n)
        def _():
            @when(p > 0)
            def _():
                for ab in AB:
                    self.along(T, k, dirn, ab).wait_recv()
                for ab in AB:
                    self.add(T, k, self.zrows(T, ab, dirn), self.rz[T][rem(k, self.ns), ab, dirn])
                self.give(T, credit, k, g.zm if dirn else g.zp)

            @when(p < NZ - 1)
            def _():
                self.take(T, credit, k)
                for ab in AB:
                    self.along(T, k, dirn, ab).start()

            @when(p == NZ - 1)
            def _():
                for ab in AB:
                    self.take(T, self.C3 + ab, k)
                    self.last(T, k, ab).start()

        @when(both(k > 0, p < NZ - 1))
        def _():
            for ab in AB:
                self.along(T, k - 1, dirn, ab).wait_send()

    def inner_in(self, T, k, e, ab):
        s, q = self.slots(k)
        src = self.S[T].at[s, self.zrows(T, ab, e)]
        return self.copy(T, (self.FP if e else self.FM) + ab, k, src, self.rz[T].at[q, ab, e], self.g.inward)

    def inner_across(self, T, k, ab):
        s, q = self.slots(k)
        src = self.S[T].at[s, self.zrows(T, ab, 1 - self.g.e)]
        return self.copy(T, self.FI + ab, k, src, self.ri[T].at[q, ab], self.g.across)

    def inner_send(self, T, k):
        every = [(e, ab) for e in DIRS for ab in AB]

        @when(both(self.g.sink, k < self.n))
        def _():
            self.take(T, self.CM, k)
            start([self.inner_in(T, k, e, ab) for e, ab in every])

        @when(both(self.g.sink, k > 0))
        def _():
            for e, ab in every:
                self.inner_in(T, k - 1, e, ab).wait_send()

    def inner_pass(self, T, k):
        q = rem(k, self.ns)

        @when(both(self.g.inner, k < self.n))
        def _():
            for e in DIRS:
                for ab in AB:
                    self.inner_in(T, k, e, ab).wait_recv()
                    self.add(T, k, self.zrows(T, ab, e), self.rz[T][q, ab, e])
            self.give(T, self.CM, k, self.g.outward)
            self.take(T, self.CP, k)
            start([self.inner_across(T, k, ab) for ab in AB])

        @when(both(self.g.inner, k > 0))
        def _():
            for ab in AB:
                self.inner_across(T, k - 1, ab).wait_send()

    def inner_end(self, T, k):
        @when(self.g.inner)
        def _():
            for ab in AB:
                self.inner_across(T, k, ab).wait_recv()
                self.add(T, k, self.zrows(T, ab, self.g.e), self.ri[T][rem(k, self.ns), ab])
            self.give(T, self.CP, k, self.g.across)
            for ab in AB:
                self.take(T, self.C3 + ab, k)
                self.last(T, k, ab).start()

    def after_last(self, T, k):
        g = self.g

        @when(g.inner if T in self.inside else g.sink)
        def _():
            s, q = self.slots(k)
            for ab in AB:
                self.last(T, k, ab).wait()
            for ab in AB:
                self.deliver(T, k, ab, self.S[T][(s, *g.fin(T, ab, True))] + self.r3[T][q, ab])
                self.give(T, self.C3 + ab, k, g.n2[ab])

    def due(self, s, j):
        for T in TYPES:
            run(schedule(s, j, self.lam4, T), self.n, self.after_last, T)
        for T in TYPES:
            k = schedule(s, j, self.lam2, T)
            run(k, self.n, self.after_first, T)
            if T in self.inside:
                run(k, self.n + 1, self.inner_send, T)
                run(schedule(s, j, self.lam2 + self.lz, T), self.n + 1, self.inner_pass, T)
                run(schedule(s, j, self.lam2 + 2 * self.lz, T), self.n, self.inner_end, T)
            elif k is not None:
                for dirn in DIRS:
                    run(k - self.g.place(dirn) * (self.lz // 2), self.n + 1, self.line, T, dirn)
        for T in TYPES:
            run(schedule(s, j, self.lam1, T), self.n, self.after_core, T)

    def steps(self):
        return self.n + (self.lam4 + 1) // 2 + 1


class Gather:
    FLOWS = F3, FM, FP, FE0, FE1, FD, FO = range(7)

    def __init__(self, g, n, nf, layer, lags, own, out, sems, start=0, inside=()):
        self.g, self.n, self.nf, self.layer, self.own, self.out = g, n, nf, layer, own, out
        self.inside = inside
        self.ssem, self.rsem, self.lsem = sems
        self.ns = self.ssem.shape[-1]
        l3, self.lz, le, ld = lags
        self.mu0 = start
        self.mu1 = start + l3
        self.mu2 = self.mu1 + (NZ - 1) * self.lz + le
        self.mu3 = self.mu2 + ld

    @staticmethod
    def scratch(n, ns):
        return [DMA((2, 7, ns)), DMA((2, 7, n)), DMA((2, 2, ns))]

    def region(self, T, k, rows, col=None):
        return region(self.out, T, self.layer(div(k, self.nf)), rem(k, self.nf), rows, col)

    def rows(self, T, k, row, div):
        return self.region(T, k, ds(row, SHAPES[T][0] // div))

    def copy(self, T, flow, k, src, dst, dev):
        return pltpu.make_async_remote_copy(src, dst, self.ssem.at[T, flow, rem(k, self.ns)], self.rsem.at[T, flow, k],
            device_id=(dev,), device_id_type=MESH)

    def keep(self, T, k, ab):
        rows, col = self.g.fin(T, ab, True)
        return local(self.own[T].at[k, ab], self.region(T, k, rows, col), self.lsem.at[T, ab, rem(k, self.ns)])

    def begin(self, T, k):
        g = self.g

        @when(g.inner if T in self.inside else g.sink)
        def _():
            for ab in AB:
                rows, col = g.fin(T, ab, True)
                self.keep(T, k, ab).start()
                self.copy(T, self.F3, k, self.own[T].at[k, ab], self.region(T, k, rows, col), g.n2[ab]).start()

    def over(self, T, flow, k, ref, send=True, recv=True):
        if send:
            local(ref, ref, self.ssem.at[T, flow, rem(k, self.ns)]).wait()
        if recv:
            local(ref, ref, self.rsem.at[T, flow, k]).wait()

    def line(self, T, k, dirn):
        g = self.g
        p = g.place(dirn)
        e = 1 - dirn
        flow = self.FP if dirn else self.FM
        pair = lambda k: self.rows(T, k, 0, 8)

        @when(k < self.n)
        def _():
            @when(p == 0)
            def _():
                for ab in AB:
                    self.keep(T, k, ab).wait()
                self.over(T, self.F3, k, self.own[T].at[k])

            when(p > 0)(lambda: self.over(T, flow, k, pair(k), send=False))
            parts = [self.rows(T, k, g.zrow(T, ab, e), 16) for ab in AB]

            @when(p < NZ - 1)
            def _():
                for r in parts:
                    self.copy(T, flow, k, r, r, g.zp if dirn else g.zm).start()

            for ab in AB:
                self.copy(T, self.FE0 + e, k, parts[ab], parts[ab], g.n1[ab]).start()

        when(both(k > 0, p < NZ - 1))(lambda: self.over(T, flow, k - 1, pair(k - 1), recv=False))

    def pair(self, T, k):
        return self.rows(T, k, 0, 8)

    def spread(self, T, k, e, *hops):
        g = self.g
        parts = [self.rows(T, k, g.zrow(T, ab, e), 16) for ab in AB]
        for flow, dev in hops:
            start([self.copy(T, flow, k, r, r, dev) for r in parts])
        for ab in AB:
            self.copy(T, self.FE0 + e, k, parts[ab], parts[ab], g.n1[ab]).start()

    def inner_begin(self, T, k):
        g = self.g

        @when(g.inner)
        def _():
            for ab in AB:
                self.keep(T, k, ab).wait()
            self.over(T, self.F3, k, self.own[T].at[k])
            for e in DIRS:
                when(g.e == e)(lambda: self.spread(T, k, e, (self.FP, g.across), (self.FM, g.outward)))

    def inner_pass(self, T, k):
        g = self.g
        for e in DIRS:

            @when(both(g.inner, g.e != e))
            def _():
                self.over(T, self.FP, k, self.pair(T, k), send=False)
                self.spread(T, k, e, (self.FO, g.outward))

            @when(both(g.sink, g.e == e))
            def _():
                self.over(T, self.FM, k, self.pair(T, k), send=False)
                self.spread(T, k, e)

    def inner_end(self, T, k):
        g = self.g
        for e in DIRS:

            @when(both(g.sink, g.e != e))
            def _():
                self.over(T, self.FO, k, self.pair(T, k), send=False)
                self.spread(T, k, e)

    def to_core(self, T, k):
        r = self.region(T, k, self.g.half(T, self.g.c))
        return self.copy(T, self.FD, k, r, r, self.g.partner)

    def after_first(self, T, k):
        for e in TWO:
            self.over(T, self.FE0 + e, k, self.rows(T, k, 0, 8))
        self.to_core(T, k).start()

    def done(self, T, k):
        self.to_core(T, k).wait()
        if T in self.inside:
            for flow in (self.FM, self.FP, self.FO):
                when(self.g.inner)(lambda: self.over(T, flow, k, self.pair(T, k), recv=False))

    def due(self, s, j):
        for T in TYPES:
            run(schedule(s, j, self.mu0, T), self.n, self.begin, T)
        for T in TYPES:
            k = schedule(s, j, self.mu1, T)
            if T in self.inside:
                run(k, self.n, self.inner_begin, T)
                run(schedule(s, j, self.mu1 + self.lz, T), self.n, self.inner_pass, T)
                run(schedule(s, j, self.mu1 + 2 * self.lz, T), self.n, self.inner_end, T)
            elif k is not None:
                for dirn in DIRS:
                    run(k - self.g.place(dirn) * (self.lz // 2), self.n + 1, self.line, T, dirn)
        for T in TYPES:
            run(schedule(s, j, self.mu2, T), self.n, self.after_first, T)
            run(schedule(s, j, self.mu3, T), self.n, self.done, T)

    def steps(self):
        return self.n + (self.mu3 + 1) // 2 + 1


class PairSum:
    GAP = 3

    def __init__(self, devs, bufs):
        self.devs = devs
        self.part, self.nbr, self.ssem, self.rsem = bufs

    @staticmethod
    def scratch(n):
        return [scratch(F32, n + 1, SUB, LANE), scratch(F32, n, SUB, LANE), DMA((n,)), DMA((n,))]

    def copy(self, r):
        return pltpu.make_async_remote_copy(self.part.at[r], self.nbr.at[r], self.ssem.at[r], self.rsem.at[r],
            device_id=(self.devs[r],), device_id_type=MESH)

    def finish(self, r):
        self.copy(r).wait()
        self.part[r + 1] = self.part[r] + self.nbr[r]

    def due(self, s):
        for r in range(len(self.devs)):
            when(s == r * self.GAP)(lambda: self.copy(r).start())
            when(s == r * self.GAP + self.GAP - 1)(lambda: self.finish(r))


def gelu(z):
    return z * (HALF + HALF * jnp.tanh(z * (GELU_A + (GELU_A * GELU_B) * (z * z))))


def gelu_parts(z):
    zz = z * z
    half = HALF + HALF * jnp.tanh(z * (GELU_A + (GELU_A * GELU_B) * zz))
    slope = half + (z * (half - half * half)) * (2 * GELU_A + (6 * GELU_A * GELU_B) * zz)
    return z * half, slope


AHEAD = 2


class Weights:
    def __init__(self, mats, bufs):
        self.wo_h, self.wi_h = mats
        self.wo, self.wi, self.sem = bufs

    @staticmethod
    def scratch():
        return [scratch(F32, AHEAD + 1, BLK, D), scratch(F32, AHEAD + 1, D, BLK), DMA((2, AHEAD + 1))]

    def loads(self, li, f, b):
        return [local(self.wo_h.at[li, cols(f)], self.wo.at[b], self.sem.at[0, b]), local(self.wi_h.at[li, :, cols(f)], self.wi.at[b], self.sem.at[1, b])]

    def load(self, *at):
        start(self.loads(*at))

    def ready(self, *at):
        wait(self.loads(*at))

    def w_out(self, li, f, b):
        return self.wo[b].astype(BF)

    def w_in(self, li, f, b):
        return self.wi[b].astype(BF)


class Whole:
    def __init__(self, vo, vi):
        self.vo, self.vi = vo, vi

    def load(self, *at):
        pass

    ready = load

    def w_out(self, li, f, b):
        return self.vo[li, cols(f)]

    def w_in(self, li, f, b):
        return self.vi[li, :, cols(f)]


class Acts:
    def __init__(self, hbm, bufs):
        self.h_o, self.z_o = hbm
        self.h, self.hb, self.acc, self.a, self.p, self.z, self.y, self.loss, self.hsem, self.zsem, self.isem = bufs
        self.nl, self.tok, dff = self.z_o.shape
        self.nf = dff // BLK
        self.n = self.nl * self.nf
        self.small = [pl.ds(r, PC * 7) for r in range(0, self.tok, PC * 7)]

    @staticmethod
    def scratch(tok):
        return [scratch(BF, tok, D), scratch(BF, 2, tok, D), scratch(F32, tok, D), scratch(BF, tok, BLK), scratch(BF, tok, BLK),
                scratch(BF, 2, tok, BLK), scratch(BF, tok, D), scratch(F32, SUB, LANE), DMA((2,)), DMA((2,)), DMA((2,))]

    def tiles(self, size):
        return [pl.ds(r, size) for r in range(0, self.tok, size)]

    def z_rows(self, li, f):
        return self.z_o.at[li, :, cols(f)]


class Forward:
    def __init__(self, acts, x, y, weights):
        self.t, self.x, self.y, self.w = acts, x, y, weights

    def at(self, s):
        return div(s, self.t.nf), rem(s, self.t.nf), rem(s, AHEAD + 1)

    def h_copy(self, li):
        return local(self.t.h, self.t.h_o.at[li], self.t.hsem.at[0])

    def z_copy(self, s):
        li, f, _ = self.at(s)
        b = rem(s, 2)
        return local(self.t.z.at[b], self.t.z_rows(li, f), self.t.zsem.at[b])

    def x_load(self):
        return local(self.x, self.t.h, self.t.isem.at[0])

    def y_load(self):
        return local(self.y, self.t.y, self.t.isem.at[1])

    def prologue(self):
        start([self.x_load(), self.y_load()])
        for s in range(AHEAD):
            self.w.load(*self.at(s))

    def take_x(self):
        t = self.t
        self.x_load().wait()
        for rows in t.small:
            t.acc[rows] = t.h[rows].astype(F32)
        self.h_copy(0).start()

    def block(self, s):
        t = self.t
        at = li, f, _ = self.at(s)
        b = rem(s, 2)
        self.w.ready(*at)
        when(s + AHEAD < t.n)(lambda: self.w.load(*self.at(s + AHEAD)))
        when(s > 1)(lambda: self.z_copy(s).wait())
        wi, wo = self.w.w_in(*at), self.w.w_out(*at)
        for rows in t.tiles(FT):
            z = dg(t.h[rows], wi, 1, 0).astype(BF)
            t.z[b, rows] = z
            t.a[rows] = gelu(z.astype(F32)).astype(BF)
        self.z_copy(s).start()
        for rows in t.tiles(FT):
            t.acc[rows] = t.acc[rows] + dg(t.a[rows], wo, 1, 0)
        when(f == t.nf - 1)(functools.partial(self.layer_end, li))

    def layer_end(self, li):
        t = self.t
        self.h_copy(0).wait()

        @when(li < t.nl - 1)
        def _():
            for rows in t.small:
                h = t.acc[rows].astype(BF)
                t.h[rows] = h
                t.acc[rows] = h.astype(F32)
            self.h_copy(li + 1).start()

        @when(li == t.nl - 1)
        def _():
            self.y_load().wait()
            t.loss[...] = jnp.zeros_like(t.loss)
            for rows in t.small:
                err = t.acc[rows].astype(BF).astype(F32) - t.y[rows].astype(F32)
                q = err.astype(BF)
                t.h[rows] = q
                t.acc[rows] = q.astype(F32)
                sq = jnp.sum((err * err).reshape(PC * 7 // SUB, SUB, D), axis=0)
                for c in range(0, D, LANE):
                    t.loss[...] += sq[:, c : c + LANE]

    def epilogue(self):
        wait([self.z_copy(s) for s in TWO])


class Backward:
    def __init__(self, acts, weights):
        self.t, self.w = acts, weights

    def at(self, s):
        t = self.t
        return t.nl - 1 - div(s, t.nf), rem(s, t.nf), rem(s, AHEAD + 1)

    def h_load(self, li):
        i = rem(li, 2)
        return local(self.t.h_o.at[li], self.t.hb.at[i], self.t.hsem.at[i])

    def z_load(self, s):
        li, f, _ = self.at(s)
        b = rem(s, 2)
        return local(self.t.z_rows(li, f), self.t.z.at[b], self.t.zsem.at[b])

    def prologue(self):
        self.z_load(0).start()
        for s in range(AHEAD):
            self.w.load(*self.at(s))
        self.h_load(self.t.nl - 1).start()

    def out_block(self, s, dst):
        t = self.t
        at = li, f, _ = self.at(s)
        b = rem(s, 2)
        self.z_load(s).wait()
        self.w.ready(*at)
        when(s + 1 < t.n)(lambda: self.z_load(s + 1).start())
        when(s + AHEAD < t.n)(lambda: self.w.load(*self.at(s + AHEAD)))

        @when(f == 0)
        def _():
            self.h_load(li).wait()
            when(li > 0)(lambda: self.h_load(li - 1).start())

        wo = self.w.w_out(*at)
        for rows in t.tiles(BT):
            a, slope = gelu_parts(t.z[b, rows].astype(F32))
            t.a[rows] = a.astype(BF)
            t.p[rows] = (dg(t.h[rows], wo, 1, 1) * slope).astype(BF)
        dst[...] = dg(t.a[...], t.h[...], 0, 0)

    def in_block(self, s, dst):
        t = self.t
        at = li, f, _ = self.at(s)
        dst[...] = dg(t.hb[rem(li, 2)], t.p[...], 0, 0)

        @when(li > 0)
        def _():
            wi = self.w.w_in(*at)
            for rows in t.tiles(BT):
                t.acc[rows] = t.acc[rows] + dg(t.p[rows], wi, 1, 1)

            @when(f == t.nf - 1)
            def _():
                for rows in t.small:
                    q = t.acc[rows].astype(BF)
                    t.h[rows] = q
                    t.acc[rows] = q.astype(F32)


class Owned:
    AHEAD = 4

    def __init__(self, g, n, nf, layer, mats, dst, sem, inside=()):
        self.g, self.n, self.nf, self.layer, self.mats, self.dst, self.sem, self.inside = g, n, nf, layer, mats, dst, sem, inside

    def due(self, s):
        g = self.g
        for T in TYPES:
            sem = self.sem.at[T, rem(s, self.AHEAD)]

            @when(both(g.inner if T in self.inside else g.sink, s < self.n + self.AHEAD))
            def _():
                when(s >= self.AHEAD)(lambda: local(self.dst[T].at[0], self.dst[T].at[0], sem).wait())

                @when(s < self.n)
                def _():
                    for ab in AB:
                        rows, col = g.fin(T, ab, True)
                        local(region(self.mats, T, self.layer(div(s, self.nf)), rem(s, self.nf), rows, col), self.dst[T].at[s, ab], sem).start()


def step_kernel(ns, nsl, lags, glags, lags2, glags2, scale, rho, lr, x, y, w_out, w_in, out_o, out_i, loss, h_o, z_o, *refs):
    def take(n):
        nonlocal refs
        mine, refs = refs[:n], refs[n:]
        return mine

    g = Geo()
    g.greet()
    mats = w_out, w_in
    acts = Acts((h_o, z_o), take(11))
    blocks = Weights(mats, take(3))
    whole = vo, vi = take(2)
    sc_bufs, ga_bufs = take(15), take(3)
    own, w_p, pieces = take(2), take(2), take(2)
    sq, wsem = take(2)
    shares, ssem, rsem = take(3)
    total = PairSum((g.partner, g.xn, g.yn, g.z1, g.z2), take(4))
    n, nf = acts.n, acts.nf
    last_first = lambda q: acts.nl - 1 - q

    fw = Forward(acts, x, y, blocks)
    fw.prologue()
    fw.take_x()

    def forward_step(s, _):
        fw.block(s)
        return 0

    lax.fori_loop(0, n, forward_step, 0)
    fw.epilogue()

    g.meet()
    sq[...] = jnp.zeros_like(sq)
    bw = Backward(acts, blocks)
    bw.prologue()
    owned = Owned(g, n, nf, last_first, mats, w_p, wsem)

    def keep_sums(T, k, ab, val):
        val = val * scale
        own[T][k, ab] = val
        sq[...] += val * val

    def add_up(bw, sc, s, j):
        block = bw.in_block if j else bw.out_block

        @when(s < n)
        def _():
            block(s, sc.S[j].at[rem(s, nsl)])
            sc.begin(j, s)

        sc.due(s, j)

    sc = Scatter(g, n, ns, nsl, lags, sc_bufs, keep_sums)

    def first_sums(s, _):
        owned.due(s)
        for j in TWO:
            add_up(bw, sc, s, j)
        return 0

    lax.fori_loop(0, sc.steps(), first_sums, 0)

    fw = Forward(acts, x, y, Whole(vo, vi))
    fw.prologue()

    @when(g.sink)
    def _():
        quarters = [sq[i * SUB : (i + 1) * SUB, j * LANE : (j + 1) * LANE] for i in TWO for j in TWO]
        shares[0] = sum(quarters[1:], quarters[0])
        copies = [pltpu.make_async_remote_copy(shares.at[0], shares.at[d], ssem.at[d], rsem.at[d], device_id=(g.mirror(d),), device_id_type=MESH)
                  for d in range(1, 16)]
        start(copies)
        wait(copies)
        squares = jnp.sum(jnp.sum(shares[...], axis=0))
        sq[...] = jnp.broadcast_to(rho / jnp.sqrt(jnp.broadcast_to(squares, (1, 1))), sq.shape)

    def piece(k):
        of = last_first(div(k, nf)) * nf + rem(k, nf)

        @when(both(g.sink, k < n))
        def _():
            for T in TYPES:
                for ab in AB:
                    pieces[T][k, ab] = (w_p[T][of, ab] + sq[...] * own[T][of, ab]).astype(BF)

    ga = Gather(g, n, nf, lambda q: q, glags, pieces, whole, ga_bufs)
    lead = (ga.mu3 + 1) // 2
    piece(0)

    def gather_step(s, _):
        piece(s + 1)
        ga.due(s, 0)
        when(s == 1)(fw.take_x)
        when(both(s >= lead, s < lead + n))(lambda: fw.block(s - lead))
        ga.due(s, 1)
        return 0

    lax.fori_loop(0, ga.steps(), gather_step, 0)
    fw.epilogue()

    bw2 = Backward(acts, Whole(vo, vi))
    bw2.prologue()
    total.part[0] = acts.loss[...]

    def update(T, k, ab, val):
        w_p[T][k, ab] = w_p[T][k, ab] - lr * (val * scale)

    owned2 = Owned(g, n, nf, last_first, mats, w_p, wsem, INSIDE)
    sc2 = Scatter(g, n, ns, nsl, lags2, sc_bufs, update, INSIDE)
    ga2 = Gather(g, n, nf, last_first, glags2, w_p, (out_o, out_i), ga_bufs, sc2.lam4 + 1, INSIDE)

    def second_sums(s, _):
        owned2.due(s)
        for j in TWO:
            add_up(bw2, sc2, s, j)
            ga2.due(s, j)
        total.due(s)
        return 0

    lax.fori_loop(0, ga2.steps(), second_sums, 0)
    loss[0, 0] = HALF * (jnp.sum(total.part[5]) * scale)


def sam_step(x, y, w_out, w_in, scale, rho, lr, ns=4, nsl=12, lags=(1, 4, 4, 4), glags=(4, 4, 4, 3), lags2=(1, 4, 2, 2), glags2=(4, 2, 2, 2), ngs=12):
    nl, dff, _ = w_out.shape
    tok = x.shape[0]
    n = nl * dff // BLK
    S = jax.ShapeDtypeStruct
    piece = lambda dt: [scratch(dt, n, 2, PC, BLK)] * 2
    bufs = Acts.scratch(tok) + Weights.scratch() + [scratch(BF, nl, dff, D), scratch(BF, nl, D, dff)]
    bufs += Scatter.scratch(ns, nsl) + Gather.scratch(n, ngs) + piece(F32) + piece(F32) + piece(BF)
    bufs += [scratch(F32, PC, BLK), DMA((2, Owned.AHEAD))] + [scratch(F32, 16, SUB, LANE), DMA((16,)), DMA((16,))] + PairSum.scratch(5)
    return pl.pallas_call(
        functools.partial(step_kernel, ns, nsl, lags, glags, lags2, glags2, scale, rho, lr),
        out_shape=[S(w_out.shape, F32), S(w_in.shape, F32), S((1, 1), F32), S((nl, tok, D), BF), S((nl, tok, dff), BF)],
        in_specs=[HBM] * 4,
        out_specs=[HBM] * 2 + [pl.BlockSpec(memory_space=pltpu.SMEM)] + [HBM] * 2,
        scratch_shapes=bufs,
        cost_estimate=pl.CostEstimate(flops=tok * D * dff * nl * 24, bytes_accessed=200 * MIB, transcendentals=0),
        compiler_params=pltpu.CompilerParams(collective_id=1, has_side_effects=True, vmem_limit_bytes=67043328),
        name="sam_step",
    )(x, y, w_out, w_in)


def solution(mesh):
    n_dev = mesh.shape["data"]

    def local_step(x_loc, y_loc, w_in, w_out):
        nl, d_model, d_ff = w_in.shape
        scale = 1.0 / (x_loc.shape[0] * n_dev * x_loc.shape[1] * d_model)
        rho = RHO_FRAC * math.sqrt(nl * (d_model + d_ff))
        x, y = [v.transpose(1, 0, 2).reshape(-1, d_model) for v in (x_loc, y_loc)]
        new_out, new_in, loss, _, _ = sam_step(x, y, w_out, w_in, scale, rho, LEARN_RATE)
        return new_in, new_out, loss.reshape(())

    specs = P("data"), P("data"), P(), P()
    return jax.shard_map(local_step, mesh=mesh, in_specs=specs, out_specs=(P(), P(), P()), check_vma=False)
```

```python
import functools
import math

import jax
import jax.numpy as jnp
from jax import lax
from jax.experimental import pallas as pl
from jax.experimental.pallas import tpu as pltpu
from jax.sharding import PartitionSpec as P

MESH = pl.DeviceIdType.MESH
F32, BF = jnp.float32, jnp.bfloat16
RHO_FRAC = 0.1
LEARN_RATE = 1.0
D = 512
BLK = 256
PC = 16
FT = 224
BT = 1568
SUB, LANE = 8, 128
NZ = 4
INSIDE = (1,)
HALF = 0.5
MIB = 2**20
GELU_A = math.sqrt(2.0 / math.pi)
GELU_B = 0.044715
TWO = AB = TYPES = DIRS = (0, 1)
SHAPES = ((BLK, D), (D, BLK))
ANY = pl.BlockSpec(memory_space=pl.ANY)
HBM = pl.BlockSpec(memory_space=pltpu.HBM)
VM = pl.BlockSpec(memory_space=pltpu.VMEM)
DMA = pltpu.SemaphoreType.DMA
rem, div = lax.rem, lax.div
when = pl.when


def both(*conds):
    return functools.reduce(jnp.logical_and, conds)


def ds(start, size):
    return pl.ds(pl.multiple_of(start, SUB), size)


def cols(f):
    return pl.ds(pl.multiple_of(f * BLK, BLK), BLK)


def dg(a, b, ca, cb):
    return lax.dot_general(a, b, (((ca,), (cb,)), ((), ())), preferred_element_type=F32)


def scratch(dtype, *shape):
    return pltpu.VMEM(shape, dtype)


def local(src, dst, sem):
    return pltpu.make_async_copy(src, dst, sem)


def start(copies):
    for c in copies:
        c.start()


def wait(copies):
    for c in copies:
        c.wait()


class Geo:
    def __init__(self):
        me = lax.axis_index("data")
        flip = lambda step: me + step - 2 * step * rem(me // step, 2)
        self.me = me
        self.c, self.x, self.y, self.z = [rem(me // step, n) for step, n in ((1, 2), (2, 2), (4, 2), (8, NZ))]
        self.partner, self.xn, self.yn, self.z1, self.z2 = [flip(1 << k) for k in range(5)]
        self.zm, self.zp = me - 8, me + 8
        self.e = self.z // 2
        self.sink = rem(self.z, NZ - 1) == 0
        self.inner = jnp.logical_not(self.sink)
        self.outward = self.me + 16 * self.e - 8
        self.inward = self.me + 8 - 16 * self.e
        self.across = self.inward
        self.w = (self.x, self.y)
        self.w2 = (self.y, self.x)
        self.n1 = (self.xn, self.yn)
        self.n2 = (self.yn, self.xn)

    def place(self, dirn):
        return self.z if dirn else NZ - 1 - self.z

    def greet(self):
        self.bar = pltpu.get_barrier_semaphore()
        hello = lambda dev: pl.semaphore_signal(self.bar, device_id=(dev,), device_id_type=MESH)
        for dev in (self.partner, self.xn, self.yn, self.z2):
            hello(dev)
        when(self.z > 0)(lambda: hello(self.zm))
        when(self.z < NZ - 1)(lambda: hello(self.zp))
        known = 1, 2, 4
        rest = [d for d in range(1, 16) if d not in known]
        when(self.sink)(lambda: [hello(self.mirror(d)) for d in rest] and None)
        self.sink_hellos = len(rest)

    def mirror(self, d):
        flips = (1 - 2 * self.c, 2 - 4 * self.x, 4 - 8 * self.y, 24 - 48 * self.e)
        return self.me + sum(flip for i, flip in enumerate(flips) if d >> i & 1)

    def meet(self):
        when(self.sink)(lambda: pl.semaphore_wait(self.bar, 5 + self.sink_hellos))
        when(self.inner)(lambda: pl.semaphore_wait(self.bar, 6))

    def half(self, T, c):
        R = SHAPES[T][0]
        return ds(c * (R // 2), R // 2)

    def part(self, T, ab, w):
        R = SHAPES[T][0]
        return self.c * (R // 2) + ab * (R // 4) + w * (R // 8)

    def zrow(self, T, ab, e):
        return self.part(T, ab, self.w[ab]) + e * (SHAPES[T][0] // 16)

    def fin(self, T, ab, mine):
        row = self.zrow(T, ab, self.e)
        w = self.w2[ab] if mine else 1 - self.w2[ab]
        if T:
            return ds(row + w * PC, PC), slice(None)
        return ds(row, PC), cols(w)


def region(out, T, li, f, rows, col=None):
    if T:
        return out[T].at[li, rows, cols(f)]
    return out[T].at[li, ds(f * BLK + rows.start, rows.size), slice(None) if col is None else col]


def schedule(s, j, lag, T):
    d = j - T - lag
    return None if d % 2 else s + d // 2


def run(k, n, what, T, *more):
    if k is not None:
        when(both(k >= 0, k < n))(functools.partial(what, T, k, *more))


class Scatter:
    FLOWS = FD, F1, F3, FM, FP, FI = range(0, 12, 2)
    CREDITS = CD, C1, C3, CM, CP = range(0, 10, 2)

    def __init__(self, g, n, ns, nsl, lags, bufs, deliver, inside=()):
        self.g, self.n, self.ns, self.nsl, self.deliver, self.inside = g, n, ns, nsl, deliver, inside
        self.S, self.rD, self.r1, self.rz, self.r3, self.ri = [bufs[2 * i : 2 * i + 2] for i in range(6)]
        self.ssem, self.rsem, self.cred = bufs[12:]
        ld, l1, self.lz, l3 = lags
        self.lam1 = ld
        self.lam2 = ld + l1
        self.lam4 = self.lam2 + (NZ - 1) * self.lz + l3

    @staticmethod
    def scratch(ns, nsl):
        out = []
        for lead, div in (((nsl,), 1), ((ns,), 2), ((ns, 2), 8), ((ns, 2, 2), 16), ((ns, 2), 0), ((ns, 2), 16)):
            for R, C in SHAPES:
                out.append(scratch(F32, *lead, *((R // div, C) if div else (PC, BLK))))
        return out + [DMA((2, 12, ns))] * 2 + [pltpu.SemaphoreType.REGULAR((2, 10))]

    def copy(self, T, flow, k, src, dst, dev):
        i = (T, flow, rem(k, self.ns))
        return pltpu.make_async_remote_copy(src, dst, self.ssem.at[i], self.rsem.at[i], device_id=(dev,), device_id_type=MESH)

    def take(self, T, credit, k):
        when(k >= self.ns)(lambda: pl.semaphore_wait(self.cred.at[T, credit]))

    def give(self, T, credit, k, dev):
        when(k + self.ns < self.n)(lambda: pl.semaphore_signal(self.cred.at[T, credit], device_id=(dev,), device_id_type=MESH))

    def slots(self, k):
        return rem(k, self.nsl), rem(k, self.ns)

    def to_core(self, T, k):
        s, q = self.slots(k)
        return self.copy(T, self.FD, k, self.S[T].at[s, self.g.half(T, 1 - self.g.c)], self.rD[T].at[q], self.g.partner)

    def first(self, T, k, ab):
        s, q = self.slots(k)
        rows = ds(self.g.part(T, ab, 1 - self.g.w[ab]), SHAPES[T][0] // 8)
        return self.copy(T, self.F1 + ab, k, self.S[T].at[s, rows], self.r1[T].at[q, ab], self.g.n1[ab])

    def zrows(self, T, ab, e):
        return ds(self.g.zrow(T, ab, e), SHAPES[T][0] // 16)

    def along(self, T, k, dirn, ab):
        s, q = self.slots(k)
        flow = (self.FP if dirn else self.FM) + ab
        src = self.S[T].at[s, self.zrows(T, ab, dirn)]
        return self.copy(T, flow, k, src, self.rz[T].at[q, ab, dirn], self.g.zp if dirn else self.g.zm)

    def last(self, T, k, ab):
        s, q = self.slots(k)
        return self.copy(T, self.F3 + ab, k, self.S[T].at[(s, *self.g.fin(T, ab, False))], self.r3[T].at[q, ab], self.g.n2[ab])

    def add(self, T, k, rows, val):
        s, _ = self.slots(k)
        self.S[T][s, rows] = self.S[T][s, rows] + val

    def begin(self, T, k):
        self.take(T, self.CD, k)
        self.to_core(T, k).start()

    def after_core(self, T, k):
        g = self.g
        self.to_core(T, k).wait()
        self.add(T, k, g.half(T, g.c), self.rD[T][rem(k, self.ns)])
        self.give(T, self.CD, k, g.partner)
        for ab in AB:
            self.take(T, self.C1 + ab, k)
            self.first(T, k, ab).start()

    def after_first(self, T, k):
        g = self.g
        for ab in AB:
            self.first(T, k, ab).wait()
        for ab in AB:
            self.add(T, k, ds(g.part(T, ab, g.w[ab]), SHAPES[T][0] // 8), self.r1[T][rem(k, self.ns), ab])
            self.give(T, self.C1 + ab, k, g.n1[ab])

    def line(self, T, k, dirn):
        g = self.g
        p = g.place(dirn)
        credit = self.CP if dirn else self.CM

        @when(k < self.n)
        def _():
            @when(p > 0)
            def _():
                for ab in AB:
                    self.along(T, k, dirn, ab).wait_recv()
                for ab in AB:
                    self.add(T, k, self.zrows(T, ab, dirn), self.rz[T][rem(k, self.ns), ab, dirn])
                self.give(T, credit, k, g.zm if dirn else g.zp)

            @when(p < NZ - 1)
            def _():
                self.take(T, credit, k)
                for ab in AB:
                    self.along(T, k, dirn, ab).start()

            @when(p == NZ - 1)
            def _():
                for ab in AB:
                    self.take(T, self.C3 + ab, k)
                    self.last(T, k, ab).start()

        @when(both(k > 0, p < NZ - 1))
        def _():
            for ab in AB:
                self.along(T, k - 1, dirn, ab).wait_send()

    def inner_in(self, T, k, e, ab):
        s, q = self.slots(k)
        src = self.S[T].at[s, self.zrows(T, ab, e)]
        return self.copy(T, (self.FP if e else self.FM) + ab, k, src, self.rz[T].at[q, ab, e], self.g.inward)

    def inner_across(self, T, k, ab):
        s, q = self.slots(k)
        src = self.S[T].at[s, self.zrows(T, ab, 1 - self.g.e)]
        return self.copy(T, self.FI + ab, k, src, self.ri[T].at[q, ab], self.g.across)

    def inner_send(self, T, k):
        every = [(e, ab) for e in DIRS for ab in AB]

        @when(both(self.g.sink, k < self.n))
        def _():
            self.take(T, self.CM, k)
            start([self.inner_in(T, k, e, ab) for e, ab in every])

        @when(both(self.g.sink, k > 0))
        def _():
            for e, ab in every:
                self.inner_in(T, k - 1, e, ab).wait_send()

    def inner_pass(self, T, k):
        q = rem(k, self.ns)

        @when(both(self.g.inner, k < self.n))
        def _():
            for e in DIRS:
                for ab in AB:
                    self.inner_in(T, k, e, ab).wait_recv()
                    self.add(T, k, self.zrows(T, ab, e), self.rz[T][q, ab, e])
            self.give(T, self.CM, k, self.g.outward)
            self.take(T, self.CP, k)
            start([self.inner_across(T, k, ab) for ab in AB])

        @when(both(self.g.inner, k > 0))
        def _():
            for ab in AB:
                self.inner_across(T, k - 1, ab).wait_send()

    def inner_end(self, T, k):
        @when(self.g.inner)
        def _():
            for ab in AB:
                self.inner_across(T, k, ab).wait_recv()
                self.add(T, k, self.zrows(T, ab, self.g.e), self.ri[T][rem(k, self.ns), ab])
            self.give(T, self.CP, k, self.g.across)
            for ab in AB:
                self.take(T, self.C3 + ab, k)
                self.last(T, k, ab).start()

    def after_last(self, T, k):
        g = self.g

        @when(g.inner if T in self.inside else g.sink)
        def _():
            s, q = self.slots(k)
            for ab in AB:
                self.last(T, k, ab).wait()
            for ab in AB:
                self.deliver(T, k, ab, self.S[T][(s, *g.fin(T, ab, True))] + self.r3[T][q, ab])
                self.give(T, self.C3 + ab, k, g.n2[ab])

    def due(self, s, j):
        for T in TYPES:
            run(schedule(s, j, self.lam4, T), self.n, self.after_last, T)
        for T in TYPES:
            k = schedule(s, j, self.lam2, T)
            run(k, self.n, self.after_first, T)
            if T in self.inside:
                run(k, self.n + 1, self.inner_send, T)
                run(schedule(s, j, self.lam2 + self.lz, T), self.n + 1, self.inner_pass, T)
                run(schedule(s, j, self.lam2 + 2 * self.lz, T), self.n, self.inner_end, T)
            elif k is not None:
                for dirn in DIRS:
                    run(k - self.g.place(dirn) * (self.lz // 2), self.n + 1, self.line, T, dirn)
        for T in TYPES:
            run(schedule(s, j, self.lam1, T), self.n, self.after_core, T)

    def steps(self):
        return self.n + (self.lam4 + 1) // 2 + 1


class Gather:
    FLOWS = F3, FM, FP, FE0, FE1, FD, FO = range(7)

    def __init__(self, g, n, nf, layer, lags, own, out, sems, start=0, inside=()):
        self.g, self.n, self.nf, self.layer, self.own, self.out = g, n, nf, layer, own, out
        self.inside = inside
        self.ssem, self.rsem, self.lsem = sems
        self.ns = self.ssem.shape[-1]
        l3, self.lz, le, ld = lags
        self.mu0 = start
        self.mu1 = start + l3
        self.mu2 = self.mu1 + (NZ - 1) * self.lz + le
        self.mu3 = self.mu2 + ld

    @staticmethod
    def scratch(n, ns):
        return [DMA((2, 7, ns)), DMA((2, 7, n)), DMA((2, 2, ns))]

    def region(self, T, k, rows, col=None):
        return region(self.out, T, self.layer(div(k, self.nf)), rem(k, self.nf), rows, col)

    def rows(self, T, k, row, div):
        return self.region(T, k, ds(row, SHAPES[T][0] // div))

    def copy(self, T, flow, k, src, dst, dev):
        return pltpu.make_async_remote_copy(src, dst, self.ssem.at[T, flow, rem(k, self.ns)], self.rsem.at[T, flow, k],
            device_id=(dev,), device_id_type=MESH)

    def keep(self, T, k, ab):
        rows, col = self.g.fin(T, ab, True)
        return local(self.own[T].at[k, ab], self.region(T, k, rows, col), self.lsem.at[T, ab, rem(k, self.ns)])

    def begin(self, T, k):
        g = self.g

        @when(g.inner if T in self.inside else g.sink)
        def _():
            for ab in AB:
                rows, col = g.fin(T, ab, True)
                self.keep(T, k, ab).start()
                self.copy(T, self.F3, k, self.own[T].at[k, ab], self.region(T, k, rows, col), g.n2[ab]).start()

    def over(self, T, flow, k, ref, send=True, recv=True):
        if send:
            local(ref, ref, self.ssem.at[T, flow, rem(k, self.ns)]).wait()
        if recv:
            local(ref, ref, self.rsem.at[T, flow, k]).wait()

    def line(self, T, k, dirn):
        g = self.g
        p = g.place(dirn)
        e = 1 - dirn
        flow = self.FP if dirn else self.FM
        pair = lambda k: self.rows(T, k, 0, 8)

        @when(k < self.n)
        def _():
            @when(p == 0)
            def _():
                for ab in AB:
                    self.keep(T, k, ab).wait()
                self.over(T, self.F3, k, self.own[T].at[k])

            when(p > 0)(lambda: self.over(T, flow, k, pair(k), send=False))
            parts = [self.rows(T, k, g.zrow(T, ab, e), 16) for ab in AB]

            @when(p < NZ - 1)
            def _():
                for r in parts:
                    self.copy(T, flow, k, r, r, g.zp if dirn else g.zm).start()

            for ab in AB:
                self.copy(T, self.FE0 + e, k, parts[ab], parts[ab], g.n1[ab]).start()

        when(both(k > 0, p < NZ - 1))(lambda: self.over(T, flow, k - 1, pair(k - 1), recv=False))

    def pair(self, T, k):
        return self.rows(T, k, 0, 8)

    def spread(self, T, k, e, *hops):
        g = self.g
        parts = [self.rows(T, k, g.zrow(T, ab, e), 16) for ab in AB]
        for flow, dev in hops:
            start([self.copy(T, flow, k, r, r, dev) for r in parts])
        for ab in AB:
            self.copy(T, self.FE0 + e, k, parts[ab], parts[ab], g.n1[ab]).start()

    def inner_begin(self, T, k):
        g = self.g

        @when(g.inner)
        def _():
            for ab in AB:
                self.keep(T, k, ab).wait()
            self.over(T, self.F3, k, self.own[T].at[k])
            for e in DIRS:
                when(g.e == e)(lambda: self.spread(T, k, e, (self.FP, g.across), (self.FM, g.outward)))

    def inner_pass(self, T, k):
        g = self.g
        for e in DIRS:

            @when(both(g.inner, g.e != e))
            def _():
                self.over(T, self.FP, k, self.pair(T, k), send=False)
                self.spread(T, k, e, (self.FO, g.outward))

            @when(both(g.sink, g.e == e))
            def _():
                self.over(T, self.FM, k, self.pair(T, k), send=False)
                self.spread(T, k, e)

    def inner_end(self, T, k):
        g = self.g
        for e in DIRS:

            @when(both(g.sink, g.e != e))
            def _():
                self.over(T, self.FO, k, self.pair(T, k), send=False)
                self.spread(T, k, e)

    def to_core(self, T, k):
        r = self.region(T, k, self.g.half(T, self.g.c))
        return self.copy(T, self.FD, k, r, r, self.g.partner)

    def after_first(self, T, k):
        for e in TWO:
            self.over(T, self.FE0 + e, k, self.rows(T, k, 0, 8))
        self.to_core(T, k).start()

    def done(self, T, k):
        self.to_core(T, k).wait()
        if T in self.inside:
            for flow in (self.FM, self.FP, self.FO):
                when(self.g.inner)(lambda: self.over(T, flow, k, self.pair(T, k), recv=False))

    def due(self, s, j):
        for T in TYPES:
            run(schedule(s, j, self.mu0, T), self.n, self.begin, T)
        for T in TYPES:
            k = schedule(s, j, self.mu1, T)
            if T in self.inside:
                run(k, self.n, self.inner_begin, T)
                run(schedule(s, j, self.mu1 + self.lz, T), self.n, self.inner_pass, T)
                run(schedule(s, j, self.mu1 + 2 * self.lz, T), self.n, self.inner_end, T)
            elif k is not None:
                for dirn in DIRS:
                    run(k - self.g.place(dirn) * (self.lz // 2), self.n + 1, self.line, T, dirn)
        for T in TYPES:
            run(schedule(s, j, self.mu2, T), self.n, self.after_first, T)
            run(schedule(s, j, self.mu3, T), self.n, self.done, T)

    def steps(self):
        return self.n + (self.mu3 + 1) // 2 + 1


class PairSum:
    GAP = 3

    def __init__(self, devs, bufs):
        self.devs = devs
        self.part, self.nbr, self.ssem, self.rsem = bufs

    @staticmethod
    def scratch(n):
        return [scratch(F32, n + 1, SUB, LANE), scratch(F32, n, SUB, LANE), DMA((n,)), DMA((n,))]

    def copy(self, r):
        return pltpu.make_async_remote_copy(self.part.at[r], self.nbr.at[r], self.ssem.at[r], self.rsem.at[r],
            device_id=(self.devs[r],), device_id_type=MESH)

    def finish(self, r):
        self.copy(r).wait()
        self.part[r + 1] = self.part[r] + self.nbr[r]

    def due(self, s):
        for r in range(len(self.devs)):
            when(s == r * self.GAP)(lambda: self.copy(r).start())
            when(s == r * self.GAP + self.GAP - 1)(lambda: self.finish(r))


def gelu(z):
    return z * (HALF + HALF * jnp.tanh(z * (GELU_A + (GELU_A * GELU_B) * (z * z))))


def gelu_parts(z):
    zz = z * z
    half = HALF + HALF * jnp.tanh(z * (GELU_A + (GELU_A * GELU_B) * zz))
    slope = half + (z * (half - half * half)) * (2 * GELU_A + (6 * GELU_A * GELU_B) * zz)
    return z * half, slope


AHEAD = 2


class Weights:
    def __init__(self, mats, bufs):
        self.wo_h, self.wi_h = mats
        self.wo, self.wi, self.sem = bufs

    @staticmethod
    def scratch():
        return [scratch(F32, AHEAD + 1, BLK, D), scratch(F32, AHEAD + 1, D, BLK), DMA((2, AHEAD + 1))]

    def loads(self, li, f, b):
        return [local(self.wo_h.at[li, cols(f)], self.wo.at[b], self.sem.at[0, b]), local(self.wi_h.at[li, :, cols(f)], self.wi.at[b], self.sem.at[1, b])]

    def load(self, *at):
        start(self.loads(*at))

    def ready(self, *at):
        wait(self.loads(*at))

    def w_out(self, li, f, b):
        return self.wo[b].astype(BF)

    def w_in(self, li, f, b):
        return self.wi[b].astype(BF)


class Whole:
    def __init__(self, vo, vi):
        self.vo, self.vi = vo, vi

    def load(self, *at):
        pass

    ready = load

    def w_out(self, li, f, b):
        return self.vo[li, cols(f)]

    def w_in(self, li, f, b):
        return self.vi[li, :, cols(f)]


class Acts:
    def __init__(self, hbm, bufs):
        self.h_o, self.z_o = hbm
        self.h, self.hb, self.acc, self.a, self.p, self.z, self.y, self.loss, self.hsem, self.zsem, self.isem = bufs
        self.nl, self.tok, dff = self.z_o.shape
        self.nf = dff // BLK
        self.n = self.nl * self.nf
        self.small = [pl.ds(r, PC * 7) for r in range(0, self.tok, PC * 7)]

    @staticmethod
    def scratch(tok):
        return [scratch(BF, tok, D), scratch(BF, 2, tok, D), scratch(F32, tok, D), scratch(BF, tok, BLK), scratch(BF, tok, BLK),
                scratch(BF, 2, tok, BLK), scratch(BF, tok, D), scratch(F32, SUB, LANE), DMA((2,)), DMA((2,)), DMA((2,))]

    def tiles(self, size):
        return [pl.ds(r, size) for r in range(0, self.tok, size)]

    def z_rows(self, li, f):
        return self.z_o.at[li, :, cols(f)]


class Forward:
    def __init__(self, acts, x, y, weights):
        self.t, self.x, self.y, self.w = acts, x, y, weights

    def at(self, s):
        return div(s, self.t.nf), rem(s, self.t.nf), rem(s, AHEAD + 1)

    def h_copy(self, li):
        return local(self.t.h, self.t.h_o.at[li], self.t.hsem.at[0])

    def z_copy(self, s):
        li, f, _ = self.at(s)
        b = rem(s, 2)
        return local(self.t.z.at[b], self.t.z_rows(li, f), self.t.zsem.at[b])

    def x_load(self):
        return local(self.x, self.t.h, self.t.isem.at[0])

    def y_load(self):
        return local(self.y, self.t.y, self.t.isem.at[1])

    def prologue(self):
        start([self.x_load(), self.y_load()])
        for s in range(AHEAD):
            self.w.load(*self.at(s))

    def take_x(self):
        t = self.t
        self.x_load().wait()
        for rows in t.small:
            t.acc[rows] = t.h[rows].astype(F32)
        self.h_copy(0).start()

    def block(self, s):
        t = self.t
        at = li, f, _ = self.at(s)
        b = rem(s, 2)
        self.w.ready(*at)
        when(s + AHEAD < t.n)(lambda: self.w.load(*self.at(s + AHEAD)))
        when(s > 1)(lambda: self.z_copy(s).wait())
        wi, wo = self.w.w_in(*at), self.w.w_out(*at)
        for rows in t.tiles(FT):
            z = dg(t.h[rows], wi, 1, 0).astype(BF)
            t.z[b, rows] = z
            t.a[rows] = gelu(z.astype(F32)).astype(BF)
        self.z_copy(s).start()
        for rows in t.tiles(BT):
            t.acc[rows] = t.acc[rows] + dg(t.a[rows], wo, 1, 0)
        when(f == t.nf - 1)(functools.partial(self.layer_end, li))

    def layer_end(self, li):
        t = self.t
        self.h_copy(0).wait()

        @when(li < t.nl - 1)
        def _():
            for rows in t.small:
                h = t.acc[rows].astype(BF)
                t.h[rows] = h
                t.acc[rows] = h.astype(F32)
            self.h_copy(li + 1).start()

        @when(li == t.nl - 1)
        def _():
            self.y_load().wait()
            t.loss[...] = jnp.zeros_like(t.loss)
            for rows in t.small:
                err = t.acc[rows].astype(BF).astype(F32) - t.y[rows].astype(F32)
                q = err.astype(BF)
                t.h[rows] = q
                t.acc[rows] = q.astype(F32)
                sq = jnp.sum((err * err).reshape(PC * 7 // SUB, SUB, D), axis=0)
                for c in range(0, D, LANE):
                    t.loss[...] += sq[:, c : c + LANE]

    def epilogue(self):
        wait([self.z_copy(s) for s in TWO])


class Backward:
    def __init__(self, acts, weights):
        self.t, self.w = acts, weights

    def at(self, s):
        t = self.t
        return t.nl - 1 - div(s, t.nf), rem(s, t.nf), rem(s, AHEAD + 1)

    def h_load(self, li):
        i = rem(li, 2)
        return local(self.t.h_o.at[li], self.t.hb.at[i], self.t.hsem.at[i])

    def z_load(self, s):
        li, f, _ = self.at(s)
        b = rem(s, 2)
        return local(self.t.z_rows(li, f), self.t.z.at[b], self.t.zsem.at[b])

    def prologue(self):
        self.z_load(0).start()
        for s in range(AHEAD):
            self.w.load(*self.at(s))
        self.h_load(self.t.nl - 1).start()

    def out_block(self, s, dst):
        t = self.t
        at = li, f, _ = self.at(s)
        b = rem(s, 2)
        self.z_load(s).wait()
        self.w.ready(*at)
        when(s + 1 < t.n)(lambda: self.z_load(s + 1).start())
        when(s + AHEAD < t.n)(lambda: self.w.load(*self.at(s + AHEAD)))

        @when(f == 0)
        def _():
            self.h_load(li).wait()
            when(li > 0)(lambda: self.h_load(li - 1).start())

        wo = self.w.w_out(*at)
        for rows in t.tiles(BT):
            a, slope = gelu_parts(t.z[b, rows].astype(F32))
            t.a[rows] = a.astype(BF)
            t.p[rows] = (dg(t.h[rows], wo, 1, 1) * slope).astype(BF)
        dst[...] = dg(t.a[...], t.h[...], 0, 0)

    def in_block(self, s, dst):
        t = self.t
        at = li, f, _ = self.at(s)
        dst[...] = dg(t.hb[rem(li, 2)], t.p[...], 0, 0)

        @when(li > 0)
        def _():
            wi = self.w.w_in(*at)
            for rows in t.tiles(BT):
                t.acc[rows] = t.acc[rows] + dg(t.p[rows], wi, 1, 1)

            @when(f == t.nf - 1)
            def _():
                for rows in t.small:
                    q = t.acc[rows].astype(BF)
                    t.h[rows] = q
                    t.acc[rows] = q.astype(F32)


class Owned:
    AHEAD = 4

    def __init__(self, g, n, nf, layer, mats, dst, sem, inside=()):
        self.g, self.n, self.nf, self.layer, self.mats, self.dst, self.sem, self.inside = g, n, nf, layer, mats, dst, sem, inside

    def due(self, s):
        g = self.g
        for T in TYPES:
            sem = self.sem.at[T, rem(s, self.AHEAD)]

            @when(both(g.inner if T in self.inside else g.sink, s < self.n + self.AHEAD))
            def _():
                when(s >= self.AHEAD)(lambda: local(self.dst[T].at[0], self.dst[T].at[0], sem).wait())

                @when(s < self.n)
                def _():
                    for ab in AB:
                        rows, col = g.fin(T, ab, True)
                        local(region(self.mats, T, self.layer(div(s, self.nf)), rem(s, self.nf), rows, col), self.dst[T].at[s, ab], sem).start()


def step_kernel(ns, nsl, lags, glags, lags2, glags2, scale, rho, lr, x, y, w_out, w_in, out_o, out_i, loss, h_o, z_o, *refs):
    def take(n):
        nonlocal refs
        mine, refs = refs[:n], refs[n:]
        return mine

    g = Geo()
    g.greet()
    mats = w_out, w_in
    acts = Acts((h_o, z_o), take(11))
    blocks = Weights(mats, take(3))
    whole = vo, vi = take(2)
    sc_bufs, ga_bufs = take(15), take(3)
    own, w_p, pieces = take(2), take(2), take(2)
    sq, wsem = take(2)
    shares, ssem, rsem = take(3)
    total = PairSum((g.partner, g.xn, g.yn, g.z1, g.z2), take(4))
    n, nf = acts.n, acts.nf
    last_first = lambda q: acts.nl - 1 - q

    fw = Forward(acts, x, y, blocks)
    fw.prologue()
    fw.take_x()

    def forward_step(s, _):
        fw.block(s)
        return 0

    lax.fori_loop(0, n, forward_step, 0)
    fw.epilogue()

    bw = Backward(acts, blocks)
    bw.prologue()
    sq[...] = jnp.zeros_like(sq)
    g.meet()
    owned = Owned(g, n, nf, last_first, mats, w_p, wsem)

    def keep_sums(T, k, ab, val):
        val = val * scale
        own[T][k, ab] = val
        sq[...] += val * val

    def add_up(bw, sc, s, j):
        block = bw.in_block if j else bw.out_block

        @when(s < n)
        def _():
            block(s, sc.S[j].at[rem(s, nsl)])
            sc.begin(j, s)

        sc.due(s, j)

    sc = Scatter(g, n, ns, nsl, lags, sc_bufs, keep_sums)

    def first_sums(s, _):
        owned.due(s)
        for j in TWO:
            add_up(bw, sc, s, j)
        return 0

    lax.fori_loop(0, sc.steps(), first_sums, 0)

    fw = Forward(acts, x, y, Whole(vo, vi))
    fw.prologue()

    @when(g.sink)
    def _():
        quarters = [sq[i * SUB : (i + 1) * SUB, j * LANE : (j + 1) * LANE] for i in TWO for j in TWO]
        shares[0] = sum(quarters[1:], quarters[0])
        copies = [pltpu.make_async_remote_copy(shares.at[0], shares.at[d], ssem.at[d], rsem.at[d], device_id=(g.mirror(d),), device_id_type=MESH)
                  for d in range(1, 16)]
        start(copies)
        wait(copies)
        squares = jnp.sum(jnp.sum(shares[...], axis=0))
        sq[...] = jnp.broadcast_to(rho / jnp.sqrt(jnp.broadcast_to(squares, (1, 1))), sq.shape)

    def piece(k):
        of = last_first(div(k, nf)) * nf + rem(k, nf)

        @when(both(g.sink, k < n))
        def _():
            for T in TYPES:
                for ab in AB:
                    pieces[T][k, ab] = (w_p[T][of, ab] + sq[...] * own[T][of, ab]).astype(BF)

    ga = Gather(g, n, nf, lambda q: q, glags, pieces, whole, ga_bufs)
    lead = (ga.mu3 + 1) // 2
    piece(0)

    def gather_step(s, _):
        piece(s + 1)
        ga.due(s, 0)
        when(s == 1)(fw.take_x)
        when(both(s >= lead, s < lead + n))(lambda: fw.block(s - lead))
        ga.due(s, 1)
        return 0

    lax.fori_loop(0, ga.steps(), gather_step, 0)
    fw.epilogue()

    bw2 = Backward(acts, Whole(vo, vi))
    bw2.prologue()
    total.part[0] = acts.loss[...]

    def update(T, k, ab, val):
        w_p[T][k, ab] = w_p[T][k, ab] - lr * (val * scale)

    owned2 = Owned(g, n, nf, last_first, mats, w_p, wsem, INSIDE)
    sc2 = Scatter(g, n, ns, nsl, lags2, sc_bufs, update, INSIDE)
    ga2 = Gather(g, n, nf, last_first, glags2, w_p, (out_o, out_i), ga_bufs, sc2.lam4 + 1, INSIDE)

    def second_sums(s, _):
        owned2.due(s)
        for j in TWO:
            add_up(bw2, sc2, s, j)
            ga2.due(s, j)
        total.due(s)
        return 0

    lax.fori_loop(0, ga2.steps(), second_sums, 0)
    loss[0, 0] = HALF * (jnp.sum(total.part[5]) * scale)


def sam_step(x, y, w_out, w_in, scale, rho, lr, ns=4, nsl=12, lags=(1, 4, 4, 4), glags=(4, 4, 4, 3), lags2=(1, 4, 2, 2), glags2=(4, 2, 2, 2), ngs=12):
    nl, dff, _ = w_out.shape
    tok = x.shape[0]
    n = nl * dff // BLK
    S = jax.ShapeDtypeStruct
    piece = lambda dt: [scratch(dt, n, 2, PC, BLK)] * 2
    bufs = Acts.scratch(tok) + Weights.scratch() + [scratch(BF, nl, dff, D), scratch(BF, nl, D, dff)]
    bufs += Scatter.scratch(ns, nsl) + Gather.scratch(n, ngs) + piece(F32) + piece(F32) + piece(BF)
    bufs += [scratch(F32, PC, BLK), DMA((2, Owned.AHEAD))] + [scratch(F32, 16, SUB, LANE), DMA((16,)), DMA((16,))] + PairSum.scratch(5)
    return pl.pallas_call(
        functools.partial(step_kernel, ns, nsl, lags, glags, lags2, glags2, scale, rho, lr),
        out_shape=[S(w_out.shape, F32), S(w_in.shape, F32), S((1, 1), F32), S((nl, tok, D), BF), S((nl, tok, dff), BF)],
        in_specs=[HBM] * 4,
        out_specs=[HBM] * 2 + [pl.BlockSpec(memory_space=pltpu.SMEM)] + [HBM] * 2,
        scratch_shapes=bufs,
        cost_estimate=pl.CostEstimate(flops=tok * D * dff * nl * 24, bytes_accessed=200 * MIB, transcendentals=0),
        compiler_params=pltpu.CompilerParams(collective_id=1, has_side_effects=True, vmem_limit_bytes=67043328),
        name="sam_step",
    )(x, y, w_out, w_in)


def solution(mesh):
    n_dev = mesh.shape["data"]

    def local_step(x_loc, y_loc, w_in, w_out):
        nl, d_model, d_ff = w_in.shape
        scale = 1.0 / (x_loc.shape[0] * n_dev * x_loc.shape[1] * d_model)
        rho = RHO_FRAC * math.sqrt(nl * (d_model + d_ff))
        x, y = [v.transpose(1, 0, 2).reshape(-1, d_model) for v in (x_loc, y_loc)]
        new_out, new_in, loss, _, _ = sam_step(x, y, w_out, w_in, scale, rho, LEARN_RATE)
        return new_in, new_out, loss.reshape(())

    specs = P("data"), P("data"), P(), P()
    return jax.shard_map(local_step, mesh=mesh, in_specs=specs, out_specs=(P(), P(), P()), check_vma=False)
```
